32 devices in a mesh: seq: 8 (over z, x), head: 4 (over y, core).
Axes of the slice: x: 2, y: 2, z: 4, core: 2. Of those that a mesh axis runs over, the one named last changes fastest.
Arguments:
- inputs: float32 [4096, 2048], P('seq'), may hold values from -6 to 6
- decay_exponent: int32 [8], P('head'), may hold values from 5 to 18, as said below
- first_gain: bfloat16 [2048], P('seq'), may hold values from 0.099609375 to 1.8984375
- first_bias: bfloat16 [2048], P('seq'), may hold values from -3 to 3
- query_weight: bfloat16 [2048, 2048], P('seq', 'head'), may hold values from -0.125 to 0.125
- key_weight: bfloat16 [2048, 2048], P('seq', 'head'), may hold values from -0.125 to 0.125
- value_weight: bfloat16 [2048, 4096], P('seq', 'head'), may hold values from -0.125 to 0.125
- gate_weight: bfloat16 [2048, 4096], P('seq', 'head'), may hold values from -0.125 to 0.125
- out_weight: bfloat16 [4096, 2048], P('head', 'seq'), may hold values from -0.09375 to 0.09375
- second_gain: bfloat16 [2048], P('seq'), may hold values from 0.099609375 to 1.8984375
- second_bias: bfloat16 [2048], P('seq'), may hold values from -3 to 3
- up_weight: bfloat16 [2048, 4096], P('seq', 'head'), may hold values from -0.125 to 0.125
- down_weight: bfloat16 [4096, 2048], P('head', 'seq'), may hold values from -0.09375 to 0.09375
- cotangent: float32 [4096, 2048], P('seq', 'head'), may hold values from -6 to 6
Outputs:
- layer_out: float32 [4096, 2048], P('seq', 'head')
- grad_inputs: float32 [4096, 2048], P('seq', 'head')
- grad_first_gain: float32 [2048], P('seq')
- grad_first_bias: float32 [2048], P('seq')
- grad_query_weight: float32 [2048, 2048], P('seq', 'head')
- grad_key_weight: float32 [2048, 2048], P('seq', 'head')
- grad_value_weight: float32 [2048, 4096], P('seq', 'head')
- grad_gate_weight: float32 [2048, 4096], P('seq', 'head')
- grad_out_weight: float32 [4096, 2048], P('head', 'seq')
- grad_second_gain: float32 [2048], P('seq')
- grad_second_bias: float32 [2048], P('seq')
- grad_up_weight: float32 [2048, 4096], P('seq', 'head')
- grad_down_weight: float32 [4096, 2048], P('head', 'seq')
The draws below stay inside these ranges and needn't reach their ends.
Inputs may be any that keep to these rules, and one draw needn't show every extreme that they name: `decay_exponent`: holds each of 5, 6, 8, 11, 15, 16, 17 and 18 once, in an order drawn from the seed.
All inputs are finite; a program needn't handle non-finite values.
Results may differ from the reference program's by a relative error of at most 0.02.
Values may be sent and summed in bfloat16 or wider, within the bound.
A program may use at most 256 MiB of HBM per device.

```python
import math
import jax
import jax.numpy as jnp
from jax import lax

D = 2048
H = 8
DK = 256
DV = 512
FF = 4096
SPAN = 512
TOKENS = 4096


def draw_decay_exponent(key, part):
    exponents = jnp.array([5, 6, 8, 11, 15, 16, 17, 18], dtype=jnp.int32)
    shuffled = jax.random.permutation(jax.random.fold_in(key, 7), H)
    return exponents[shuffled]


def block_scale(key, extent, pieces, least, top_value):
    gain = 1.0
    for axis_at, blocks in pieces:
        heights = jax.random.uniform(jax.random.fold_in(jax.random.fold_in(key, 6), axis_at), (blocks,), jnp.float32, least / len(pieces), top_value / len(pieces))
        gain = gain * jnp.repeat(jnp.exp(heights), extent[axis_at] // blocks).reshape((-1,) + (1,) * (len(extent) - 1 - axis_at))
    return gain


def gaussian(key, dims, deviation, limit, cuts=(), kind=jnp.bfloat16):
    level = block_scale(key, dims, cuts, -0.22, 0.18) if cuts else 1.0
    drawn = jax.random.normal(key, dims, jnp.float32) * deviation * level
    return jnp.minimum(jnp.maximum(drawn, -limit), limit).astype(kind)


def setup_inputs(seed: int = 0) -> dict:
    keys = jax.random.split(jax.random.key(seed), 15)
    inputs = gaussian(keys[0], (TOKENS, D), 1.0, 6.0, ((0, 8),), jnp.float32)
    decay_exponent = draw_decay_exponent(jax.random.fold_in(keys[14], 71), 0)
    first_gain = jnp.clip(1.0 + 0.18 * jax.random.normal(keys[2], (D,), jnp.float32), 0.099609375, 1.8984375).astype(jnp.bfloat16)
    first_bias = gaussian(keys[3], (D,), 0.5, 3.0, ((0, 8),))
    query_weight = gaussian(keys[4], (D, H * DK), D ** -0.5, 0.125, ((0, 8), (1, 4)))
    key_weight = gaussian(keys[5], (D, H * DK), D ** -0.5, 0.125, ((0, 8), (1, 4)))
    value_weight = gaussian(keys[6], (D, H * DV), D ** -0.5, 0.125, ((0, 8), (1, 4)))
    gate_weight = gaussian(keys[7], (D, H * DV), D ** -0.5, 0.125, ((0, 8), (1, 4)))
    out_weight = gaussian(keys[8], (H * DV, D), (H * DV) ** -0.5, 0.09375, ((0, 4), (1, 8)))
    second_gain = jnp.clip(1.0 + 0.18 * jax.random.normal(keys[9], (D,), jnp.float32), 0.099609375, 1.8984375).astype(jnp.bfloat16)
    second_bias = gaussian(keys[10], (D,), 0.5, 3.0, ((0, 8),))
    up_weight = gaussian(keys[11], (D, FF), D ** -0.5, 0.125, ((0, 8), (1, 4)))
    down_weight = gaussian(keys[12], (FF, D), FF ** -0.5, 0.09375, ((0, 4), (1, 8)))
    cotangent = gaussian(keys[13], (TOKENS, D), 1.0, 6.0, ((0, 8), (1, 4)), jnp.float32)
    return {"inputs": inputs, "decay_exponent": decay_exponent, "first_gain": first_gain, "first_bias": first_bias, "query_weight": query_weight, "key_weight": key_weight, "value_weight": value_weight, "gate_weight": gate_weight, "out_weight": out_weight, "second_gain": second_gain, "second_bias": second_bias, "up_weight": up_weight, "down_weight": down_weight, "cotangent": cotangent}


EPSILON = 1e-05
HIGHEST = lax.Precision.HIGHEST

def matmul(left_side, right_side):
    return jnp.dot(left_side, right_side, preferred_element_type=jnp.float32)

def layer_norm(stream, gain_vec, bias_vec):
    center = stream - lax.optimization_barrier(jnp.mean(stream, axis=-1, keepdims=True))
    inverse = lax.rsqrt(lax.optimization_barrier(jnp.mean(center * center, axis=-1, keepdims=True)) + EPSILON)
    normed = center * inverse
    return (normed * gain_vec + bias_vec, normed, inverse)

def group_norm(stream):
    center = stream - lax.optimization_barrier(jnp.mean(stream, axis=-1, keepdims=True))
    inverse = lax.rsqrt(lax.optimization_barrier(jnp.mean(center * center, axis=-1, keepdims=True)) + EPSILON)
    return (center * inverse, inverse)

def norm_back(upstream, gain_vec, normed, inverse):
    scaled = upstream * gain_vec
    return inverse * (scaled - lax.optimization_barrier(jnp.mean(scaled, axis=-1, keepdims=True)) - normed * lax.optimization_barrier(jnp.mean(scaled * normed, axis=-1, keepdims=True)))

def rotary_tables(positions, half_size):
    frequency = jnp.exp(-math.log(10000.0) * jnp.arange(half_size, dtype=jnp.float32) / (half_size - 1))
    angles = positions[:, None] * frequency[None, :]
    return (jnp.cos(angles)[:, None, :], jnp.sin(angles)[:, None, :])

def rotate(values, cos_table, sin_table):
    half_size = values.shape[-1] // 2
    first_half, second_half = (values[..., :half_size], values[..., half_size:])
    return jnp.concatenate([first_half * cos_table - second_half * sin_table, first_half * sin_table + second_half * cos_table], axis=-1)

def unrotate(values, cos_table, sin_table):
    half_size = values.shape[-1] // 2
    first_half, second_half = (values[..., :half_size], values[..., half_size:])
    return jnp.concatenate([first_half * cos_table + second_half * sin_table, second_half * cos_table - first_half * sin_table], axis=-1)

def gelu_parts(preact):
    normal_cdf = 0.5 * (1.0 + lax.erf(preact * 0.7071067811865476))
    density = jnp.exp(-0.5 * preact * preact) * 0.3989422804014327
    return (preact * normal_cdf, normal_cdf + preact * density)

def retain(query_in, key_in, value_in, lograte, reverse, span):
    length, head_count = (query_in.shape[0], query_in.shape[1])
    block_count = length // span
    offset = jnp.arange(span, dtype=jnp.float32)
    if reverse:
        offset = span - 1.0 - offset
    distance = offset[:, None] - offset[None, :]
    decay_mask = jnp.where(distance[None] >= 0, jnp.exp(jnp.maximum(distance, 0.0)[None] * lograte[:, None, None]), 0.0)
    weight_in = jnp.exp(offset[:, None] * lograte[None, :])[:, :, None]
    weight_out = jnp.exp((span - offset)[:, None] * lograte[None, :])[:, :, None]
    block_decay = jnp.exp(span * lograte)[:, None, None]

    def advance(carried, block):
        query_block, key_block, value_block = block
        query_wide = query_block.astype(jnp.float32)
        value_wide = value_block.astype(jnp.float32)
        scores = jnp.einsum('ihd,jhd->hij', query_wide, key_block.astype(jnp.float32), precision=HIGHEST)
        weights = (scores * decay_mask).astype(jnp.bfloat16).astype(jnp.float32)
        inner_sum = jnp.einsum('hij,jhe->ihe', weights, value_wide, precision=HIGHEST)
        cross_term = jnp.einsum('ihd,hde->ihe', query_wide, carried, precision=HIGHEST) * weight_in
        fresh_state = jnp.einsum('jhd,jhe->hde', key_block.astype(jnp.float32) * weight_out, value_wide, precision=HIGHEST)
        return (carried * block_decay + fresh_state, inner_sum + cross_term)
    blocks = (query_in.reshape(block_count, span, head_count, -1), key_in.reshape(block_count, span, head_count, -1), value_in.reshape(block_count, span, head_count, -1))
    start_state = jnp.zeros((head_count, query_in.shape[2], value_in.shape[2]), jnp.float32)
    final_state, outputs = lax.scan(advance, start_state, blocks, reverse=reverse)
    return (outputs.reshape(length, head_count, value_in.shape[2]), final_state)

def reference(inputs, decay_exponent, first_gain, first_bias, query_weight, key_weight, value_weight, gate_weight, out_weight, second_gain, second_bias, up_weight, down_weight, cotangent):
    bfloat = jnp.bfloat16
    total = inputs.shape[0]
    lograte = jnp.log1p(-jnp.exp2(-decay_exponent.astype(jnp.float32)))
    cos_table, sin_table = rotary_tables(jnp.arange(total, dtype=jnp.float32), DK // 2)
    gain_first = first_gain.astype(jnp.float32)
    gain_second = second_gain.astype(jnp.float32)
    normed_in, first_normed, first_inverse = layer_norm(inputs, gain_first, first_bias.astype(jnp.float32))
    hidden_in = normed_in.astype(bfloat)
    queries = rotate(matmul(hidden_in, query_weight).reshape(total, H, DK), cos_table, sin_table).astype(bfloat)
    rotated_keys = rotate(matmul(hidden_in, key_weight).reshape(total, H, DK), cos_table, sin_table).astype(bfloat)
    values = matmul(hidden_in, value_weight).astype(bfloat).reshape(total, H, DV)
    gate_act = matmul(hidden_in, gate_weight).reshape(total, H, DV)
    retained, final_state = retain(queries, rotated_keys, values, lograte, False, SPAN)
    group_normed, group_inverse = group_norm(retained)
    logistic = jax.nn.sigmoid(gate_act)
    swish_g = gate_act * logistic
    gated = (swish_g * group_normed).astype(bfloat).reshape(total, H * DV)
    middle = inputs + matmul(gated, out_weight)
    normed_mid, second_normed, second_inverse = layer_norm(middle, gain_second, second_bias.astype(jnp.float32))
    hidden_mid = normed_mid.astype(bfloat)
    preact = matmul(hidden_mid, up_weight)
    activated, gelu_slope = gelu_parts(preact)
    hidden_ff = activated.astype(bfloat)
    layer_out = middle + matmul(hidden_ff, down_weight)
    cot_bf = cotangent.astype(bfloat)
    grad_down_weight = matmul(hidden_ff.T, cot_bf)
    grad_preact = (matmul(cot_bf, down_weight.T) * gelu_slope).astype(bfloat)
    grad_up_weight = matmul(hidden_mid.T, grad_preact)
    grad_hidden_mid = matmul(grad_preact, up_weight.T)
    grad_second_gain = lax.optimization_barrier(jnp.sum(grad_hidden_mid * second_normed, axis=0))
    grad_second_bias = lax.optimization_barrier(jnp.sum(grad_hidden_mid, axis=0))
    grad_middle = cotangent + norm_back(grad_hidden_mid, gain_second, second_normed, second_inverse)
    grad_mid_bf = grad_middle.astype(bfloat)
    grad_out_weight = matmul(gated.T, grad_mid_bf)
    grad_gated = matmul(grad_mid_bf, out_weight.T).reshape(total, H, DV)
    grad_gates = (grad_gated * group_normed * (logistic + swish_g * (1.0 - logistic))).astype(bfloat).reshape(total, H * DV)
    grad_mixed = norm_back(grad_gated * swish_g, 1.0, group_normed, group_inverse).astype(bfloat)
    grad_query_rot, unused_one = retain(grad_mixed, values, rotated_keys, lograte, False, SPAN)
    grad_values_wide, unused_two = retain(rotated_keys, queries, grad_mixed, lograte, True, SPAN)
    grad_keys_rot, unused_three = retain(values, grad_mixed, queries, lograte, True, SPAN)
    grad_values = grad_values_wide.astype(bfloat).reshape(total, H * DV)
    grad_query_raw = unrotate(grad_query_rot, cos_table, sin_table).astype(bfloat).reshape(total, H * DK)
    grad_keys_raw = unrotate(grad_keys_rot, cos_table, sin_table).astype(bfloat).reshape(total, H * DK)
    grad_query_weight = matmul(hidden_in.T, grad_query_raw)
    grad_key_weight = matmul(hidden_in.T, grad_keys_raw)
    grad_value_weight = matmul(hidden_in.T, grad_values)
    grad_gate_weight = matmul(hidden_in.T, grad_gates)
    grad_hidden_in = matmul(grad_query_raw, query_weight.T) + matmul(grad_keys_raw, key_weight.T) + matmul(grad_values, value_weight.T) + matmul(grad_gates, gate_weight.T)
    grad_first_gain = lax.optimization_barrier(jnp.sum(grad_hidden_in * first_normed, axis=0))
    grad_first_bias = lax.optimization_barrier(jnp.sum(grad_hidden_in, axis=0))
    grad_inputs = grad_middle + norm_back(grad_hidden_in, gain_first, first_normed, first_inverse)
    return (layer_out, grad_inputs, grad_first_gain, grad_first_bias, grad_query_weight, grad_key_weight, grad_value_weight, grad_gate_weight, grad_out_weight, grad_second_gain, grad_second_bias, grad_up_weight, grad_down_weight)
```

```python
import functools
import math

import jax
import jax.numpy as jnp
from jax import lax
from jax.experimental import pallas as pl
from jax.experimental.pallas import tpu as pltpu
from jax.sharding import Mesh, PartitionSpec as P

EPSILON = 1e-05
BF = jnp.bfloat16
F32 = jnp.float32
MESH = pl.DeviceIdType.MESH
SWAP = ((0, 1), (1, 0))


def swap(array, axis):
    return lax.ppermute(array, axis, SWAP)


def ordered(bit, own, other, axis):
    low = jnp.where(bit == 0, own, other)
    high = jnp.where(bit == 0, other, own)
    return jnp.stack([low, high], axis=axis)


def pick(array, index, axis):
    return lax.dynamic_index_in_dim(array, index, axis, keepdims=False)


def dot(left, right, contract):
    return lax.dot_general(left, right, (contract, ((), ())), preferred_element_type=F32)


def mm(left, right):
    return dot(left, right, ((1,), (0,)))


def mm_t(left, right):
    return dot(left, right, ((1,), (1,)))


def t_mm(left, right):
    return dot(left, right, ((0,), (0,)))


class Plan:
    def __init__(self, seq_bits, head_bits):
        self.seq = [f"s{i}" for i in range(seq_bits)]
        self.head = [f"h{i}" for i in range(head_bits)]
        self.names = tuple(reversed(self.seq)) + ()
        self.seq_axes = tuple(reversed(self.seq))
        self.head_axes = tuple(reversed(self.head))
        self.pair = "s1" if seq_bits > 1 else "s0"
        self.low = [a for a in self.seq if a < self.pair]
        self.high = [a for a in self.seq if a > self.pair]


def gather_rows(plan, halves):
    bit = lax.axis_index(plan.pair)
    full = ordered(bit, pick(halves, bit, 0), swap(pick(halves, 1 - bit, 0), plan.pair), 0)
    rows, cols = full.shape[-2:]
    for axis in plan.high:
        full = ordered(lax.axis_index(axis), full, swap(full, axis), 0)
    full = full.reshape(-1, rows, cols)
    for axis in plan.low:
        full = ordered(lax.axis_index(axis), full, swap(full, axis), 1)
    return full.reshape(-1, cols)


def scatter_rows(plan, partial, rows):
    cols = partial.shape[1]
    part = partial.astype(BF)
    for axis in plan.low:
        bit = lax.axis_index(axis)
        part = part.reshape(-1, 2, rows, cols)
        got = swap(pick(part, 1 - bit, 1), axis)
        part = (pick(part, bit, 1).astype(F32) + got.astype(F32)).astype(BF)
    for axis in reversed(plan.high):
        bit = lax.axis_index(axis)
        part = part.reshape(2, -1, rows, cols)
        got = swap(pick(part, 1 - bit, 0), axis)
        part = (pick(part, bit, 0).astype(F32) + got.astype(F32)).astype(BF)
    part = part.reshape(2, rows, cols)
    bit = lax.axis_index(plan.pair)
    got = swap(pick(part, 1 - bit, 0), plan.pair)
    return ordered(bit, pick(part, bit, 0), got, 0).astype(F32)


class Square:
    def __init__(self, pair):
        self.pair = pair
        self.p = lax.axis_index(pair)
        self.y = lax.axis_index("h1")
        self.c = lax.axis_index("h0")
        self.S = {pair: 1 - self.p}
        self.Y = {"h1": 1 - self.y}
        self.C = {"h0": 1 - self.c}
        self.X = {"h1": 1 - self.y, "h0": 1 - self.c}

    def greet(self, cross=True):
        barrier = pltpu.get_barrier_semaphore()
        peers = [self.S, self.Y, self.C] + ([self.X] if cross else [])
        for peer in peers:
            pl.semaphore_signal(barrier, inc=1, device_id=peer, device_id_type=MESH)
        pl.semaphore_wait(barrier, len(peers))


def remote(source, target, sends, receives, index, device):
    return pltpu.make_async_remote_copy(
        src_ref=source,
        dst_ref=target,
        send_sem=sends.at[index],
        recv_sem=receives.at[index],
        device_id=device,
        device_id_type=MESH,
    )


def spread(sq, block, full, sends, receives, base, local_sem):
    rows, width = block.shape
    half = rows // 2

    def place(p, y, c, start, count):
        return full.at[p, pl.ds(start, count), pl.ds(pl.multiple_of((y * 2 + c) * width, width), width)]

    p, y, c = sq.p, sq.y, sq.c
    top, low = (0, half), (half, half)

    def own(part):
        return block.at[pl.ds(part[0], part[1]), :]

    def send(index, source, target, device):
        copy = remote(source, target, sends, receives, base + index, device)
        copy.start()
        return copy

    def relay(index, p_, y_, part, device):
        return send(index, place(p_, y_, c, *part), place(p_, y_, c, *part), device)

    k0 = send(0, own(top), place(p, y, c, *top), sq.S)
    k2 = send(2, own(low), place(p, y, c, *low), sq.Y)
    k6 = send(6, block, place(p, y, c, 0, rows), sq.C)
    k1 = send(1, own(low), place(p, y, c, *low), sq.S)
    k3 = send(3, own(top), place(p, y, c, *top), sq.Y)
    keep = pltpu.make_async_copy(block, place(p, y, c, 0, rows), local_sem)
    keep.start()
    k2.wait_recv()
    k4 = relay(4, p, 1 - y, low, sq.S)
    k9 = relay(9, p, 1 - y, low, sq.C)
    k0.wait_recv()
    k5 = relay(5, 1 - p, y, top, sq.Y)
    k7 = relay(7, 1 - p, y, top, sq.C)
    k1.wait_recv()
    k8 = relay(8, 1 - p, y, low, sq.C)
    k3.wait_recv()
    k10 = relay(10, p, 1 - y, top, sq.C)
    k5.wait_recv()
    k11 = relay(11, 1 - p, 1 - y, top, sq.C)
    k4.wait_recv()
    k12 = relay(12, 1 - p, 1 - y, low, sq.C)
    for copy in (k6, k7, k8, k9, k10, k11, k12):
        copy.wait_recv()
    for copy in (k0, k1, k2, k3, k4, k5, k6, k7, k8, k9, k10, k11, k12):
        copy.wait_send()
    keep.wait()


SPREAD_COPIES = 13
REDUCE_COPIES = 10


def reduce_in(sq, partial, result, near, total, arrived, sends, receives, base):
    rows, width = result.shape
    half = rows // 2
    p, y, c = sq.p, sq.y, sq.c
    top, low = pl.ds(0, half), pl.ds(half, half)

    def columns(y_, c_):
        return pl.ds(pl.multiple_of((y_ * 2 + c_) * width, width), width)

    def send(index, source, target, device):
        copy = remote(source, target, sends, receives, base + index, device)
        copy.start()
        return copy

    order = ((1 - p, 1 - y), (1 - p, y), (p, 1 - y), (p, y))
    hand = [
        send(i, partial.at[p_, :, columns(y_, 1 - c)], near.at[p_, y_], sq.C)
        for i, (p_, y_) in enumerate(order)
    ]

    def join(p_, y_):
        return partial[p_, :, columns(y_, c)].astype(F32) + near[p_, y_].astype(F32)

    hand[0].wait_recv()
    total[1 - p, 1 - y] = join(1 - p, 1 - y).astype(BF)
    a = send(4, total.at[1 - p, 1 - y, low], arrived.at[0], sq.S)
    b = send(5, total.at[1 - p, 1 - y, top], arrived.at[1], sq.Y)
    hand[1].wait_recv()
    total[1 - p, y] = join(1 - p, y).astype(BF)
    e = send(6, total.at[1 - p, y, low], arrived.at[2], sq.S)
    hand[2].wait_recv()
    total[p, 1 - y] = join(p, 1 - y).astype(BF)
    f = send(7, total.at[p, 1 - y, top], arrived.at[3], sq.Y)
    hand[3].wait_recv()
    result[...] = join(p, y)
    b.wait_recv()
    total[1 - p, y, top] = (total[1 - p, y, top].astype(F32) + arrived[1].astype(F32)).astype(BF)
    g = send(8, total.at[1 - p, y, top], arrived.at[4], sq.S)
    a.wait_recv()
    total[p, 1 - y, low] = (total[p, 1 - y, low].astype(F32) + arrived[0].astype(F32)).astype(BF)
    d = send(9, total.at[p, 1 - y, low], arrived.at[5], sq.Y)
    e.wait_recv()
    f.wait_recv()
    g.wait_recv()
    result[top, :] += arrived[4].astype(F32) + arrived[3].astype(F32)
    d.wait_recv()
    result[low, :] += arrived[2].astype(F32) + arrived[5].astype(F32)
    for copy in hand + [a, b, e, f, g, d]:
        copy.wait_send()


def reduce_scratch(rows, width):
    return [
        pltpu.VMEM((2, 2, rows, width), BF),
        pltpu.VMEM((2, 2, rows, width), BF),
        pltpu.VMEM((6, rows // 2, width), BF),
    ]


def semaphores(count):
    return [pltpu.SemaphoreType.DMA((count,)), pltpu.SemaphoreType.DMA((count,))]


def exchange(sq, first, second, stats, sends, receives, base):
    rows = first.shape[0]
    lane = lax.broadcasted_iota(jnp.int32, (rows, 128), 1)
    packed = jnp.where(lane == 0, first, second).T
    mine = sq.y * 2 + sq.c
    stats[mine] = packed[:8]
    copies = []
    for index, device in enumerate((sq.Y, sq.C, sq.X)):
        copy = remote(stats.at[mine], stats.at[mine], sends, receives, base + index, device)
        copy.start()
        copies.append(copy)
    for copy in copies:
        copy.wait_recv()
    for copy in copies:
        copy.wait_send()
    return [stats[q][0:1] for q in range(4)], [stats[q][1:2] for q in range(4)]


def upright(first, second):
    rows = first.shape[1]
    line = lax.broadcasted_iota(jnp.int32, (128, rows), 0)
    turned = jnp.where(line == 0, first, second).T
    return turned[:, 0:1], turned[:, 1:2]


def gather_kernel(pair, block, full, sends, receives, local_sem):
    sq = Square(pair)
    sq.greet(cross=False)
    spread(sq, block, full, sends, receives, 0, local_sem)


def gather_block(plan, block, number):
    rows, width = block.shape
    out = pl.pallas_call(
        functools.partial(gather_kernel, plan.pair),
        out_shape=jax.ShapeDtypeStruct((2, rows, 4 * width), block.dtype),
        in_specs=[pl.BlockSpec(memory_space=pltpu.VMEM)],
        out_specs=pl.BlockSpec(memory_space=pl.ANY),
        scratch_shapes=semaphores(SPREAD_COPIES) + [pltpu.SemaphoreType.DMA],
        compiler_params=pltpu.CompilerParams(collective_id=number, has_side_effects=True),
        name=f"gather_{number}",
    )(block)
    return out.reshape(2 * rows, 4 * width)


def scatter_kernel(pair, partial, result, near, total, arrived, sends, receives):
    sq = Square(pair)
    sq.greet(cross=False)
    reduce_in(sq, partial, result, near, total, arrived, sends, receives, 0)


def scatter_block(plan, partial, number):
    rows, width = partial.shape[0] // 2, partial.shape[1] // 4
    return pl.pallas_call(
        functools.partial(scatter_kernel, plan.pair),
        out_shape=jax.ShapeDtypeStruct((rows, width), F32),
        in_specs=[pl.BlockSpec(memory_space=pltpu.VMEM)],
        out_specs=pl.BlockSpec(memory_space=pltpu.VMEM),
        scratch_shapes=reduce_scratch(rows, width) + semaphores(REDUCE_COPIES),
        compiler_params=pltpu.CompilerParams(collective_id=number, has_side_effects=True),
        name=f"scatter_{number}",
    )(partial.astype(BF).reshape(2, rows, 4 * width))


def forward_kernel(
    pair, partial, stream, gain, bias, middle, normed, inverse, full,
    near, total, arrived, block, stats, sends, receives, local_sem,
):
    sq = Square(pair)
    sq.greet()
    reduce_in(sq, partial, middle, near, total, arrived, sends, receives, 0)
    whole = middle[...] + stream[...]
    middle[...] = whole
    mean = jnp.mean(whole, axis=1, keepdims=True)
    spread_ = jnp.mean(jnp.square(whole - mean), axis=1, keepdims=True)
    means, spreads = exchange(sq, mean, spread_, stats, sends, receives, REDUCE_COPIES)
    center = sum(means) * (1.0 / len(means))
    variance = sum(s + jnp.square(m - center) for m, s in zip(means, spreads)) * (1.0 / len(means))
    mean, scale = upright(center, lax.rsqrt(variance + EPSILON))
    inverse[...] = scale
    value = (middle[...] - mean) * scale
    normed[...] = value
    block[...] = (value * gain[...] + bias[...]).astype(BF)
    spread(sq, block, full, sends, receives, REDUCE_COPIES + 3, local_sem)


def backward_norm(sq, upstream, base_stream, gain, normed, inverse, result, sums, stats, sends, receives):
    value = upstream[...]
    product = value * normed[...]
    sums[0:1, :] = jnp.sum(product, axis=0, keepdims=True)
    sums[1:2, :] = jnp.sum(value, axis=0, keepdims=True)
    first = jnp.mean(value * gain[...], axis=1, keepdims=True)
    second = jnp.mean(product * gain[...], axis=1, keepdims=True)
    firsts, seconds = exchange(sq, first, second, stats, sends, receives, REDUCE_COPIES)
    share = 1.0 / len(firsts)
    first, second = upright(sum(firsts) * share, sum(seconds) * share)
    result[...] = base_stream[...] + inverse[...] * (upstream[...] * gain[...] - first - normed[...] * second)


def backward_kernel(
    pair, partial, stream, gain, normed, inverse, result, sums, full,
    near, total, arrived, upstream, block, stats, sends, receives, local_sem,
):
    sq = Square(pair)
    sq.greet()
    reduce_in(sq, partial, upstream, near, total, arrived, sends, receives, 0)
    backward_norm(sq, upstream, stream, gain, normed, inverse, result, sums, stats, sends, receives)
    block[...] = result[...].astype(BF)
    spread(sq, block, full, sends, receives, REDUCE_COPIES + 3, local_sem)


def last_kernel(
    pair, partial, stream, gain, normed, inverse, result, sums,
    near, total, arrived, upstream, stats, sends, receives,
):
    sq = Square(pair)
    sq.greet()
    reduce_in(sq, partial, upstream, near, total, arrived, sends, receives, 0)
    backward_norm(sq, upstream, stream, gain, normed, inverse, result, sums, stats, sends, receives)


def vmem(count):
    return [pl.BlockSpec(memory_space=pltpu.VMEM)] * count


def params(number):
    return pltpu.CompilerParams(collective_id=number, has_side_effects=True)


def forward_norm(plan, partial, stream, gain, bias, number):
    rows, width = stream.shape
    middle, normed, inverse, full = pl.pallas_call(
        functools.partial(forward_kernel, plan.pair),
        out_shape=(
            jax.ShapeDtypeStruct((rows, width), F32),
            jax.ShapeDtypeStruct((rows, width), F32),
            jax.ShapeDtypeStruct((rows, 1), F32),
            jax.ShapeDtypeStruct((2, rows, 4 * width), BF),
        ),
        in_specs=vmem(4),
        out_specs=tuple(vmem(3)) + (pl.BlockSpec(memory_space=pl.ANY),),
        scratch_shapes=reduce_scratch(rows, width)
        + [pltpu.VMEM((rows, width), BF), pltpu.VMEM((4, 8, rows), F32)]
        + semaphores(REDUCE_COPIES + 3 + SPREAD_COPIES)
        + [pltpu.SemaphoreType.DMA],
        compiler_params=params(number),
        name=f"forward_norm_{number}",
    )(partial.astype(BF).reshape(2, rows, 4 * width), stream, gain[None], bias[None])
    return middle, normed, inverse, full.reshape(2 * rows, 4 * width)


def middle_norm(plan, partial, stream, gain, normed, inverse, number):
    rows, width = stream.shape
    result, sums, full = pl.pallas_call(
        functools.partial(backward_kernel, plan.pair),
        out_shape=(
            jax.ShapeDtypeStruct((rows, width), F32),
            jax.ShapeDtypeStruct((2, width), F32),
            jax.ShapeDtypeStruct((2, rows, 4 * width), BF),
        ),
        in_specs=vmem(5),
        out_specs=tuple(vmem(2)) + (pl.BlockSpec(memory_space=pl.ANY),),
        scratch_shapes=reduce_scratch(rows, width)
        + [pltpu.VMEM((rows, width), F32), pltpu.VMEM((rows, width), BF), pltpu.VMEM((4, 8, rows), F32)]
        + semaphores(REDUCE_COPIES + 3 + SPREAD_COPIES)
        + [pltpu.SemaphoreType.DMA],
        compiler_params=params(number),
        name=f"middle_norm_{number}",
    )(partial.astype(BF).reshape(2, rows, 4 * width), stream, gain[None], normed, inverse)
    return result, sums, full.reshape(2 * rows, 4 * width)


def last_norm(plan, partial, stream, gain, normed, inverse, number):
    rows, width = stream.shape
    return pl.pallas_call(
        functools.partial(last_kernel, plan.pair),
        out_shape=(jax.ShapeDtypeStruct((rows, width), F32), jax.ShapeDtypeStruct((2, width), F32)),
        in_specs=vmem(5),
        out_specs=tuple(vmem(2)),
        scratch_shapes=reduce_scratch(rows, width)
        + [pltpu.VMEM((rows, width), F32), pltpu.VMEM((4, 8, rows), F32)]
        + semaphores(REDUCE_COPIES + 3),
        compiler_params=params(number),
        name=f"last_norm_{number}",
    )(partial.astype(BF).reshape(2, rows, 4 * width), stream, gain[None], normed, inverse)


def rotate(values, cosine, sine):
    half = values.shape[1] // 2
    first, second = values[:, :half], values[:, half:]
    return jnp.concatenate([first * cosine - second * sine, first * sine + second * cosine], axis=1)


def unrotate(values, cosine, sine):
    half = values.shape[1] // 2
    first, second = values[:, :half], values[:, half:]
    return jnp.concatenate([first * cosine + second * sine, second * cosine - first * sine], axis=1)


def carry(plan, local, lograte, length, reverse):
    state = list(local)
    reach = [jnp.zeros_like(s) for s in local]
    blocks = jnp.float32(length)

    def decay(count):
        return jnp.exp(count * blocks * lograte)

    low_index = jnp.float32(0)
    span = 1.0
    for axis in plan.low:
        bit = lax.axis_index(axis)
        late = (bit == 1) != reverse
        got = swap(jnp.stack([s.astype(BF) for s in state]), axis).astype(F32)
        between = low_index if not reverse else span - 1.0 - low_index
        for slot in range(2):
            reach[slot] = reach[slot] + jnp.where(late, decay(between), 0.0) * got[slot]
            before = jnp.where(late, got[slot], state[slot])
            after = jnp.where(late, state[slot], got[slot])
            state[slot] = before * decay(span) + after
        low_index = low_index + bit.astype(F32) * span
        span *= 2.0
    between = low_index if not reverse else span - 1.0 - low_index
    early, later = (1, 0) if reverse else (0, 1)
    reach[later] = reach[later] + decay(between) * state[early]
    total = state[early] * decay(span) + state[later]
    index = [low_index, low_index + span]
    span *= 2.0
    for axis in plan.high:
        bit = lax.axis_index(axis)
        late = (bit == 1) != reverse
        got = swap(total.astype(BF), axis).astype(F32)
        for slot in range(2):
            between = index[slot] if not reverse else span - 1.0 - index[slot]
            reach[slot] = reach[slot] + jnp.where(late, decay(between), 0.0) * got
            index[slot] = index[slot] + bit.astype(F32) * span
        before = jnp.where(late, got, total)
        after = jnp.where(late, total, got)
        total = before * decay(span) + after
        span *= 2.0
    return reach


def on_device(
    plan,
    inputs,
    decay_exponent,
    first_gain,
    first_bias,
    query_weight,
    key_weight,
    value_weight,
    gate_weight,
    out_weight,
    second_gain,
    second_bias,
    up_weight,
    down_weight,
    cotangent,
):
    length, model = inputs.shape
    rows = query_weight.shape[0]
    pair_bit = lax.axis_index(plan.pair)
    column = lax.axis_index(plan.head_axes)
    width = cotangent.shape[1]

    def halves(weight):
        return jnp.stack(jnp.split(weight, 2, axis=1))

    key_size = query_weight.shape[1] // 2
    value_size = value_weight.shape[1] // 2
    hidden = up_weight.shape[1] // 2

    group_one = jnp.concatenate([halves(query_weight), halves(key_weight), halves(value_weight)], axis=2)
    group_two = jnp.concatenate([halves(gate_weight), halves(out_weight.T)], axis=2)
    group_three = jnp.concatenate([halves(up_weight), halves(down_weight.T)], axis=2)
    qkv_full = gather_rows(plan, group_one)
    full_two = gather_rows(plan, group_two)
    full_three = gather_rows(plan, group_three)
    gate_full, out_full = full_two[:, :value_size], full_two[:, value_size:]
    up_full, down_full = full_three[:, :hidden], full_three[:, hidden:]
    vectors = lax.all_gather(
        jnp.stack([first_gain, first_bias, second_gain, second_bias]), plan.seq_axes, axis=1, tiled=True
    )
    vectors = lax.dynamic_slice_in_dim(vectors, column * width, width, 1).astype(F32)
    gain_one, bias_one, gain_two, bias_two = vectors[0], vectors[1], vectors[2], vectors[3]

    exponent = pick(decay_exponent, pair_bit, 0).astype(F32)
    lograte = jnp.log1p(-jnp.exp2(-exponent))
    offset = jnp.arange(length, dtype=F32)
    seq_index = lax.axis_index(plan.seq_axes)
    pair_weight = 2 ** plan.seq.index(plan.pair)
    first_slot = seq_index - pair_bit * pair_weight
    starts = jnp.stack([first_slot, first_slot + pair_weight]) * length
    positions = (starts.astype(F32)[:, None] + offset[None, :]).reshape(-1)
    frequency = jnp.exp(-math.log(10000.0) * jnp.arange(key_size // 2, dtype=F32) / (key_size // 2 - 1))
    angles = positions[:, None] * frequency[None, :]
    cosine, sine = jnp.cos(angles), jnp.sin(angles)
    distance = offset[:, None] - offset[None, :]
    mask = jnp.where(distance >= 0, jnp.exp(jnp.maximum(distance, 0.0) * lograte), 0.0)
    weight_in = jnp.exp(offset * lograte)[:, None]
    weight_out = jnp.exp((length - offset) * lograte)[:, None]
    weight_in_back = jnp.exp((length - 1.0 - offset) * lograte)[:, None]
    weight_out_back = jnp.exp((offset + 1.0) * lograte)[:, None]

    mean_one = jnp.mean(inputs, axis=1, keepdims=True)
    inverse_one = lax.rsqrt(jnp.mean(jnp.square(inputs - mean_one), axis=1, keepdims=True) + EPSILON)
    input_block = lax.dynamic_slice_in_dim(inputs, column * width, width, 1)
    normed_one = (input_block - mean_one) * inverse_one
    hidden_in = gather_block(plan, (normed_one * gain_one + bias_one).astype(BF), 1)
    cot_bf = gather_block(plan, cotangent.astype(BF), 2)

    projected = mm(hidden_in, qkv_full)
    queries = rotate(projected[:, :key_size], cosine, sine).astype(BF)
    keys = rotate(projected[:, key_size : 2 * key_size], cosine, sine).astype(BF)
    values = projected[:, 2 * key_size :].astype(BF)
    slots = [slice(0, length), slice(length, 2 * length)]
    local = [t_mm((keys[s].astype(F32) * weight_out).astype(BF), values[s]) for s in slots]
    incoming = [r.astype(BF) for r in carry(plan, local, lograte, length, False)]
    retained = []
    for s, state in zip(slots, incoming):
        weights = (mm_t(queries[s], keys[s]) * mask).astype(BF)
        retained.append(mm(weights, values[s]) + mm(queries[s], state) * weight_in)
    retained = jnp.concatenate(retained)
    center = retained - jnp.mean(retained, axis=1, keepdims=True)
    group_inverse = lax.rsqrt(jnp.mean(center * center, axis=1, keepdims=True) + EPSILON)
    group_normed = center * group_inverse
    gate_act = mm(hidden_in, gate_full)
    logistic = jax.nn.sigmoid(gate_act)
    swish = gate_act * logistic
    gated = (swish * group_normed).astype(BF)
    middle, normed_two, inverse_two, hidden_mid = forward_norm(
        plan, mm_t(gated, out_full), input_block, gain_two, bias_two, 3
    )

    preact = mm(hidden_mid, up_full)
    cdf = 0.5 * (1.0 + lax.erf(preact * 0.7071067811865476))
    slope = cdf + preact * (jnp.exp(-0.5 * preact * preact) * 0.3989422804014327)
    hidden_ff = (preact * cdf).astype(BF)
    layer_out = middle + scatter_block(plan, mm_t(hidden_ff, down_full), 4)

    grad_down = t_mm(cot_bf, hidden_ff)
    grad_preact = (mm(cot_bf, down_full) * slope).astype(BF)
    grad_up = t_mm(hidden_mid, grad_preact)
    grad_three = scatter_rows(plan, jnp.concatenate([grad_up, grad_down], axis=1), rows)
    grad_middle, sums_two, grad_mid_bf = middle_norm(
        plan, mm_t(grad_preact, up_full), cotangent, gain_two, normed_two, inverse_two, 5
    )
    grad_out = t_mm(grad_mid_bf, gated)
    grad_gated = mm(grad_mid_bf, out_full)
    grad_gates = (grad_gated * group_normed * (logistic + swish * (1.0 - logistic))).astype(BF)
    scaled = grad_gated * swish
    grad_mixed = (
        group_inverse
        * (
            scaled
            - jnp.mean(scaled, axis=1, keepdims=True)
            - group_normed * jnp.mean(scaled * group_normed, axis=1, keepdims=True)
        )
    ).astype(BF)
    grad_gate = t_mm(hidden_in, grad_gates)
    grad_two = scatter_rows(plan, jnp.concatenate([grad_gate, grad_out], axis=1), rows)

    back_local = [t_mm((queries[s].astype(F32) * weight_out_back).astype(BF), grad_mixed[s]) for s in slots]
    outgoing = [r.astype(BF) for r in carry(plan, back_local, lograte, length, True)]
    grad_query, grad_key, grad_value = [], [], []
    for s, state, back in zip(slots, incoming, outgoing):
        weights = (mm_t(grad_mixed[s], values[s]) * mask).astype(BF)
        grad_query.append(mm(weights, keys[s]) + mm_t(grad_mixed[s], state) * weight_in)
        grad_key.append(t_mm(weights, queries[s]) + mm_t(values[s], back) * weight_in_back)
        forward = (mm_t(queries[s], keys[s]) * mask).astype(BF)
        grad_value.append(t_mm(forward, grad_mixed[s]) + mm(keys[s], back) * weight_in_back)
    grad_query = unrotate(jnp.concatenate(grad_query), cosine, sine).astype(BF)
    grad_key = unrotate(jnp.concatenate(grad_key), cosine, sine).astype(BF)
    grad_value = jnp.concatenate(grad_value).astype(BF)
    grad_qkv = jnp.concatenate([grad_query, grad_key, grad_value], axis=1)
    grad_one = scatter_rows(plan, t_mm(hidden_in, grad_qkv), rows)
    partial_in = mm_t(grad_qkv, qkv_full) + mm_t(grad_gates, gate_full)
    grad_inputs, sums_one = last_norm(plan, partial_in, grad_middle, gain_one, normed_one, inverse_one, 6)

    sums = jnp.concatenate([sums_one, sums_two])
    placed = lax.dynamic_update_slice_in_dim(jnp.zeros((4, model), F32), sums, column * width, 1)
    placed = lax.psum(placed, plan.seq_axes + plan.head_axes)
    mine = lax.dynamic_slice_in_dim(placed, seq_index * rows, rows, 1)

    def joined(grad, start, size):
        piece = lax.slice_in_dim(grad, start, start + size, axis=2)
        return jnp.concatenate([piece[0], piece[1]], axis=1)

    return (
        layer_out,
        grad_inputs,
        mine[0],
        mine[1],
        joined(grad_one, 0, key_size),
        joined(grad_one, key_size, key_size),
        joined(grad_one, 2 * key_size, value_size),
        joined(grad_two, 0, value_size),
        joined(grad_two, value_size, value_size).T,
        mine[2],
        mine[3],
        joined(grad_three, 0, hidden),
        joined(grad_three, hidden, hidden).T,
    )


def solution(mesh):
    seq_bits = (mesh.shape["seq"]).bit_length() - 1
    head_bits = (mesh.shape["head"]).bit_length() - 1
    plan = Plan(seq_bits, head_bits)
    seq, head = plan.seq_axes, plan.head_axes
    fine = Mesh(mesh.devices.reshape((2,) * (seq_bits + head_bits)), seq + head)
    in_specs = (
        P(seq, None),
        P(head),
        P(seq),
        P(seq),
        P(seq, head),
        P(seq, head),
        P(seq, head),
        P(seq, head),
        P(head, seq),
        P(seq),
        P(seq),
        P(seq, head),
        P(head, seq),
        P(seq, head),
    )
    out_specs = (
        P(seq, head),
        P(seq, head),
        P(seq),
        P(seq),
        P(seq, head),
        P(seq, head),
        P(seq, head),
        P(seq, head),
        P(head, seq),
        P(seq),
        P(seq),
        P(seq, head),
        P(head, seq),
    )

    def step(*args):
        return on_device(plan, *args)

    return jax.shard_map(step, mesh=fine, in_specs=in_specs, out_specs=out_specs, check_vma=False)
```

```python
import functools
import math
import types

import jax
import jax.numpy as jnp
import numpy as np
from jax import lax
from jax.experimental import pallas as pl
from jax.experimental.pallas import tpu as pltpu
from jax.sharding import Mesh, PartitionSpec as P

EPSILON = 1e-05
BF = jnp.bfloat16
F32 = jnp.float32
MESH = pl.DeviceIdType.MESH
VMEM_LIMIT = 64000000
SWAP = ((0, 1), (1, 0))


def swap(array, axis):
    return lax.ppermute(array, axis, SWAP)


def ordered(bit, own, other, axis):
    low = jnp.where(bit == 0, own, other)
    high = jnp.where(bit == 0, other, own)
    return jnp.stack([low, high], axis=axis)


def pick(array, index, axis):
    return lax.dynamic_index_in_dim(array, index, axis, keepdims=False)


def dot(left, right, contract):
    return lax.dot_general(left, right, (contract, ((), ())), preferred_element_type=F32)


def mm(left, right):
    return dot(left, right, ((1,), (0,)))


def mm_t(left, right):
    return dot(left, right, ((1,), (1,)))


def t_mm(left, right):
    return dot(left, right, ((0,), (0,)))


class Plan:
    def __init__(self, seq_bits, head_bits):
        self.seq = [f"s{i}" for i in range(seq_bits)]
        self.head = [f"h{i}" for i in range(head_bits)]
        self.names = tuple(reversed(self.seq)) + ()
        self.seq_axes = tuple(reversed(self.seq))
        self.head_axes = tuple(reversed(self.head))
        self.pair = "s1" if seq_bits > 1 else "s0"
        self.low = [a for a in self.seq if a < self.pair]
        self.high = [a for a in self.seq if a > self.pair]


def gather_rows(plan, halves):
    bit = lax.axis_index(plan.pair)
    full = ordered(bit, pick(halves, bit, 0), swap(pick(halves, 1 - bit, 0), plan.pair), 0)
    rows, cols = full.shape[-2:]
    for axis in plan.high:
        full = ordered(lax.axis_index(axis), full, swap(full, axis), 0)
    full = full.reshape(-1, rows, cols)
    for axis in plan.low:
        full = ordered(lax.axis_index(axis), full, swap(full, axis), 1)
    return full.reshape(-1, cols)


def scatter_rows(plan, partial, rows):
    cols = partial.shape[1]
    part = partial.astype(BF)
    for axis in plan.low:
        bit = lax.axis_index(axis)
        part = part.reshape(-1, 2, rows, cols)
        got = swap(pick(part, 1 - bit, 1), axis)
        part = (pick(part, bit, 1).astype(F32) + got.astype(F32)).astype(BF)
    for axis in reversed(plan.high):
        bit = lax.axis_index(axis)
        part = part.reshape(2, -1, rows, cols)
        got = swap(pick(part, 1 - bit, 0), axis)
        part = (pick(part, bit, 0).astype(F32) + got.astype(F32)).astype(BF)
    part = part.reshape(2, rows, cols)
    bit = lax.axis_index(plan.pair)
    got = swap(pick(part, 1 - bit, 0), plan.pair)
    return ordered(bit, pick(part, bit, 0), got, 0).astype(F32)


class Square:
    def __init__(self, pair):
        self.pair = pair
        self.p = lax.axis_index(pair)
        self.y = lax.axis_index("h1")
        self.c = lax.axis_index("h0")
        self.S = {pair: 1 - self.p}
        self.Y = {"h1": 1 - self.y}
        self.C = {"h0": 1 - self.c}
        self.X = {"h1": 1 - self.y, "h0": 1 - self.c}

    def greet(self, cross=True):
        barrier = pltpu.get_barrier_semaphore()
        peers = [self.S, self.Y, self.C] + ([self.X] if cross else [])
        for peer in peers:
            pl.semaphore_signal(barrier, inc=1, device_id=peer, device_id_type=MESH)
        pl.semaphore_wait(barrier, len(peers))


def remote(source, target, sends, receives, index, device):
    return pltpu.make_async_remote_copy(
        src_ref=source,
        dst_ref=target,
        send_sem=sends.at[index],
        recv_sem=receives.at[index],
        device_id=device,
        device_id_type=MESH,
    )


def spread(sq, block, full, sends, receives, base, local_sem):
    rows, width = block.shape
    half = rows // 2

    def place(p, y, c, start, count):
        return full.at[p, pl.ds(start, count), pl.ds(pl.multiple_of((y * 2 + c) * width, width), width)]

    p, y, c = sq.p, sq.y, sq.c
    top, low = (0, half), (half, half)

    def own(part):
        return block.at[pl.ds(part[0], part[1]), :]

    def send(index, source, target, device):
        copy = remote(source, target, sends, receives, base + index, device)
        copy.start()
        return copy

    def relay(index, p_, y_, part, device):
        return send(index, place(p_, y_, c, *part), place(p_, y_, c, *part), device)

    k0 = send(0, own(top), place(p, y, c, *top), sq.S)
    k2 = send(2, own(low), place(p, y, c, *low), sq.Y)
    k6 = send(6, block, place(p, y, c, 0, rows), sq.C)
    k1 = send(1, own(low), place(p, y, c, *low), sq.S)
    k3 = send(3, own(top), place(p, y, c, *top), sq.Y)
    keep = pltpu.make_async_copy(block, place(p, y, c, 0, rows), local_sem)
    keep.start()
    k2.wait_recv()
    k4 = relay(4, p, 1 - y, low, sq.S)
    k9 = relay(9, p, 1 - y, low, sq.C)
    k0.wait_recv()
    k5 = relay(5, 1 - p, y, top, sq.Y)
    k7 = relay(7, 1 - p, y, top, sq.C)
    k1.wait_recv()
    k8 = relay(8, 1 - p, y, low, sq.C)
    k3.wait_recv()
    k10 = relay(10, p, 1 - y, top, sq.C)
    k5.wait_recv()
    k11 = relay(11, 1 - p, 1 - y, top, sq.C)
    k4.wait_recv()
    k12 = relay(12, 1 - p, 1 - y, low, sq.C)
    for copy in (k6, k7, k8, k9, k10, k11, k12):
        copy.wait_recv()
    for copy in (k0, k1, k2, k3, k4, k5, k6, k7, k8, k9, k10, k11, k12):
        copy.wait_send()
    keep.wait()


SPREAD_COPIES = 13
REDUCE_COPIES = 10


def reduce_in(sq, partial, result, near, total, arrived, sends, receives, base):
    rows, width = result.shape
    half = rows // 2
    p, y, c = sq.p, sq.y, sq.c
    top, low = pl.ds(0, half), pl.ds(half, half)

    def columns(y_, c_):
        return pl.ds(pl.multiple_of((y_ * 2 + c_) * width, width), width)

    def send(index, source, target, device):
        copy = remote(source, target, sends, receives, base + index, device)
        copy.start()
        return copy

    order = ((1 - p, 1 - y), (1 - p, y), (p, 1 - y), (p, y))
    hand = [
        send(i, partial.at[p_, :, columns(y_, 1 - c)], near.at[p_, y_], sq.C)
        for i, (p_, y_) in enumerate(order)
    ]

    def join(p_, y_):
        return partial[p_, :, columns(y_, c)].astype(F32) + near[p_, y_].astype(F32)

    hand[0].wait_recv()
    total[1 - p, 1 - y] = join(1 - p, 1 - y).astype(BF)
    a = send(4, total.at[1 - p, 1 - y, low], arrived.at[0], sq.S)
    b = send(5, total.at[1 - p, 1 - y, top], arrived.at[1], sq.Y)
    hand[1].wait_recv()
    total[1 - p, y] = join(1 - p, y).astype(BF)
    e = send(6, total.at[1 - p, y, low], arrived.at[2], sq.S)
    hand[2].wait_recv()
    total[p, 1 - y] = join(p, 1 - y).astype(BF)
    f = send(7, total.at[p, 1 - y, top], arrived.at[3], sq.Y)
    hand[3].wait_recv()
    result[...] = join(p, y)
    b.wait_recv()
    total[1 - p, y, top] = (total[1 - p, y, top].astype(F32) + arrived[1].astype(F32)).astype(BF)
    g = send(8, total.at[1 - p, y, top], arrived.at[4], sq.S)
    a.wait_recv()
    total[p, 1 - y, low] = (total[p, 1 - y, low].astype(F32) + arrived[0].astype(F32)).astype(BF)
    d = send(9, total.at[p, 1 - y, low], arrived.at[5], sq.Y)
    e.wait_recv()
    f.wait_recv()
    g.wait_recv()
    result[top, :] += arrived[4].astype(F32) + arrived[3].astype(F32)
    d.wait_recv()
    result[low, :] += arrived[2].astype(F32) + arrived[5].astype(F32)
    for copy in hand + [a, b, e, f, g, d]:
        copy.wait_send()


def reduce_scratch(rows, width):
    return [
        pltpu.VMEM((2, 2, rows, width), BF),
        pltpu.VMEM((2, 2, rows, width), BF),
        pltpu.VMEM((6, rows // 2, width), BF),
    ]


def semaphores(count):
    return [pltpu.SemaphoreType.DMA((count,)), pltpu.SemaphoreType.DMA((count,))]


def exchange(sq, first, second, stats, sends, receives, base):
    rows = first.shape[0]
    lane = lax.broadcasted_iota(jnp.int32, (rows, 128), 1)
    packed = jnp.where(lane == 0, first, second).T
    mine = sq.y * 2 + sq.c
    stats[mine] = packed[:8]
    copies = []
    for index, device in enumerate((sq.Y, sq.C, sq.X)):
        copy = remote(stats.at[mine], stats.at[mine], sends, receives, base + index, device)
        copy.start()
        copies.append(copy)
    for copy in copies:
        copy.wait_recv()
    for copy in copies:
        copy.wait_send()
    return [stats[q][0:1] for q in range(4)], [stats[q][1:2] for q in range(4)]


def upright(first, second):
    rows = first.shape[1]
    line = lax.broadcasted_iota(jnp.int32, (128, rows), 0)
    turned = jnp.where(line == 0, first, second).T
    return turned[:, 0:1], turned[:, 1:2]


def gather_kernel(pair, block, full, sends, receives, local_sem):
    sq = Square(pair)
    sq.greet(cross=False)
    spread(sq, block, full, sends, receives, 0, local_sem)


def gather_block(plan, block, number):
    rows, width = block.shape
    out = pl.pallas_call(
        functools.partial(gather_kernel, plan.pair),
        out_shape=jax.ShapeDtypeStruct((2, rows, 4 * width), block.dtype),
        in_specs=[pl.BlockSpec(memory_space=pltpu.VMEM)],
        out_specs=pl.BlockSpec(memory_space=pl.ANY),
        scratch_shapes=semaphores(SPREAD_COPIES) + [pltpu.SemaphoreType.DMA],
        compiler_params=pltpu.CompilerParams(collective_id=number, has_side_effects=True),
        name=f"gather_{number}",
    )(block)
    return out.reshape(2 * rows, 4 * width)


def scatter_kernel(pair, partial, result, near, total, arrived, sends, receives):
    sq = Square(pair)
    sq.greet(cross=False)
    reduce_in(sq, partial, result, near, total, arrived, sends, receives, 0)


def scatter_block(plan, partial, number):
    rows, width = partial.shape[0] // 2, partial.shape[1] // 4
    return pl.pallas_call(
        functools.partial(scatter_kernel, plan.pair),
        out_shape=jax.ShapeDtypeStruct((rows, width), F32),
        in_specs=[pl.BlockSpec(memory_space=pltpu.VMEM)],
        out_specs=pl.BlockSpec(memory_space=pltpu.VMEM),
        scratch_shapes=reduce_scratch(rows, width) + semaphores(REDUCE_COPIES),
        compiler_params=pltpu.CompilerParams(collective_id=number, has_side_effects=True),
        name=f"scatter_{number}",
    )(partial.astype(BF).reshape(2, rows, 4 * width))


def forward_kernel(
    pair, partial, stream, gain, bias, middle, normed, inverse, full,
    near, total, arrived, block, stats, sends, receives, local_sem,
):
    sq = Square(pair)
    sq.greet()
    reduce_in(sq, partial, middle, near, total, arrived, sends, receives, 0)
    whole = middle[...] + stream[...]
    middle[...] = whole
    mean = jnp.mean(whole, axis=1, keepdims=True)
    spread_ = jnp.mean(jnp.square(whole - mean), axis=1, keepdims=True)
    means, spreads = exchange(sq, mean, spread_, stats, sends, receives, REDUCE_COPIES)
    center = sum(means) * (1.0 / len(means))
    variance = sum(s + jnp.square(m - center) for m, s in zip(means, spreads)) * (1.0 / len(means))
    mean, scale = upright(center, lax.rsqrt(variance + EPSILON))
    inverse[...] = scale
    value = (middle[...] - mean) * scale
    normed[...] = value
    block[...] = (value * gain[...] + bias[...]).astype(BF)
    spread(sq, block, full, sends, receives, REDUCE_COPIES + 3, local_sem)


def backward_norm(sq, upstream, base_stream, gain, normed, inverse, result, sums, stats, sends, receives):
    value = upstream[...]
    product = value * normed[...]
    sums[0:1, :] = jnp.sum(product, axis=0, keepdims=True)
    sums[1:2, :] = jnp.sum(value, axis=0, keepdims=True)
    first = jnp.mean(value * gain[...], axis=1, keepdims=True)
    second = jnp.mean(product * gain[...], axis=1, keepdims=True)
    firsts, seconds = exchange(sq, first, second, stats, sends, receives, REDUCE_COPIES)
    share = 1.0 / len(firsts)
    first, second = upright(sum(firsts) * share, sum(seconds) * share)
    result[...] = base_stream[...] + inverse[...] * (upstream[...] * gain[...] - first - normed[...] * second)


def backward_kernel(
    pair, partial, stream, gain, normed, inverse, result, sums, full,
    near, total, arrived, upstream, block, stats, sends, receives, local_sem,
):
    sq = Square(pair)
    sq.greet()
    reduce_in(sq, partial, upstream, near, total, arrived, sends, receives, 0)
    backward_norm(sq, upstream, stream, gain, normed, inverse, result, sums, stats, sends, receives)
    block[...] = result[...].astype(BF)
    spread(sq, block, full, sends, receives, REDUCE_COPIES + 3, local_sem)


def last_kernel(
    pair, partial, stream, gain, normed, inverse, result, sums,
    near, total, arrived, upstream, stats, sends, receives,
):
    sq = Square(pair)
    sq.greet()
    reduce_in(sq, partial, upstream, near, total, arrived, sends, receives, 0)
    backward_norm(sq, upstream, stream, gain, normed, inverse, result, sums, stats, sends, receives)


def vmem(count):
    return [pl.BlockSpec(memory_space=pltpu.VMEM)] * count


def params(number):
    return pltpu.CompilerParams(collective_id=number, has_side_effects=True)


def forward_norm(plan, partial, stream, gain, bias, number):
    rows, width = stream.shape
    middle, normed, inverse, full = pl.pallas_call(
        functools.partial(forward_kernel, plan.pair),
        out_shape=(
            jax.ShapeDtypeStruct((rows, width), F32),
            jax.ShapeDtypeStruct((rows, width), F32),
            jax.ShapeDtypeStruct((rows, 1), F32),
            jax.ShapeDtypeStruct((2, rows, 4 * width), BF),
        ),
        in_specs=vmem(4),
        out_specs=tuple(vmem(3)) + (pl.BlockSpec(memory_space=pl.ANY),),
        scratch_shapes=reduce_scratch(rows, width)
        + [pltpu.VMEM((rows, width), BF), pltpu.VMEM((4, 8, rows), F32)]
        + semaphores(REDUCE_COPIES + 3 + SPREAD_COPIES)
        + [pltpu.SemaphoreType.DMA],
        compiler_params=params(number),
        name=f"forward_norm_{number}",
    )(partial.astype(BF).reshape(2, rows, 4 * width), stream, gain[None], bias[None])
    return middle, normed, inverse, full.reshape(2 * rows, 4 * width)


def middle_norm(plan, partial, stream, gain, normed, inverse, number):
    rows, width = stream.shape
    result, sums, full = pl.pallas_call(
        functools.partial(backward_kernel, plan.pair),
        out_shape=(
            jax.ShapeDtypeStruct((rows, width), F32),
            jax.ShapeDtypeStruct((2, width), F32),
            jax.ShapeDtypeStruct((2, rows, 4 * width), BF),
        ),
        in_specs=vmem(5),
        out_specs=tuple(vmem(2)) + (pl.BlockSpec(memory_space=pl.ANY),),
        scratch_shapes=reduce_scratch(rows, width)
        + [pltpu.VMEM((rows, width), F32), pltpu.VMEM((rows, width), BF), pltpu.VMEM((4, 8, rows), F32)]
        + semaphores(REDUCE_COPIES + 3 + SPREAD_COPIES)
        + [pltpu.SemaphoreType.DMA],
        compiler_params=params(number),
        name=f"middle_norm_{number}",
    )(partial.astype(BF).reshape(2, rows, 4 * width), stream, gain[None], normed, inverse)
    return result, sums, full.reshape(2 * rows, 4 * width)


def last_norm(plan, partial, stream, gain, normed, inverse, number):
    rows, width = stream.shape
    return pl.pallas_call(
        functools.partial(last_kernel, plan.pair),
        out_shape=(jax.ShapeDtypeStruct((rows, width), F32), jax.ShapeDtypeStruct((2, width), F32)),
        in_specs=vmem(5),
        out_specs=tuple(vmem(2)),
        scratch_shapes=reduce_scratch(rows, width)
        + [pltpu.VMEM((rows, width), F32), pltpu.VMEM((4, 8, rows), F32)]
        + semaphores(REDUCE_COPIES + 3),
        compiler_params=params(number),
        name=f"last_norm_{number}",
    )(partial.astype(BF).reshape(2, rows, 4 * width), stream, gain[None], normed, inverse)


class Bulk:
    def __init__(self, plan, at, shards, wholes, sends, receives, local_sem):
        self.shards, self.wholes, self.at = shards, wholes, at
        self.sends, self.receives, self.local_sem = sends, receives, local_sem
        self.axes = [plan.pair] + plan.high + plan.low
        self.high, self.low, self.lows = plan.high, plan.low, len(plan.low)
        self.bit = {axis: 1 << plan.seq.index(axis) for axis in self.axes}
        self.me = sum(at[axis] * self.bit[axis] for axis in self.axes)
        self.size = 1 << len(self.axes)
        self.copies, self.kept, self.passed = [], {}, set()

    def piece(self, unit, mask):
        rows = self.shards[unit].shape[0]
        return self.wholes[unit].at[pl.ds(pl.multiple_of((self.me ^ mask) * rows, rows), rows), :]

    def half(self, unit, which):
        width = self.wholes[unit].shape[1]
        return self.shards[unit].at[:, pl.ds(pl.multiple_of(which * width, width), width)]

    def link(self, unit, source, held, axis):
        return remote(
            source,
            self.piece(unit, held),
            self.sends,
            self.receives,
            unit * self.size + (held | self.bit[axis]),
            {axis: 1 - self.at[axis]},
        )

    def send(self, unit, source, held, axis):
        copy = self.link(unit, source, held, axis)
        copy.start()
        self.copies.append(copy)

    def begin(self, unit, axes):
        own = self.at[self.axes[0]]
        for axis in axes:
            self.send(unit, self.half(unit, 1 - own if axis == self.axes[0] else own), 0, axis)
        if self.axes[0] in axes:
            keep = pltpu.make_async_copy(self.half(unit, own), self.piece(unit, 0), self.local_sem.at[unit])
            keep.start()
            self.kept[unit] = keep

    def held_before(self, stage):
        held = [0]
        for axis in self.axes[:stage]:
            held = held + [m | self.bit[axis] for m in held]
        return held

    def forward(self, unit, mask, axes):
        for later in axes:
            self.send(unit, self.piece(unit, mask), mask, later)

    def arrive(self, unit, stage, masks, axes=None):
        axis = self.axes[stage]
        for held in self.held_before(stage):
            mask = held | self.bit[axis]
            if not masks(mask):
                continue
            pltpu.make_async_remote_copy(
                src_ref=self.piece(unit, mask),
                dst_ref=self.piece(unit, mask),
                send_sem=self.sends.at[unit * self.size + mask],
                recv_sem=self.receives.at[unit * self.size + mask],
                device_id={axis: 1 - self.at[axis]},
                device_id_type=MESH,
            ).wait_recv()
            self.forward(unit, mask, self.axes[stage + 1 :] if axes is None else axes)

    def paired(self, unit, axes=None):
        self.arrive(unit, 0, lambda mask: True, axes)

    def first(self, unit):
        for stage in range(1, len(self.axes) - self.lows):
            self.arrive(unit, stage, lambda mask: not mask & self.bit[self.axes[0]])

    def second(self, unit):
        for stage in range(1, len(self.axes) - self.lows):
            self.arrive(unit, stage, lambda mask: mask & self.bit[self.axes[0]])

    def finish(self, unit):
        for stage in range(len(self.axes) - self.lows, len(self.axes)):
            self.arrive(unit, stage, lambda mask: True)
        self.kept[unit].wait()

    def drain(self):
        for copy in self.copies:
            copy.wait_send()


def together(process, *hooks):
    for number, _ in enumerate(process):
        if number < len(hooks):
            hooks[number]()


def carried(plan, at, state, reach, low_buf, high_buf, rate, length, reverse, sends, receives, base):
    index = base
    low_index = jnp.float32(0)
    span = 1.0
    copies = []

    def decay(count):
        return jnp.exp(rate * (count * float(length)))

    for slot in range(2):
        reach[slot] = jnp.zeros(reach.shape[1:], F32)
    for number, axis in enumerate(plan.low):
        bit = at[axis].astype(F32)
        late = 1.0 - bit if reverse else bit
        for slot in range(2):
            low_buf[2 * number, slot] = state[slot].astype(BF)
        copy = remote(low_buf.at[2 * number], low_buf.at[2 * number + 1], sends, receives, index, {axis: 1 - at[axis]})
        copy.start()
        copies.append(copy)
        index += 1
        yield
        copy.wait_recv()
        between = span - 1.0 - low_index if reverse else low_index
        step_decay = decay(span)
        take, keep = late * step_decay + (1.0 - late), late + (1.0 - late) * step_decay
        for slot in range(2):
            got = low_buf[2 * number + 1, slot].astype(F32)
            reach[slot] += got * (late * decay(between))
            state[slot] = got * take + state[slot] * keep
        low_index = low_index + bit * span
        span *= 2.0
    between = span - 1.0 - low_index if reverse else low_index
    early, later = (1, 0) if reverse else (0, 1)
    reach[later] += state[early] * decay(between)
    state[0] = state[early] * decay(span) + state[later]
    order = [low_index, low_index + span]
    span *= 2.0
    for number, axis in enumerate(plan.high):
        bit = at[axis].astype(F32)
        late = 1.0 - bit if reverse else bit
        high_buf[2 * number] = state[0].astype(BF)
        copy = remote(high_buf.at[2 * number], high_buf.at[2 * number + 1], sends, receives, index, {axis: 1 - at[axis]})
        copy.start()
        copies.append(copy)
        index += 1
        yield
        copy.wait_recv()
        step_decay = decay(span)
        take, keep = late * step_decay + (1.0 - late), late + (1.0 - late) * step_decay
        got = high_buf[2 * number + 1].astype(F32)
        for slot in range(2):
            between = span - 1.0 - order[slot] if reverse else order[slot]
            reach[slot] += got * (late * decay(between))
            order[slot] = order[slot] + bit * span
        state[0] = got * take + state[0] * keep
        span *= 2.0
    for copy in copies:
        copy.wait_send()


def carry_buffers(plan, key_size, value_size):
    return [
        pltpu.VMEM((2, key_size, value_size), F32),
        pltpu.VMEM((2, key_size, value_size), F32),
        pltpu.VMEM((2 * max(len(plan.low), 1), 2, key_size, value_size), BF),
        pltpu.VMEM((2 * max(len(plan.high), 1), key_size, value_size), BF),
    ]


def spread_steps(sq, block, full, sends, receives, base, local_sem):
    rows, width = block.shape
    half = rows // 2
    p, y, c = sq.p, sq.y, sq.c
    top, low = (0, half), (half, half)

    def place(p_, y_, c_, start, count):
        return full.at[p_, pl.ds(start, count), pl.ds(pl.multiple_of((y_ * 2 + c_) * width, width), width)]

    def own(part):
        return block.at[pl.ds(part[0], part[1]), :]

    def send(index, source, target, device):
        copy = remote(source, target, sends, receives, base + index, device)
        copy.start()
        return copy

    def relay(index, p_, y_, part, device):
        return send(index, place(p_, y_, c, *part), place(p_, y_, c, *part), device)

    k0 = send(0, own(top), place(p, y, c, *top), sq.S)
    k2 = send(2, own(low), place(p, y, c, *low), sq.Y)
    k6 = send(6, block, place(p, y, c, 0, rows), sq.C)
    k1 = send(1, own(low), place(p, y, c, *low), sq.S)
    k3 = send(3, own(top), place(p, y, c, *top), sq.Y)
    keep = pltpu.make_async_copy(block, place(p, y, c, 0, rows), local_sem)
    keep.start()
    yield
    k2.wait_recv()
    k4 = relay(4, p, 1 - y, low, sq.S)
    k9 = relay(9, p, 1 - y, low, sq.C)
    k0.wait_recv()
    k5 = relay(5, 1 - p, y, top, sq.Y)
    k7 = relay(7, 1 - p, y, top, sq.C)
    yield
    k1.wait_recv()
    k8 = relay(8, 1 - p, y, low, sq.C)
    k3.wait_recv()
    k10 = relay(10, p, 1 - y, top, sq.C)
    yield
    k5.wait_recv()
    k11 = relay(11, 1 - p, 1 - y, top, sq.C)
    k4.wait_recv()
    k12 = relay(12, 1 - p, 1 - y, low, sq.C)
    for copy in (k6, k7, k8, k9, k10, k11, k12):
        copy.wait_recv()
    for copy in (k0, k1, k2, k3, k4, k5, k6, k7, k8, k9, k10, k11, k12):
        copy.wait_send()
    keep.wait()


def pass_steps(sq, block, full, sends, receives, base, wide):
    rows = full.shape[1]
    width = full.shape[2] // 4
    half = rows // 2
    p, y, c = sq.p, sq.y, sq.c
    parts = ((0, half), (half, half))
    copies = []

    def place(p_, y_, part):
        columns = pl.ds(pl.multiple_of((y_ * 2 + c) * width, width), width)
        return full.at[p_, pl.ds(part[0], part[1]), columns]

    def send(index, source, p_, y_, part, device):
        copy = remote(source, place(p_, y_, part), sends, receives, base + index, device)
        copy.start()
        copies.append(copy)
        return copy

    def own(part):
        return block.at[pl.ds(part[0], part[1]), :]

    far = [send(i, own(part), p, y, part, sq.S) for i, part in enumerate(parts)]
    beside, near = [], []
    if wide:
        beside += [send(2 + i, own(part), p, y, part, sq.Y) for i, part in enumerate(parts)]
        near += [send(4 + i, own(part), p, y, part, sq.C) for i, part in enumerate(parts)]
    yield
    other = []
    for i, part in enumerate(parts):
        far[i].wait_recv()
        other.append(send(6 + i, place(1 - p, y, part), 1 - p, y, part, sq.Y))
        near.append(send(8 + i, place(1 - p, y, part), 1 - p, y, part, sq.C))
    yield
    for i, part in enumerate(parts):
        if wide:
            beside[i].wait_recv()
            near.append(send(10 + i, place(p, 1 - y, part), p, 1 - y, part, sq.C))
        other[i].wait_recv()
        near.append(send(12 + i, place(1 - p, 1 - y, part), 1 - p, 1 - y, part, sq.C))
    yield
    for copy in near:
        copy.wait_recv()
    for copy in copies:
        copy.wait_send()


PASS_COPIES = 14


def reduce_steps(sq, block_of, result, hand, near, total, arrived, sends, receives, base):
    rows, width = result.shape
    half = rows // 2
    p, y, c = sq.p, sq.y, sq.c
    top, low = pl.ds(0, half), pl.ds(half, half)

    def send(index, source, target, device):
        copy = remote(source, target, sends, receives, base + index, device)
        copy.start()
        return copy

    order = ((1 - p, 1 - y), (1 - p, y), (p, 1 - y), (p, y))
    given = []
    for i, (p_, y_) in enumerate(order):
        hand[p_, y_] = block_of(p_, y_, 1 - c).astype(BF)
        given.append(send(i, hand.at[p_, y_], near.at[p_, y_], sq.C))

    def join(i):
        p_, y_ = order[i]
        own = block_of(p_, y_, c)
        given[i].wait_recv()
        return own + near[p_, y_].astype(F32)

    total[1 - p, 1 - y] = join(0).astype(BF)
    a = send(4, total.at[1 - p, 1 - y, low], arrived.at[0], sq.S)
    b = send(5, total.at[1 - p, 1 - y, top], arrived.at[1], sq.Y)
    total[1 - p, y] = join(1).astype(BF)
    e = send(6, total.at[1 - p, y, low], arrived.at[2], sq.S)
    total[p, 1 - y] = join(2).astype(BF)
    f = send(7, total.at[p, 1 - y, top], arrived.at[3], sq.Y)
    result[...] = join(3)
    yield
    b.wait_recv()
    total[1 - p, y, top] = (total[1 - p, y, top].astype(F32) + arrived[1].astype(F32)).astype(BF)
    g = send(8, total.at[1 - p, y, top], arrived.at[4], sq.S)
    a.wait_recv()
    total[p, 1 - y, low] = (total[p, 1 - y, low].astype(F32) + arrived[0].astype(F32)).astype(BF)
    d = send(9, total.at[p, 1 - y, low], arrived.at[5], sq.Y)
    yield
    e.wait_recv()
    f.wait_recv()
    g.wait_recv()
    result[top, :] += arrived[4].astype(F32) + arrived[3].astype(F32)
    d.wait_recv()
    result[low, :] += arrived[2].astype(F32) + arrived[5].astype(F32)
    for copy in given + [a, b, e, f, g, d]:
        copy.wait_send()


def reduce_room(rows, width):
    return [pltpu.VMEM((2, 2, rows, width), BF)] * 3 + [pltpu.VMEM((6, rows // 2, width), BF)]


def flipped(plan, at, mask):
    return {axis: 1 - at[axis] for i, axis in enumerate(plan.seq) if mask >> i & 1}


def greet_all(plan, at, sq):
    barrier = pltpu.get_barrier_semaphore()
    peers = [flipped(plan, at, mask) for mask in range(1, 1 << len(plan.seq))] + [sq.Y, sq.C, sq.X]
    for peer in peers:
        pl.semaphore_signal(barrier, inc=1, device_id=peer, device_id_type=MESH)
    pl.semaphore_wait(barrier, len(peers))


def column_of(rows, start, sign, rate):
    offset = lax.broadcasted_iota(jnp.int32, (rows, 1), 0).astype(F32)
    return jnp.exp((start + sign * offset) * rate)


def decay_mask(mask, rate):
    rows = mask.shape[0]

    @pl.loop(0, rows // 128)
    def _(i):
        start = pl.multiple_of(i * 128, 128)
        line = lax.broadcasted_iota(jnp.int32, (128, rows), 0) + start
        lane = lax.broadcasted_iota(jnp.int32, (128, rows), 1)
        distance = (line - lane).astype(F32)
        mask[pl.ds(start, 128), :] = jnp.where(distance >= 0, jnp.exp(jnp.maximum(distance, 0.0) * rate), 0.0)


TILE = 256


def row_tiles(full, body):
    rows = full.shape[1]
    each = rows // TILE

    @pl.loop(0, 2 * each)
    def _(i):
        body(i // each, pl.multiple_of(i % each * TILE, TILE), pl.multiple_of(i * TILE, TILE))


def turned(r, slot, start):
    base = r.turn[slot]
    cos_at, sin_at = base[0:1], base[1:2]
    cos_off, sin_off = r.cos_off[pl.ds(start, TILE), :], r.sin_off[pl.ds(start, TILE), :]
    return cos_at * cos_off - sin_at * sin_off, sin_at * cos_off + cos_at * sin_off


def front_kernel(plan, names, *refs):
    r = types.SimpleNamespace(**dict(zip(names, refs)))
    at = {axis: lax.axis_index(axis) for axis in plan.seq + plan.head}
    sq = Square(plan.pair)
    length, model = r.inputs.shape
    width = r.block.shape[1]
    mine = sq.y * 2 + sq.c
    column = pl.multiple_of(mine * width, width)
    rate = r.rate[0:1, 0:1]
    weights = [r.wq, r.wk, r.wv, r.wg, r.wo, r.wu, r.wd]
    key_size, value_size = r.wq.shape[1], r.wv.shape[1]
    saved = []

    def save(source, target):
        copy = pltpu.make_async_copy(source, target, r.save_sem.at[len(saved)])
        copy.start()
        saved.append(copy)

    greet_all(plan, at, sq)
    bulk = Bulk(plan, at, [r.sq, r.sk, r.sv, r.sg, r.so, r.su, r.sd], weights, r.bulk_send, r.bulk_receive, r.bulk_local)
    QUERY, KEY, VALUE, GATE, OUT, UP, DOWN = range(7)
    pair, high, low = [bulk.axes[0]], bulk.high, bulk.low

    size = 1 << len(plan.seq)
    copies = []
    for mask in range(1, size):
        copy = remote(r.vec, r.vecs.at[bulk.me], r.vec_send, r.vec_receive, mask, flipped(plan, at, mask))
        copy.start()
        copies.append(copy)
    r.vecs[bulk.me] = r.vec[...]
    bulk.begin(QUERY, bulk.axes)
    bulk.begin(KEY, bulk.axes)
    for unit in (VALUE, GATE, OUT):
        bulk.begin(unit, low)

    for copy in copies:
        copy.wait_recv()
    step = r.vec.shape[1]
    for j in range(size):
        r.all_gains[:, j * step : (j + 1) * step] = r.vecs[j]
    r.gains[...] = r.all_gains[:, pl.ds(column, width)]

    @pl.loop(0, length // 128)
    def _(i):
        rows = pl.ds(pl.multiple_of(i * 128, 128), 128)
        stream = r.inputs[rows, :]
        mean = jnp.mean(stream, axis=1, keepdims=True)
        inverse = lax.rsqrt(jnp.mean(jnp.square(stream - mean), axis=1, keepdims=True) + EPSILON)
        r.inverse_one[rows, :] = jnp.broadcast_to(inverse, (128, 128))
        normed = (stream - mean) * inverse
        hidden = (normed * r.all_gains[0:1, :] + r.all_gains[1:2, :]).astype(BF)
        r.hidden[sq.p, rows, :] = hidden
        own = (r.inputs[rows, pl.ds(column, width)] - mean) * inverse
        r.normed_one[rows, :] = own
        r.block[rows, :] = (own * r.gains[0:1, :] + r.gains[1:2, :]).astype(BF)

    gains = r.gains[...]
    hid = pass_steps(sq, r.block, r.hidden, r.hid_send, r.hid_receive, 0, False)
    cot = pass_steps(sq, r.cot, r.cot_out, r.cot_send, r.cot_receive, 0, True)
    keep_cot = pltpu.make_async_copy(r.cot, r.cot_out.at[sq.p, :, pl.ds(column, width)], r.local_sem.at[0])
    keep_cot.start()
    next(hid)
    bulk.begin(VALUE, pair + high)
    bulk.paired(QUERY)
    bulk.paired(KEY)
    bulk.first(QUERY)
    bulk.first(KEY)
    bulk.begin(GATE, pair + high)
    bulk.begin(OUT, pair + high)
    next(hid)
    bulk.second(QUERY)
    bulk.second(KEY)
    bulk.paired(VALUE)
    decay_mask(r.mask, rate)
    bulk.first(VALUE)
    next(hid)
    next(hid, None)
    bulk.paired(GATE)
    bulk.paired(OUT)
    bulk.first(GATE)
    bulk.first(OUT)
    bulk.second(VALUE)
    save(r.hidden, r.hidden_out)

    bulk.finish(QUERY)
    bulk.finish(KEY)
    save(r.wq, r.wq_out)
    save(r.wk, r.wk_out)

    def project_keys(slot, start, row):
        hidden = r.hidden[slot, pl.ds(start, TILE), :]
        cosine, sine = turned(r, slot, start)
        for weight, target in ((r.wq, r.q), (r.wk, r.k)):
            value = mm(hidden, weight[...])
            target[pl.ds(row, TILE), :] = rotate(value, cosine, sine).astype(BF)

    row_tiles(r.hidden, project_keys)

    bulk.begin(UP, pair)
    bulk.begin(DOWN, pair)
    bulk.finish(VALUE)
    bulk.second(GATE)
    bulk.second(OUT)
    save(r.wv, r.wv_out)

    def project_values(slot, start, row):
        r.v[pl.ds(row, TILE), :] = mm(r.hidden[slot, pl.ds(start, TILE), :], r.wv[...]).astype(BF)

    row_tiles(r.hidden, project_values)
    save(r.q, r.q_out)
    save(r.k, r.k_out)
    save(r.v, r.v_out)
    weight_out = column_of(length, float(length), -1.0, rate)
    for slot in range(2):
        rows = slice(slot * length, (slot + 1) * length)
        key = (r.k[rows, :].astype(F32) * weight_out).astype(BF)
        r.state[slot] = t_mm(key, r.v[rows, :])
    carry = carried(
        plan, at, r.state, r.reach, r.low_buf, r.high_buf, rate, length, False, r.carry_send, r.carry_receive, 0
    )
    next(carry)

    def inner(slot, start, row):
        scores = mm_t(r.q[pl.ds(row, TILE), :], r.k[pl.ds(pl.multiple_of(slot * length, length), length), :])
        weights_ = (scores * r.mask[pl.ds(start, TILE), :]).astype(BF)
        r.normed[pl.ds(row, TILE), :] = mm(weights_, r.v[pl.ds(pl.multiple_of(slot * length, length), length), :])

    row_tiles(r.hidden, inner)
    bulk.begin(UP, high + low)
    next(carry, None)
    bulk.begin(DOWN, low)
    bulk.finish(GATE)
    save(r.wg, r.wg_out)

    def gates(slot, start, row):
        r.gate[pl.ds(row, TILE), :] = mm(r.hidden[slot, pl.ds(start, TILE), :], r.wg[...])

    row_tiles(r.hidden, gates)
    save(r.gate, r.gate_out)
    bulk.paired(UP, low)
    bulk.paired(DOWN, low)
    for _ in carry:
        pass
    for slot in range(2):
        r.reach_bf[slot] = r.reach[slot].astype(BF)
    save(r.reach_bf, r.reach_out)

    def outer(slot, start, row):
        rows = pl.ds(row, TILE)
        offset = lax.broadcasted_iota(jnp.int32, (TILE, 1), 0) + start
        cross = mm(r.q[rows, :], r.reach_bf[slot]) * jnp.exp(offset.astype(F32) * rate)
        retained = r.normed[rows, :] + cross
        center = retained - jnp.mean(retained, axis=1, keepdims=True)
        inverse = lax.rsqrt(jnp.mean(center * center, axis=1, keepdims=True) + EPSILON)
        value = center * inverse
        r.normed[rows, :] = value
        r.inverse[rows, :] = jnp.broadcast_to(inverse, (TILE, 128))
        gate = r.gate[rows, :]
        r.gated[rows, :] = (gate * jax.nn.sigmoid(gate) * value).astype(BF)

    row_tiles(r.hidden, outer)
    save(r.normed, r.normed_out)
    save(r.inverse, r.inverse_out)
    save(r.gated, r.gated_out)
    bulk.finish(OUT)
    save(r.wo, r.wo_out)

    def out_block(p_, y_, c_):
        rows = pl.ds(pl.multiple_of(p_ * length, length), length)
        return mm_t(r.gated[rows, :], r.wo[pl.ds(pl.multiple_of((y_ * 2 + c_) * width, width), width), :])

    def nothing():
        pass

    def rest_of_up():
        bulk.forward(UP, bulk.bit[pair[0]], high)
        bulk.begin(DOWN, high)

    def rest_of_down():
        bulk.forward(DOWN, bulk.bit[pair[0]], high)
        next(cot)
        bulk.first(UP)

    def second_up():
        bulk.second(UP)
        bulk.first(DOWN)

    reduce = reduce_steps(
        sq, out_block, r.middle, r.hand, r.near, r.total, r.arrived, r.sends, r.receives, SPREAD_COPIES
    )
    together(reduce, nothing, rest_of_up)
    whole = r.middle[...] + r.inputs[:, pl.ds(column, width)]
    r.middle[...] = whole
    mean = jnp.mean(whole, axis=1, keepdims=True)
    deviation = jnp.mean(jnp.square(whole - mean), axis=1, keepdims=True)
    base = SPREAD_COPIES + REDUCE_COPIES
    means, spreads = exchange(sq, mean, deviation, r.stats, r.sends, r.receives, base)
    center = sum(means) * (1.0 / len(means))
    variance = sum(s + jnp.square(m - center) for m, s in zip(means, spreads)) * (1.0 / len(means))
    mean, scale = upright(center, lax.rsqrt(variance + EPSILON))
    r.inverse_two[...] = jnp.broadcast_to(scale, r.inverse_two.shape)
    value = (r.middle[...] - mean) * scale
    r.normed_two[...] = value
    r.block[...] = (value * gains[2:3] + gains[3:4]).astype(BF)
    spread = spread_steps(sq, r.block, r.mid_out, r.sends, r.receives, 0, r.local_sem.at[1])
    together(spread, nothing, rest_of_down, second_up)
    bulk.finish(UP)
    save(r.wu, r.wu_out)
    next(cot)
    bulk.second(DOWN)
    next(cot)
    next(cot, None)
    bulk.finish(DOWN)
    save(r.wd, r.wd_out)
    bulk.drain()
    keep_cot.wait()
    for copy in copies:
        copy.wait_send()
    for copy in saved:
        copy.wait()


def front(plan, shards, inputs, cot, vec, rate, turn, cos_off, sin_off, number):
    length, model = inputs.shape
    width = cot.shape[1]
    size = 1 << len(plan.seq)
    key_size, value_size, hidden = shards[0].shape[1] // 2, shards[2].shape[1] // 2, shards[5].shape[1] // 2
    any_spec, vmem_spec = pl.BlockSpec(memory_space=pl.ANY), pl.BlockSpec(memory_space=pltpu.VMEM)
    both = 2 * length

    def shape(dims, kind=BF):
        return jax.ShapeDtypeStruct(dims, kind)

    ins = [(n, a, any_spec) for n, a in zip(("sq", "sk", "sv", "sg", "so", "su", "sd"), shards)]
    ins += [
        (n, a, vmem_spec)
        for n, a in (
            ("inputs", inputs),
            ("cot", cot),
            ("vec", vec),
            ("rate", rate),
            ("turn", turn),
            ("cos_off", cos_off),
            ("sin_off", sin_off),
        )
    ]
    whole = [(model, s.shape[1] // 2) for s in shards]
    outs = [(f"w{n}_out", shape(d), any_spec) for n, d in zip("qkvgoud", whole)]
    outs += [
        ("hidden_out", shape((2, length, model)), any_spec),
        ("cot_out", shape((2, length, model)), any_spec),
        ("mid_out", shape((2, length, model)), any_spec),
        ("q_out", shape((both, key_size)), any_spec),
        ("k_out", shape((both, key_size)), any_spec),
        ("v_out", shape((both, value_size)), any_spec),
        ("reach_out", shape((2, key_size, value_size)), any_spec),
        ("gate_out", shape((both, value_size), F32), any_spec),
        ("normed_out", shape((both, value_size), F32), any_spec),
        ("inverse_out", shape((both, 128), F32), any_spec),
        ("gated_out", shape((both, value_size)), any_spec),
        ("middle", shape((length, width), F32), vmem_spec),
        ("normed_one", shape((length, width), F32), vmem_spec),
        ("inverse_one", shape((length, 128), F32), vmem_spec),
        ("normed_two", shape((length, width), F32), vmem_spec),
        ("inverse_two", shape((length, 128), F32), vmem_spec),
        ("gains", shape((8, width), F32), vmem_spec),
    ]
    carries = carry_buffers(plan, key_size, value_size)
    count = SPREAD_COPIES + REDUCE_COPIES + 3
    dma = pltpu.SemaphoreType.DMA
    scratch = [(f"w{n}", pltpu.VMEM(d, BF)) for n, d in zip("qkvgoud", whole)]
    scratch += [
        ("hidden", pltpu.VMEM((2, length, model), BF)),
        ("block", pltpu.VMEM((length, width), BF)),
        ("q", pltpu.VMEM((both, key_size), BF)),
        ("k", pltpu.VMEM((both, key_size), BF)),
        ("v", pltpu.VMEM((both, value_size), BF)),
        ("gate", pltpu.VMEM((both, value_size), F32)),
        ("normed", pltpu.VMEM((both, value_size), F32)),
        ("inverse", pltpu.VMEM((both, 128), F32)),
        ("gated", pltpu.VMEM((both, value_size), BF)),
        ("mask", pltpu.VMEM((length, length), F32)),
        ("state", carries[0]),
        ("reach", carries[1]),
        ("low_buf", carries[2]),
        ("high_buf", carries[3]),
        ("reach_bf", pltpu.VMEM((2, key_size, value_size), BF)),
        ("vecs", pltpu.VMEM((size,) + vec.shape, F32)),
        ("stats", pltpu.VMEM((4, 8, length), F32)),
        *zip(("hand", "near", "total", "arrived"), reduce_room(length, width)),
        ("bulk_send", dma((7 * size,))),
        ("bulk_receive", dma((7 * size,))),
        ("bulk_local", dma((7,))),
        ("vec_send", dma((size,))),
        ("vec_receive", dma((size,))),
        ("carry_send", dma((len(plan.seq),))),
        ("carry_receive", dma((len(plan.seq),))),
        ("all_gains", pltpu.VMEM((8, model), F32)),
        ("hid_send", dma((PASS_COPIES,))),
        ("hid_receive", dma((PASS_COPIES,))),
        ("cot_send", dma((PASS_COPIES,))),
        ("cot_receive", dma((PASS_COPIES,))),
        ("sends", dma((count,))),
        ("receives", dma((count,))),
        ("local_sem", dma((3,))),
        ("save_sem", dma((32,))),
    ]
    names = [n for n, *_ in ins] + [n for n, *_ in outs] + [n for n, _ in scratch]
    results = pl.pallas_call(
        functools.partial(front_kernel, plan, names),
        out_shape=tuple(s for _, s, _ in outs),
        in_specs=[s for *_, s in ins],
        out_specs=tuple(s for *_, s in outs),
        scratch_shapes=[s for _, s in scratch],
        compiler_params=pltpu.CompilerParams(
            collective_id=number, has_side_effects=True, vmem_limit_bytes=VMEM_LIMIT
        ),
        name="front",
    )(*[a for _, a, _ in ins])
    return types.SimpleNamespace(**dict(zip([n for n, *_ in outs], results)))


def rotate(values, cosine, sine):
    half = values.shape[1] // 2
    first, second = values[:, :half], values[:, half:]
    return jnp.concatenate([first * cosine - second * sine, first * sine + second * cosine], axis=1)


def unrotate(values, cosine, sine):
    half = values.shape[1] // 2
    first, second = values[:, :half], values[:, half:]
    return jnp.concatenate([first * cosine + second * sine, second * cosine - first * sine], axis=1)


def carry(plan, local, lograte, length, reverse):
    state = list(local)
    reach = [jnp.zeros_like(s) for s in local]
    blocks = jnp.float32(length)

    def decay(count):
        return jnp.exp(count * blocks * lograte)

    low_index = jnp.float32(0)
    span = 1.0
    for axis in plan.low:
        bit = lax.axis_index(axis)
        late = (bit == 1) != reverse
        got = swap(jnp.stack([s.astype(BF) for s in state]), axis).astype(F32)
        between = low_index if not reverse else span - 1.0 - low_index
        for slot in range(2):
            reach[slot] = reach[slot] + jnp.where(late, decay(between), 0.0) * got[slot]
            before = jnp.where(late, got[slot], state[slot])
            after = jnp.where(late, state[slot], got[slot])
            state[slot] = before * decay(span) + after
        low_index = low_index + bit.astype(F32) * span
        span *= 2.0
    between = low_index if not reverse else span - 1.0 - low_index
    early, later = (1, 0) if reverse else (0, 1)
    reach[later] = reach[later] + decay(between) * state[early]
    total = state[early] * decay(span) + state[later]
    index = [low_index, low_index + span]
    span *= 2.0
    for axis in plan.high:
        bit = lax.axis_index(axis)
        late = (bit == 1) != reverse
        got = swap(total.astype(BF), axis).astype(F32)
        for slot in range(2):
            between = index[slot] if not reverse else span - 1.0 - index[slot]
            reach[slot] = reach[slot] + jnp.where(late, decay(between), 0.0) * got
            index[slot] = index[slot] + bit.astype(F32) * span
        before = jnp.where(late, got, total)
        after = jnp.where(late, total, got)
        total = before * decay(span) + after
        span *= 2.0
    return reach


def on_device(
    plan,
    inputs,
    decay_exponent,
    first_gain,
    first_bias,
    query_weight,
    key_weight,
    value_weight,
    gate_weight,
    out_weight,
    second_gain,
    second_bias,
    up_weight,
    down_weight,
    cotangent,
):
    length, model = inputs.shape
    rows = query_weight.shape[0]
    pair_bit = lax.axis_index(plan.pair)
    column = lax.axis_index(plan.head_axes)
    width = cotangent.shape[1]

    def halves(weight):
        return jnp.stack(jnp.split(weight, 2, axis=1))

    key_size = query_weight.shape[1] // 2
    value_size = value_weight.shape[1] // 2
    hidden = up_weight.shape[1] // 2

    vec = jnp.stack([first_gain, first_bias, second_gain, second_bias] * 2).astype(F32)

    exponent = pick(decay_exponent, pair_bit, 0).astype(F32)
    lograte = jnp.log1p(-jnp.exp2(-exponent))
    offset = jnp.arange(length, dtype=F32)
    seq_index = lax.axis_index(plan.seq_axes)
    pair_weight = 2 ** plan.seq.index(plan.pair)
    first_slot = seq_index - pair_bit * pair_weight
    starts = jnp.stack([first_slot, first_slot + pair_weight]) * length
    frequency = np.exp(-math.log(10000.0) * np.arange(key_size // 2, dtype=np.float32) / (key_size // 2 - 1))
    frequency = frequency.astype(np.float32)
    angles = np.arange(length)[:, None] * frequency.astype(np.float64)[None, :]
    cos_off, sin_off = jnp.asarray(np.cos(angles), F32), jnp.asarray(np.sin(angles), F32)
    start_angles = starts.astype(F32)[:, None] * frequency[None, :]
    turn = jnp.stack([jnp.cos(start_angles), jnp.sin(start_angles)] * 4, axis=1)
    shards = [query_weight, key_weight, value_weight, gate_weight, out_weight.T, up_weight, down_weight.T]
    rate = jnp.full((8, 128), lograte, F32)
    f = front(plan, shards, inputs, cotangent.astype(BF), vec, rate, turn, cos_off, sin_off, 1)
    full = (2 * length, model)
    cosine = (turn[:, 0:1] * cos_off - turn[:, 1:2] * sin_off).reshape(2 * length, -1)
    sine = (turn[:, 1:2] * cos_off + turn[:, 0:1] * sin_off).reshape(2 * length, -1)
    distance = offset[:, None] - offset[None, :]
    mask = jnp.where(distance >= 0, jnp.exp(jnp.maximum(distance, 0.0) * lograte), 0.0)
    weight_in = jnp.exp(offset * lograte)[:, None]
    weight_out = jnp.exp((length - offset) * lograte)[:, None]
    weight_in_back = jnp.exp((length - 1.0 - offset) * lograte)[:, None]
    weight_out_back = jnp.exp((offset + 1.0) * lograte)[:, None]

    slots = [slice(0, length), slice(length, 2 * length)]
    hidden_in, cot_bf, hidden_mid = f.hidden_out.reshape(full), f.cot_out.reshape(full), f.mid_out.reshape(full)
    qkv_full = jnp.concatenate([f.wq_out, f.wk_out, f.wv_out], axis=1)
    gate_full, out_full, up_full, down_full = f.wg_out, f.wo_out, f.wu_out, f.wd_out
    queries, keys, values, incoming = f.q_out, f.k_out, f.v_out, f.reach_out
    gate_act, group_normed, group_inverse, gated = f.gate_out, f.normed_out, f.inverse_out[:, :1], f.gated_out
    middle, normed_one, normed_two = f.middle, f.normed_one, f.normed_two
    inverse_one, inverse_two = f.inverse_one[:, :1], f.inverse_two[:, :1]
    gain_one, gain_two = f.gains[0], f.gains[2]
    logistic = jax.nn.sigmoid(gate_act)
    swish = gate_act * logistic

    preact = mm(hidden_mid, up_full)
    cdf = 0.5 * (1.0 + lax.erf(preact * 0.7071067811865476))
    slope = cdf + preact * (jnp.exp(-0.5 * preact * preact) * 0.3989422804014327)
    hidden_ff = (preact * cdf).astype(BF)
    layer_out = middle + scatter_block(plan, mm_t(hidden_ff, down_full), 4)

    grad_down = t_mm(cot_bf, hidden_ff)
    grad_preact = (mm(cot_bf, down_full) * slope).astype(BF)
    grad_up = t_mm(hidden_mid, grad_preact)
    grad_three = scatter_rows(plan, jnp.concatenate([grad_up, grad_down], axis=1), rows)
    grad_middle, sums_two, grad_mid_bf = middle_norm(
        plan, mm_t(grad_preact, up_full), cotangent, gain_two, normed_two, inverse_two, 5
    )
    grad_out = t_mm(grad_mid_bf, gated)
    grad_gated = mm(grad_mid_bf, out_full)
    grad_gates = (grad_gated * group_normed * (logistic + swish * (1.0 - logistic))).astype(BF)
    scaled = grad_gated * swish
    grad_mixed = (
        group_inverse
        * (
            scaled
            - jnp.mean(scaled, axis=1, keepdims=True)
            - group_normed * jnp.mean(scaled * group_normed, axis=1, keepdims=True)
        )
    ).astype(BF)
    grad_gate = t_mm(hidden_in, grad_gates)
    grad_two = scatter_rows(plan, jnp.concatenate([grad_gate, grad_out], axis=1), rows)

    back_local = [t_mm((queries[s].astype(F32) * weight_out_back).astype(BF), grad_mixed[s]) for s in slots]
    outgoing = [r.astype(BF) for r in carry(plan, back_local, lograte, length, True)]
    grad_query, grad_key, grad_value = [], [], []
    for s, state, back in zip(slots, incoming, outgoing):
        weights = (mm_t(grad_mixed[s], values[s]) * mask).astype(BF)
        grad_query.append(mm(weights, keys[s]) + mm_t(grad_mixed[s], state) * weight_in)
        grad_key.append(t_mm(weights, queries[s]) + mm_t(values[s], back) * weight_in_back)
        forward = (mm_t(queries[s], keys[s]) * mask).astype(BF)
        grad_value.append(t_mm(forward, grad_mixed[s]) + mm(keys[s], back) * weight_in_back)
    grad_query = unrotate(jnp.concatenate(grad_query), cosine, sine).astype(BF)
    grad_key = unrotate(jnp.concatenate(grad_key), cosine, sine).astype(BF)
    grad_value = jnp.concatenate(grad_value).astype(BF)
    grad_qkv = jnp.concatenate([grad_query, grad_key, grad_value], axis=1)
    grad_one = scatter_rows(plan, t_mm(hidden_in, grad_qkv), rows)
    partial_in = mm_t(grad_qkv, qkv_full) + mm_t(grad_gates, gate_full)
    grad_inputs, sums_one = last_norm(plan, partial_in, grad_middle, gain_one, normed_one, inverse_one, 6)

    sums = jnp.concatenate([sums_one, sums_two])
    placed = lax.dynamic_update_slice_in_dim(jnp.zeros((4, model), F32), sums, column * width, 1)
    placed = lax.psum(placed, plan.seq_axes + plan.head_axes)
    mine = lax.dynamic_slice_in_dim(placed, seq_index * rows, rows, 1)

    def joined(grad, start, size):
        piece = lax.slice_in_dim(grad, start, start + size, axis=2)
        return jnp.concatenate([piece[0], piece[1]], axis=1)

    return (
        layer_out,
        grad_inputs,
        mine[0],
        mine[1],
        joined(grad_one, 0, key_size),
        joined(grad_one, key_size, key_size),
        joined(grad_one, 2 * key_size, value_size),
        joined(grad_two, 0, value_size),
        joined(grad_two, value_size, value_size).T,
        mine[2],
        mine[3],
        joined(grad_three, 0, hidden),
        joined(grad_three, hidden, hidden).T,
    )


def solution(mesh):
    seq_bits = (mesh.shape["seq"]).bit_length() - 1
    head_bits = (mesh.shape["head"]).bit_length() - 1
    plan = Plan(seq_bits, head_bits)
    seq, head = plan.seq_axes, plan.head_axes
    fine = Mesh(mesh.devices.reshape((2,) * (seq_bits + head_bits)), seq + head)
    in_specs = (
        P(seq, None),
        P(head),
        P(seq),
        P(seq),
        P(seq, head),
        P(seq, head),
        P(seq, head),
        P(seq, head),
        P(head, seq),
        P(seq),
        P(seq),
        P(seq, head),
        P(head, seq),
        P(seq, head),
    )
    out_specs = (
        P(seq, head),
        P(seq, head),
        P(seq),
        P(seq),
        P(seq, head),
        P(seq, head),
        P(seq, head),
        P(seq, head),
        P(head, seq),
        P(seq),
        P(seq),
        P(seq, head),
        P(head, seq),
    )

    def step(*args):
        return on_device(plan, *args)

    return jax.shard_map(step, mesh=fine, in_specs=in_specs, out_specs=out_specs, check_vma=False)
```

```python
import functools
import math
import types

import jax
import jax.numpy as jnp
import numpy as np
from jax import lax
from jax.experimental import pallas as pl
from jax.experimental.pallas import tpu as pltpu
from jax.sharding import Mesh, PartitionSpec as P

EPSILON = 1e-05
BF = jnp.bfloat16
F32 = jnp.float32
MESH = pl.DeviceIdType.MESH
VMEM_LIMIT = 67043328

def pick(array, index, axis):
    return lax.dynamic_index_in_dim(array, index, axis, keepdims=False)


def dot(left, right, contract):
    return lax.dot_general(left, right, (contract, ((), ())), preferred_element_type=F32)


def mm(left, right):
    return dot(left, right, ((1,), (0,)))


def mm_t(left, right):
    return dot(left, right, ((1,), (1,)))


def t_mm(left, right):
    return dot(left, right, ((0,), (0,)))


class Plan:
    def __init__(self, seq_bits, head_bits):
        self.seq = [f"s{i}" for i in range(seq_bits)]
        self.head = [f"h{i}" for i in range(head_bits)]
        self.names = tuple(reversed(self.seq)) + ()
        self.seq_axes = tuple(reversed(self.seq))
        self.head_axes = tuple(reversed(self.head))
        self.pair = "s1" if seq_bits > 1 else "s0"
        self.low = [a for a in self.seq if a < self.pair]
        self.high = [a for a in self.seq if a > self.pair]


class Square:
    def __init__(self, pair):
        self.pair = pair
        self.p = lax.axis_index(pair)
        self.y = lax.axis_index("h1")
        self.c = lax.axis_index("h0")
        self.S = {pair: 1 - self.p}
        self.Y = {"h1": 1 - self.y}
        self.C = {"h0": 1 - self.c}
        self.X = {"h1": 1 - self.y, "h0": 1 - self.c}

    def greet(self, cross=True):
        barrier = pltpu.get_barrier_semaphore()
        peers = [self.S, self.Y, self.C] + ([self.X] if cross else [])
        for peer in peers:
            pl.semaphore_signal(barrier, inc=1, device_id=peer, device_id_type=MESH)
        pl.semaphore_wait(barrier, len(peers))


def remote(source, target, sends, receives, index, device):
    return pltpu.make_async_remote_copy(
        src_ref=source,
        dst_ref=target,
        send_sem=sends.at[index],
        recv_sem=receives.at[index],
        device_id=device,
        device_id_type=MESH,
    )


SPREAD_COPIES = 13
REDUCE_COPIES = 10


def exchange(sq, first, second, stats, sends, receives, base):
    rows = first.shape[0]
    lane = lax.broadcasted_iota(jnp.int32, (rows, 128), 1)
    packed = jnp.where(lane == 0, first, second).T
    mine = sq.y * 2 + sq.c
    stats[mine] = packed[:8]
    copies = []
    for index, device in enumerate((sq.Y, sq.C, sq.X)):
        copy = remote(stats.at[mine], stats.at[mine], sends, receives, base + index, device)
        copy.start()
        copies.append(copy)
    for copy in copies:
        copy.wait_recv()
    for copy in copies:
        copy.wait_send()
    return [stats[q][0:1] for q in range(4)], [stats[q][1:2] for q in range(4)]


def upright(first, second):
    rows = first.shape[1]
    line = lax.broadcasted_iota(jnp.int32, (128, rows), 0)
    turned = jnp.where(line == 0, first, second).T
    return turned[:, 0:1], turned[:, 1:2]


class Bulk:
    def __init__(self, plan, at, shards, wholes, sends, receives, local_sem):
        self.shards, self.wholes, self.at = shards, wholes, at
        self.sends, self.receives, self.local_sem = sends, receives, local_sem
        self.axes = [plan.pair] + plan.high + plan.low
        self.high, self.low, self.lows = plan.high, plan.low, len(plan.low)
        self.bit = {axis: 1 << plan.seq.index(axis) for axis in self.axes}
        self.me = sum(at[axis] * self.bit[axis] for axis in self.axes)
        self.size = 1 << len(self.axes)
        self.copies, self.kept, self.passed = [], {}, set()

    def piece(self, unit, mask):
        rows = self.shards[unit].shape[0]
        return self.wholes[unit].at[pl.ds(pl.multiple_of((self.me ^ mask) * rows, rows), rows), :]

    def half(self, unit, which):
        width = self.wholes[unit].shape[1]
        return self.shards[unit].at[:, pl.ds(pl.multiple_of(which * width, width), width)]

    def link(self, unit, source, held, axis):
        return remote(
            source,
            self.piece(unit, held),
            self.sends,
            self.receives,
            unit * self.size + (held | self.bit[axis]),
            {axis: 1 - self.at[axis]},
        )

    def send(self, unit, source, held, axis):
        copy = self.link(unit, source, held, axis)
        copy.start()
        self.copies.append(copy)

    def begin(self, unit, axes):
        own = self.at[self.axes[0]]
        for axis in axes:
            self.send(unit, self.half(unit, 1 - own if axis == self.axes[0] else own), 0, axis)
        if self.axes[0] in axes:
            keep = pltpu.make_async_copy(self.half(unit, own), self.piece(unit, 0), self.local_sem.at[unit])
            keep.start()
            self.kept[unit] = keep

    def held_before(self, stage):
        held = [0]
        for axis in self.axes[:stage]:
            held = held + [m | self.bit[axis] for m in held]
        return held

    def forward(self, unit, mask, axes):
        for later in axes:
            self.send(unit, self.piece(unit, mask), mask, later)

    def arrive(self, unit, stage, masks, axes=None):
        axis = self.axes[stage]
        for held in self.held_before(stage):
            mask = held | self.bit[axis]
            if not masks(mask):
                continue
            pltpu.make_async_remote_copy(
                src_ref=self.piece(unit, mask),
                dst_ref=self.piece(unit, mask),
                send_sem=self.sends.at[unit * self.size + mask],
                recv_sem=self.receives.at[unit * self.size + mask],
                device_id={axis: 1 - self.at[axis]},
                device_id_type=MESH,
            ).wait_recv()
            self.forward(unit, mask, self.axes[stage + 1 :] if axes is None else axes)

    def paired(self, unit, axes=None):
        self.arrive(unit, 0, lambda mask: True, axes)

    def first(self, unit):
        for stage in range(1, len(self.axes) - self.lows):
            self.arrive(unit, stage, lambda mask: not mask & self.bit[self.axes[0]])

    def second(self, unit):
        for stage in range(1, len(self.axes) - self.lows):
            self.arrive(unit, stage, lambda mask: mask & self.bit[self.axes[0]])

    def finish(self, unit):
        for stage in range(len(self.axes) - self.lows, len(self.axes)):
            self.arrive(unit, stage, lambda mask: True)
        self.kept[unit].wait()

    def drain(self):
        for copy in self.copies:
            copy.wait_send()


def together(process, *hooks):
    for number, _ in enumerate(process):
        if number < len(hooks):
            hooks[number]()


def carried(plan, at, state, reach, low_buf, high_buf, rate, length, reverse, sends, receives, base):
    index = base
    low_index = jnp.float32(0)
    span = 1.0
    copies = []

    def decay(count):
        return jnp.exp(rate * (count * float(length)))

    for slot in range(2):
        reach[slot] = jnp.zeros(reach.shape[1:], F32)
    for number, axis in enumerate(plan.low):
        bit = at[axis].astype(F32)
        late = 1.0 - bit if reverse else bit
        for slot in range(2):
            low_buf[2 * number, slot] = state[slot].astype(BF)
        copy = remote(low_buf.at[2 * number], low_buf.at[2 * number + 1], sends, receives, index, {axis: 1 - at[axis]})
        copy.start()
        copies.append(copy)
        index += 1
        yield
        copy.wait_recv()
        between = span - 1.0 - low_index if reverse else low_index
        step_decay = decay(span)
        take, keep = late * step_decay + (1.0 - late), late + (1.0 - late) * step_decay
        for slot in range(2):
            got = low_buf[2 * number + 1, slot].astype(F32)
            reach[slot] += got * (late * decay(between))
            state[slot] = got * take + state[slot] * keep
        low_index = low_index + bit * span
        span *= 2.0
    between = span - 1.0 - low_index if reverse else low_index
    early, later = (1, 0) if reverse else (0, 1)
    reach[later] += state[early] * decay(between)
    state[0] = state[early] * decay(span) + state[later]
    order = [low_index, low_index + span]
    span *= 2.0
    for number, axis in enumerate(plan.high):
        bit = at[axis].astype(F32)
        late = 1.0 - bit if reverse else bit
        high_buf[2 * number] = state[0].astype(BF)
        copy = remote(high_buf.at[2 * number], high_buf.at[2 * number + 1], sends, receives, index, {axis: 1 - at[axis]})
        copy.start()
        copies.append(copy)
        index += 1
        yield
        copy.wait_recv()
        step_decay = decay(span)
        take, keep = late * step_decay + (1.0 - late), late + (1.0 - late) * step_decay
        got = high_buf[2 * number + 1].astype(F32)
        for slot in range(2):
            between = span - 1.0 - order[slot] if reverse else order[slot]
            reach[slot] += got * (late * decay(between))
            order[slot] = order[slot] + bit * span
        state[0] = got * take + state[0] * keep
        span *= 2.0
    for copy in copies:
        copy.wait_send()


def carry_buffers(plan, key_size, value_size):
    return [
        pltpu.VMEM((2, key_size, value_size), F32),
        pltpu.VMEM((2, key_size, value_size), F32),
        pltpu.VMEM((2 * max(len(plan.low), 1), 2, key_size, value_size), BF),
        pltpu.VMEM((2 * max(len(plan.high), 1), key_size, value_size), BF),
    ]


def spread_steps(sq, block, full, sends, receives, base, local_sem):
    rows, width = block.shape
    half = rows // 2
    p, y, c = sq.p, sq.y, sq.c
    top, low = (0, half), (half, half)

    def place(p_, y_, c_, start, count):
        return full.at[p_, pl.ds(start, count), pl.ds(pl.multiple_of((y_ * 2 + c_) * width, width), width)]

    def own(part):
        return block.at[pl.ds(part[0], part[1]), :]

    def send(index, source, target, device):
        copy = remote(source, target, sends, receives, base + index, device)
        copy.start()
        return copy

    def relay(index, p_, y_, part, device):
        return send(index, place(p_, y_, c, *part), place(p_, y_, c, *part), device)

    k0 = send(0, own(top), place(p, y, c, *top), sq.S)
    k2 = send(2, own(low), place(p, y, c, *low), sq.Y)
    k6 = send(6, block, place(p, y, c, 0, rows), sq.C)
    k1 = send(1, own(low), place(p, y, c, *low), sq.S)
    k3 = send(3, own(top), place(p, y, c, *top), sq.Y)
    keep = pltpu.make_async_copy(block, place(p, y, c, 0, rows), local_sem)
    keep.start()
    yield
    k2.wait_recv()
    k4 = relay(4, p, 1 - y, low, sq.S)
    k9 = relay(9, p, 1 - y, low, sq.C)
    k0.wait_recv()
    k5 = relay(5, 1 - p, y, top, sq.Y)
    k7 = relay(7, 1 - p, y, top, sq.C)
    yield
    k1.wait_recv()
    k8 = relay(8, 1 - p, y, low, sq.C)
    k3.wait_recv()
    k10 = relay(10, p, 1 - y, top, sq.C)
    yield
    k5.wait_recv()
    k11 = relay(11, 1 - p, 1 - y, top, sq.C)
    k4.wait_recv()
    k12 = relay(12, 1 - p, 1 - y, low, sq.C)
    for copy in (k6, k7, k8, k9, k10, k11, k12):
        copy.wait_recv()
    for copy in (k0, k1, k2, k3, k4, k5, k6, k7, k8, k9, k10, k11, k12):
        copy.wait_send()
    keep.wait()


def pass_steps(sq, block, full, sends, receives, base, wide):
    rows = full.shape[1]
    width = full.shape[2] // 4
    half = rows // 2
    p, y, c = sq.p, sq.y, sq.c
    parts = ((0, half), (half, half))
    copies = []

    def place(p_, y_, part):
        columns = pl.ds(pl.multiple_of((y_ * 2 + c) * width, width), width)
        return full.at[p_, pl.ds(part[0], part[1]), columns]

    def send(index, source, p_, y_, part, device):
        copy = remote(source, place(p_, y_, part), sends, receives, base + index, device)
        copy.start()
        copies.append(copy)
        return copy

    def own(part):
        return block.at[pl.ds(part[0], part[1]), :]

    far = [send(i, own(part), p, y, part, sq.S) for i, part in enumerate(parts)]
    beside, near = [], []
    if wide:
        beside += [send(2 + i, own(part), p, y, part, sq.Y) for i, part in enumerate(parts)]
        near += [send(4 + i, own(part), p, y, part, sq.C) for i, part in enumerate(parts)]
    yield
    other = []
    for i, part in enumerate(parts):
        far[i].wait_recv()
        other.append(send(6 + i, place(1 - p, y, part), 1 - p, y, part, sq.Y))
        near.append(send(8 + i, place(1 - p, y, part), 1 - p, y, part, sq.C))
    yield
    for i, part in enumerate(parts):
        if wide:
            beside[i].wait_recv()
            near.append(send(10 + i, place(p, 1 - y, part), p, 1 - y, part, sq.C))
        other[i].wait_recv()
        near.append(send(12 + i, place(1 - p, 1 - y, part), 1 - p, 1 - y, part, sq.C))
    yield
    for copy in near:
        copy.wait_recv()
    for copy in copies:
        copy.wait_send()


PASS_COPIES = 14


def reduce_steps(sq, block_of, result, hand, near, total, arrived, sends, receives, base):
    rows, width = result.shape
    half = rows // 2
    p, y, c = sq.p, sq.y, sq.c
    top, low = pl.ds(0, half), pl.ds(half, half)

    def send(index, source, target, device):
        copy = remote(source, target, sends, receives, base + index, device)
        copy.start()
        return copy

    order = ((1 - p, 1 - y), (1 - p, y), (p, 1 - y), (p, y))
    given = []
    for i, (p_, y_) in enumerate(order):
        hand[p_, y_] = block_of(p_, y_, 1 - c).astype(BF)
        given.append(send(i, hand.at[p_, y_], near.at[p_, y_], sq.C))

    def join(i):
        p_, y_ = order[i]
        own = block_of(p_, y_, c)
        given[i].wait_recv()
        return own + near[p_, y_].astype(F32)

    total[1 - p, 1 - y] = join(0).astype(BF)
    a = send(4, total.at[1 - p, 1 - y, low], arrived.at[0], sq.S)
    b = send(5, total.at[1 - p, 1 - y, top], arrived.at[1], sq.Y)
    total[1 - p, y] = join(1).astype(BF)
    e = send(6, total.at[1 - p, y, low], arrived.at[2], sq.S)
    total[p, 1 - y] = join(2).astype(BF)
    f = send(7, total.at[p, 1 - y, top], arrived.at[3], sq.Y)
    result[...] = join(3)
    yield
    b.wait_recv()
    total[1 - p, y, top] = (total[1 - p, y, top].astype(F32) + arrived[1].astype(F32)).astype(BF)
    g = send(8, total.at[1 - p, y, top], arrived.at[4], sq.S)
    a.wait_recv()
    total[p, 1 - y, low] = (total[p, 1 - y, low].astype(F32) + arrived[0].astype(F32)).astype(BF)
    d = send(9, total.at[p, 1 - y, low], arrived.at[5], sq.Y)
    yield
    e.wait_recv()
    f.wait_recv()
    g.wait_recv()
    result[top, :] += arrived[4].astype(F32) + arrived[3].astype(F32)
    d.wait_recv()
    result[low, :] += arrived[2].astype(F32) + arrived[5].astype(F32)
    for copy in given + [a, b, e, f, g, d]:
        copy.wait_send()


def reduce_room(rows, width):
    return [pltpu.VMEM((2, 2, rows, width), BF)] * 3 + [pltpu.VMEM((6, rows // 2, width), BF)]


def flipped(plan, at, mask):
    return {axis: 1 - at[axis] for i, axis in enumerate(plan.seq) if mask >> i & 1}


def greet_all(plan, at, sq):
    barrier = pltpu.get_barrier_semaphore()
    peers = [flipped(plan, at, mask) for mask in range(1, 1 << len(plan.seq))] + [sq.Y, sq.C, sq.X]
    for peer in peers:
        pl.semaphore_signal(barrier, inc=1, device_id=peer, device_id_type=MESH)
    pl.semaphore_wait(barrier, len(peers))


def column_of(rows, start, sign, rate):
    offset = lax.broadcasted_iota(jnp.int32, (rows, 1), 0).astype(F32)
    return jnp.exp((start + sign * offset) * rate)


def decay_mask(mask, rate):
    rows = mask.shape[0]

    @pl.loop(0, rows // 128)
    def _(i):
        start = pl.multiple_of(i * 128, 128)
        line = lax.broadcasted_iota(jnp.int32, (128, rows), 0) + start
        lane = lax.broadcasted_iota(jnp.int32, (128, rows), 1)
        distance = (line - lane).astype(F32)
        mask[pl.ds(start, 128), :] = jnp.where(distance >= 0, jnp.exp(jnp.maximum(distance, 0.0) * rate), 0.0)


TILE = 256


def row_tiles(full, body):
    rows = full.shape[1]
    each = rows // TILE

    @pl.loop(0, 2 * each)
    def _(i):
        body(i // each, pl.multiple_of(i % each * TILE, TILE), pl.multiple_of(i * TILE, TILE))


def turned(r, slot, start):
    base = r.turn[slot]
    cos_at, sin_at = base[0:1], base[1:2]
    cos_off, sin_off = r.cos_off[pl.ds(start, TILE), :], r.sin_off[pl.ds(start, TILE), :]
    return cos_at * cos_off - sin_at * sin_off, sin_at * cos_off + cos_at * sin_off


def front_kernel(plan, names, *refs):
    r = types.SimpleNamespace(**dict(zip(names, refs)))
    at = {axis: lax.axis_index(axis) for axis in plan.seq + plan.head}
    sq = Square(plan.pair)
    length, model = r.inputs.shape
    width = r.block.shape[1]
    mine = sq.y * 2 + sq.c
    column = pl.multiple_of(mine * width, width)
    rate = r.rate[0:1, 0:1]
    weights = [r.wq, r.wk, r.wv, r.wg, r.wo, r.wu, r.wd]
    key_size, value_size = r.wq.shape[1], r.wv.shape[1]
    saved = []

    def save(source, target):
        copy = pltpu.make_async_copy(source, target, r.save_sem.at[len(saved)])
        copy.start()
        saved.append(copy)

    greet_all(plan, at, sq)
    bulk = Bulk(plan, at, [r.sq, r.sk, r.sv, r.sg, r.so, r.su, r.sd], weights, r.bulk_send, r.bulk_receive, r.bulk_local)
    QUERY, KEY, VALUE, GATE, OUT, UP, DOWN = range(7)
    pair, high, low = [bulk.axes[0]], bulk.high, bulk.low

    size = 1 << len(plan.seq)
    copies = []
    for mask in range(1, size):
        copy = remote(r.vec, r.vecs.at[bulk.me], r.vec_send, r.vec_receive, mask, flipped(plan, at, mask))
        copy.start()
        copies.append(copy)
    r.vecs[bulk.me] = r.vec[...]
    bulk.begin(QUERY, bulk.axes)
    bulk.begin(KEY, bulk.axes)
    for unit in (VALUE, GATE, OUT):
        bulk.begin(unit, low)

    for copy in copies:
        copy.wait_recv()
    step = r.vec.shape[1]
    for j in range(size):
        r.all_gains[:, j * step : (j + 1) * step] = r.vecs[j]
    r.gains[...] = r.all_gains[:, pl.ds(column, width)]

    @pl.loop(0, length // 128)
    def _(i):
        rows = pl.ds(pl.multiple_of(i * 128, 128), 128)
        stream = r.inputs[rows, :]
        mean = jnp.mean(stream, axis=1, keepdims=True)
        inverse = lax.rsqrt(jnp.mean(jnp.square(stream - mean), axis=1, keepdims=True) + EPSILON)
        r.inverse_one[rows, :] = jnp.broadcast_to(inverse, (128, 128))
        normed = (stream - mean) * inverse
        hidden = (normed * r.all_gains[0:1, :] + r.all_gains[1:2, :]).astype(BF)
        r.hidden[sq.p, rows, :] = hidden
        own = (r.inputs[rows, pl.ds(column, width)] - mean) * inverse
        r.normed_one[rows, :] = own
        r.block[rows, :] = (own * r.gains[0:1, :] + r.gains[1:2, :]).astype(BF)

    gains = r.gains[...]
    hid = pass_steps(sq, r.block, r.hidden, r.hid_send, r.hid_receive, 0, False)
    cot = pass_steps(sq, r.cot, r.cot_out, r.cot_send, r.cot_receive, 0, True)
    keep_cot = pltpu.make_async_copy(r.cot, r.cot_out.at[sq.p, :, pl.ds(column, width)], r.local_sem.at[0])
    keep_cot.start()
    next(hid)
    bulk.begin(VALUE, pair + high)
    bulk.paired(QUERY)
    bulk.paired(KEY)
    bulk.first(QUERY)
    bulk.first(KEY)
    bulk.begin(GATE, pair + high)
    bulk.begin(OUT, pair + high)
    next(hid)
    bulk.second(QUERY)
    bulk.second(KEY)
    bulk.paired(VALUE)
    decay_mask(r.mask, rate)
    bulk.first(VALUE)
    next(hid)
    next(hid, None)
    bulk.paired(GATE)
    bulk.paired(OUT)
    bulk.first(GATE)
    bulk.first(OUT)
    bulk.second(VALUE)
    save(r.hidden, r.hidden_out)

    bulk.finish(QUERY)
    bulk.finish(KEY)
    save(r.wq, r.wq_out)
    save(r.wk, r.wk_out)

    def project_keys(slot, start, row):
        hidden = r.hidden[slot, pl.ds(start, TILE), :]
        cosine, sine = turned(r, slot, start)
        for weight, target in ((r.wq, r.q), (r.wk, r.k)):
            value = mm(hidden, weight[...])
            target[pl.ds(row, TILE), :] = rotate(value, cosine, sine).astype(BF)

    row_tiles(r.hidden, project_keys)

    bulk.begin(UP, pair)
    bulk.begin(DOWN, pair)
    bulk.finish(VALUE)
    bulk.second(GATE)
    bulk.second(OUT)
    save(r.wv, r.wv_out)

    def project_values(slot, start, row):
        r.v[pl.ds(row, TILE), :] = mm(r.hidden[slot, pl.ds(start, TILE), :], r.wv[...]).astype(BF)

    row_tiles(r.hidden, project_values)
    save(r.q, r.q_out)
    save(r.k, r.k_out)
    save(r.v, r.v_out)
    weight_out = column_of(length, float(length), -1.0, rate)
    for slot in range(2):
        rows = slice(slot * length, (slot + 1) * length)
        key = (r.k[rows, :].astype(F32) * weight_out).astype(BF)
        r.state[slot] = t_mm(key, r.v[rows, :])
    carry = carried(
        plan, at, r.state, r.reach, r.low_buf, r.high_buf, rate, length, False, r.carry_send, r.carry_receive, 0
    )
    next(carry)

    def inner(slot, start, row):
        scores = mm_t(r.q[pl.ds(row, TILE), :], r.k[pl.ds(pl.multiple_of(slot * length, length), length), :])
        weights_ = (scores * r.mask[pl.ds(start, TILE), :]).astype(BF)
        r.normed[pl.ds(row, TILE), :] = mm(weights_, r.v[pl.ds(pl.multiple_of(slot * length, length), length), :])

    row_tiles(r.hidden, inner)
    bulk.begin(UP, high + low)
    next(carry, None)
    bulk.begin(DOWN, low)
    bulk.finish(GATE)
    save(r.wg, r.wg_out)

    def gates(slot, start, row):
        r.gate[pl.ds(row, TILE), :] = mm(r.hidden[slot, pl.ds(start, TILE), :], r.wg[...])

    row_tiles(r.hidden, gates)
    save(r.gate, r.gate_out)
    bulk.paired(UP, low)
    bulk.paired(DOWN, low)
    for _ in carry:
        pass
    for slot in range(2):
        r.reach_bf[slot] = r.reach[slot].astype(BF)
    save(r.reach_bf, r.reach_out)

    def outer(slot, start, row):
        rows = pl.ds(row, TILE)
        offset = lax.broadcasted_iota(jnp.int32, (TILE, 1), 0) + start
        cross = mm(r.q[rows, :], r.reach_bf[slot]) * jnp.exp(offset.astype(F32) * rate)
        retained = r.normed[rows, :] + cross
        center = retained - jnp.mean(retained, axis=1, keepdims=True)
        inverse = lax.rsqrt(jnp.mean(center * center, axis=1, keepdims=True) + EPSILON)
        value = center * inverse
        r.normed[rows, :] = value
        r.inverse[rows, :] = jnp.broadcast_to(inverse, (TILE, 128))
        gate = r.gate[rows, :]
        r.gated[rows, :] = (gate * jax.nn.sigmoid(gate) * value).astype(BF)

    row_tiles(r.hidden, outer)
    save(r.normed, r.normed_out)
    save(r.inverse, r.inverse_out)
    save(r.gated, r.gated_out)
    bulk.finish(OUT)
    save(r.wo, r.wo_out)

    def out_block(p_, y_, c_):
        rows = pl.ds(pl.multiple_of(p_ * length, length), length)
        return mm_t(r.gated[rows, :], r.wo[pl.ds(pl.multiple_of((y_ * 2 + c_) * width, width), width), :])

    def nothing():
        pass

    def rest_of_up():
        bulk.forward(UP, bulk.bit[pair[0]], high)
        bulk.begin(DOWN, high)

    def rest_of_down():
        bulk.forward(DOWN, bulk.bit[pair[0]], high)
        next(cot)
        bulk.first(UP)

    def second_up():
        bulk.second(UP)
        bulk.first(DOWN)

    reduce = reduce_steps(
        sq, out_block, r.middle, r.hand, r.near, r.total, r.arrived, r.sends, r.receives, SPREAD_COPIES
    )
    together(reduce, nothing, rest_of_up)
    whole = r.middle[...] + r.inputs[:, pl.ds(column, width)]
    r.middle[...] = whole
    mean = jnp.mean(whole, axis=1, keepdims=True)
    deviation = jnp.mean(jnp.square(whole - mean), axis=1, keepdims=True)
    base = SPREAD_COPIES + REDUCE_COPIES
    means, spreads = exchange(sq, mean, deviation, r.stats, r.sends, r.receives, base)
    center = sum(means) * (1.0 / len(means))
    variance = sum(s + jnp.square(m - center) for m, s in zip(means, spreads)) * (1.0 / len(means))
    mean, scale = upright(center, lax.rsqrt(variance + EPSILON))
    r.inverse_two[...] = jnp.broadcast_to(scale, r.inverse_two.shape)
    value = (r.middle[...] - mean) * scale
    r.normed_two[...] = value
    r.block[...] = (value * gains[2:3] + gains[3:4]).astype(BF)
    spread = spread_steps(sq, r.block, r.mid_out, r.sends, r.receives, 0, r.local_sem.at[1])
    together(spread, nothing, rest_of_down, second_up)
    bulk.finish(UP)
    save(r.wu, r.wu_out)
    next(cot)
    bulk.second(DOWN)
    next(cot)
    next(cot, None)
    bulk.finish(DOWN)
    save(r.wd, r.wd_out)
    bulk.drain()
    keep_cot.wait()
    for copy in copies:
        copy.wait_send()
    for copy in saved:
        copy.wait()


def front(plan, shards, inputs, cot, vec, rate, turn, cos_off, sin_off, number):
    length, model = inputs.shape
    width = cot.shape[1]
    size = 1 << len(plan.seq)
    key_size, value_size, hidden = shards[0].shape[1] // 2, shards[2].shape[1] // 2, shards[5].shape[1] // 2
    any_spec, vmem_spec = pl.BlockSpec(memory_space=pl.ANY), pl.BlockSpec(memory_space=pltpu.VMEM)
    both = 2 * length

    def shape(dims, kind=BF):
        return jax.ShapeDtypeStruct(dims, kind)

    ins = [(n, a, any_spec) for n, a in zip(("sq", "sk", "sv", "sg", "so", "su", "sd"), shards)]
    ins += [
        (n, a, vmem_spec)
        for n, a in (
            ("inputs", inputs),
            ("cot", cot),
            ("vec", vec),
            ("rate", rate),
            ("turn", turn),
            ("cos_off", cos_off),
            ("sin_off", sin_off),
        )
    ]
    whole = [(model, s.shape[1] // 2) for s in shards]
    outs = [(f"w{n}_out", shape(d), any_spec) for n, d in zip("qkvgoud", whole)]
    outs += [
        ("hidden_out", shape((2, length, model)), any_spec),
        ("cot_out", shape((2, length, model)), any_spec),
        ("mid_out", shape((2, length, model)), any_spec),
        ("q_out", shape((both, key_size)), any_spec),
        ("k_out", shape((both, key_size)), any_spec),
        ("v_out", shape((both, value_size)), any_spec),
        ("reach_out", shape((2, key_size, value_size)), any_spec),
        ("gate_out", shape((both, value_size), F32), any_spec),
        ("normed_out", shape((both, value_size), F32), any_spec),
        ("inverse_out", shape((both, 128), F32), any_spec),
        ("gated_out", shape((both, value_size)), any_spec),
        ("middle", shape((length, width), F32), vmem_spec),
        ("normed_one", shape((length, width), F32), vmem_spec),
        ("inverse_one", shape((length, 128), F32), vmem_spec),
        ("normed_two", shape((length, width), F32), vmem_spec),
        ("inverse_two", shape((length, 128), F32), vmem_spec),
        ("gains", shape((8, width), F32), vmem_spec),
    ]
    carries = carry_buffers(plan, key_size, value_size)
    count = SPREAD_COPIES + REDUCE_COPIES + 3
    dma = pltpu.SemaphoreType.DMA
    scratch = [(f"w{n}", pltpu.VMEM(d, BF)) for n, d in zip("qkvgoud", whole)]
    scratch += [
        ("hidden", pltpu.VMEM((2, length, model), BF)),
        ("block", pltpu.VMEM((length, width), BF)),
        ("q", pltpu.VMEM((both, key_size), BF)),
        ("k", pltpu.VMEM((both, key_size), BF)),
        ("v", pltpu.VMEM((both, value_size), BF)),
        ("gate", pltpu.VMEM((both, value_size), F32)),
        ("normed", pltpu.VMEM((both, value_size), F32)),
        ("inverse", pltpu.VMEM((both, 128), F32)),
        ("gated", pltpu.VMEM((both, value_size), BF)),
        ("mask", pltpu.VMEM((length, length), F32)),
        ("state", carries[0]),
        ("reach", carries[1]),
        ("low_buf", carries[2]),
        ("high_buf", carries[3]),
        ("reach_bf", pltpu.VMEM((2, key_size, value_size), BF)),
        ("vecs", pltpu.VMEM((size,) + vec.shape, F32)),
        ("stats", pltpu.VMEM((4, 8, length), F32)),
        *zip(("hand", "near", "total", "arrived"), reduce_room(length, width)),
        ("bulk_send", dma((7 * size,))),
        ("bulk_receive", dma((7 * size,))),
        ("bulk_local", dma((7,))),
        ("vec_send", dma((size,))),
        ("vec_receive", dma((size,))),
        ("carry_send", dma((len(plan.seq),))),
        ("carry_receive", dma((len(plan.seq),))),
        ("all_gains", pltpu.VMEM((8, model), F32)),
        ("hid_send", dma((PASS_COPIES,))),
        ("hid_receive", dma((PASS_COPIES,))),
        ("cot_send", dma((PASS_COPIES,))),
        ("cot_receive", dma((PASS_COPIES,))),
        ("sends", dma((count,))),
        ("receives", dma((count,))),
        ("local_sem", dma((3,))),
        ("save_sem", dma((32,))),
    ]
    names = [n for n, *_ in ins] + [n for n, *_ in outs] + [n for n, _ in scratch]
    results = pl.pallas_call(
        functools.partial(front_kernel, plan, names),
        out_shape=tuple(s for _, s, _ in outs),
        in_specs=[s for *_, s in ins],
        out_specs=tuple(s for *_, s in outs),
        scratch_shapes=[s for _, s in scratch],
        compiler_params=pltpu.CompilerParams(
            collective_id=number, has_side_effects=True, vmem_limit_bytes=VMEM_LIMIT
        ),
        name="front",
    )(*[a for _, a, _ in ins])
    return types.SimpleNamespace(**dict(zip([n for n, *_ in outs], results)))


class Return:
    def __init__(self, plan, at, totals, got, sends, receives):
        self.at, self.totals, self.got = at, totals, got
        self.sends, self.receives = sends, receives
        self.order = plan.low + list(reversed(plan.high)) + [plan.pair]
        self.bit = {axis: 1 << i for i, axis in enumerate(plan.seq)}
        self.size = 1 << len(plan.seq)
        self.me = sum(at[axis] * self.bit[axis] for axis in self.order)
        self.copies = {}

    def stage_of(self, mask):
        for stage, axis in enumerate(self.order):
            if mask & self.bit[axis]:
                return stage
        return len(self.order)

    def masks(self, stage):
        found = [m for m in range(1, self.size) if self.stage_of(m) == stage]
        return sorted(found, key=lambda m: (self.stage_of(m ^ self.bit[self.order[stage]]), m))

    def link(self, unit, mask):
        axis = self.order[self.stage_of(mask)]
        return remote(
            self.total(unit, mask),
            self.got.at[unit, mask - 1],
            self.sends,
            self.receives,
            unit * self.size + mask,
            {axis: 1 - self.at[axis]},
        )

    def total(self, unit, mask):
        rows = self.got.shape[2]
        return self.totals.at[unit % self.totals.shape[0], pl.ds(mask * rows, rows), :]

    def send(self, unit, mask):
        copy = self.link(unit, mask)
        copy.start()
        self.copies[unit, mask] = copy

    def put(self, unit, mask, value):
        self.total(unit, mask)[...] = value.astype(BF)
        if self.stage_of(mask) == 0:
            self.send(unit, mask)

    def collect(self, unit, stage):
        axis = self.order[stage]
        for mask in self.masks(stage):
            target = mask ^ self.bit[axis]
            self.link(unit, mask).wait_recv()
            total = self.total(unit, target)
            total[...] = (total[...].astype(F32) + self.got[unit, mask - 1].astype(F32)).astype(BF)
            if self.stage_of(target) == stage + 1 and target:
                self.send(unit, target)

    def halves(self, unit):
        last = self.bit[self.order[-1]]
        self.link(unit, last).wait_recv()
        return self.total(unit, 0)[...].astype(F32), self.got[unit, last - 1].astype(F32)

    def clear(self, unit):
        for (number, _), copy in self.copies.items():
            if number == unit:
                copy.wait_send()


def back_kernel(plan, names, *refs):
    r = types.SimpleNamespace(**dict(zip(names, refs)))
    at = {axis: lax.axis_index(axis) for axis in plan.seq + plan.head}
    sq = Square(plan.pair)
    length, width = r.cot.shape
    key_size, value_size = r.q.shape[1], r.v.shape[1]
    outs_of = [[r.gu], [r.gd], [r.go], [r.gg], [r.gv], [r.gq, r.gk]]
    mine = sq.y * 2 + sq.c
    rate = r.rate[0:1, 0:1]
    UP, DOWN, OUT, GATE, VALUE, KEYS = range(6)
    back = Return(plan, at, r.totals, r.got, r.bulk_send, r.bulk_receive)
    piece, model = r.got.shape[2], r.mid.shape[2]
    strip = r.strips.shape[2]
    per_strip = strip // piece

    loads = {}

    def load(name, source, target):
        copy = pltpu.make_async_copy(source, target, r.load_sem.at[len(loads)])
        copy.start()
        loads[name] = copy

    def ready(*wanted):
        for name in wanted:
            loads[name].wait()

    greet_all(plan, at, sq)
    load("wu", r.wu, r.weights.at[0])
    load("wd", r.wd, r.weights.at[1])

    parts = model // value_size

    def tile_copy(source, i):
        each = length // TILE
        rows = source.at[i // each, pl.ds(i % each * TILE, TILE), :]
        return [pltpu.make_async_copy(rows, r.tiles.at[i % 2], r.tile_sem.at[i % 2, 0])]

    def cot_tile(i, part):
        return r.totals.at[r.totals.shape[0] - 1, pl.ds((i % 2 * parts + part) * TILE, TILE), :]

    def cot_copy(i):
        each = length // TILE
        return [
            pltpu.make_async_copy(
                r.cotf.at[i // each, pl.ds(i % each * TILE, TILE), pl.ds(part * value_size, value_size)],
                cot_tile(i, part),
                r.tile_sem.at[i % 2, 1 + part],
            )
            for part in range(parts)
        ]

    def start(copies):
        for copy in copies:
            copy.start()

    def wait(copies):
        for copy in copies:
            copy.wait()

    tile_count = 2 * length // TILE
    start(tile_copy(r.mid, 0) + cot_copy(0))
    load("wo", r.wo, r.weights.at[2])
    load("gated", r.gated_in, r.gated)
    load("gate", r.gate_in, r.gate)
    load("normed", r.normed_in, r.normed)
    load("inverse", r.inverse_in, r.inverse)
    load("q", r.q_in, r.q)
    load("k", r.k_in, r.k)
    load("v", r.v_in, r.v)
    load("reach", r.reach_in, r.in_bf)
    load("middle", r.middle_in, r.layer_out)
    ready("wu", "wd")

    for i in range(tile_count):
        if i + 1 < tile_count:
            start(tile_copy(r.mid, i + 1) + cot_copy(i + 1))
        wait(tile_copy(r.mid, i) + cot_copy(i))
        rows = slice(i * TILE, (i + 1) * TILE)
        preact = mm(r.tiles[i % 2], r.weights[0])
        cdf = 0.5 * (1.0 + lax.erf(preact * 0.7071067811865476))
        slope = cdf + preact * (jnp.exp(-0.5 * preact * preact) * 0.3989422804014327)
        r.hidden_ff[rows, :] = (preact * cdf).astype(BF)
        grad = sum(
            mm(cot_tile(i, part)[...], r.weights[1, part * value_size : (part + 1) * value_size, :])
            for part in range(parts)
        )
        r.grad_pre[rows, :] = (grad * slope).astype(BF)

    def strip_copy(source, mask, number):
        start = pl.multiple_of((back.me ^ mask) // per_strip * strip, strip)
        half = r.strips.at[number % 2]
        return [
            pltpu.make_async_copy(
                source.at[slot, :, pl.ds(start, strip)],
                half.at[pl.ds(slot * length, length), :],
                r.strip_sem.at[number % 2, slot],
            )
            for slot in range(2)
        ]

    def produce(unit, source, grads, masks):
        for copy in strip_copy(source, masks[0], 0):
            copy.start()
        for number, mask in enumerate(masks):
            if number + 1 < len(masks):
                for copy in strip_copy(source, masks[number + 1], number + 1):
                    copy.start()
            for copy in strip_copy(source, mask, number):
                copy.wait()
            value = t_mm(r.strips[number % 2], grads[...])
            if per_strip > 1:
                r.whole_strip[...] = value
                inside = pl.multiple_of((back.me ^ mask) % per_strip * piece, piece)
                value = r.whole_strip[pl.ds(inside, piece), :]
            back.put(unit, mask, value)

    away = back.masks(0)
    home = [m for m in range(back.size) if m not in away]

    def blocks(grads, weight):
        def block_of(p_, y_, c_):
            rows = pl.ds(pl.multiple_of(p_ * length, length), length)
            columns = pl.ds(pl.multiple_of((y_ * 2 + c_) * width, width), width)
            return sum(mm_t(g[rows, :], r.weights[w, columns, :]) for g, w in zip(grads, weight))

        return block_of

    def reduce(grads, weight, result, base):
        return reduce_steps(
            sq, blocks(grads, weight), result, r.hand, r.near, r.near, r.arrived, r.sends, r.receives, base
        )

    emitted = []

    def emit(unit):
        own = at[plan.pair]
        for half, value in zip((own, 1 - own), back.halves(unit)):
            outs = outs_of[unit]
            cut = value.shape[1] // len(outs)
            for i, out in enumerate(outs):
                slot = len(emitted) % 2
                if len(emitted) >= 2:
                    emitted[-2].wait()
                part = value[:, i * cut : (i + 1) * cut]
                if out.shape[0] != piece:
                    stage = r.stage_t.at[slot, pl.ds(0, cut), :]
                    stage[...] = part.T
                    target = out.at[pl.ds(pl.multiple_of(half * cut, cut), cut), :]
                else:
                    stage = r.stage.at[slot, :, pl.ds(0, cut)]
                    stage[...] = part
                    target = out.at[:, pl.ds(pl.multiple_of(half * cut, cut), cut)]
                copy = pltpu.make_async_copy(stage, target, r.emit_sem.at[slot])
                copy.start()
                emitted.append(copy)

    def norm_sums(upstream, gain, normed, inverse, base_stream, result, row, stats, base):
        value = upstream[...]
        product = value * normed[...]
        r.sums[row : row + 1, :] = jnp.sum(product, axis=0, keepdims=True)
        r.sums[row + 1 : row + 2, :] = jnp.sum(value, axis=0, keepdims=True)
        first = jnp.mean(value * gain, axis=1, keepdims=True)
        second = jnp.mean(product * gain, axis=1, keepdims=True)
        firsts, seconds = exchange(sq, first, second, stats, r.sends, r.receives, base)
        share = 1.0 / len(firsts)
        first, second = upright(sum(firsts) * share, sum(seconds) * share)
        result[...] = base_stream[...] + inverse[:, 0:1] * (upstream[...] * gain - first - normed[...] * second)

    base = SPREAD_COPIES
    together(
        reduce([r.grad_pre], [0], r.upstream, base),
        lambda: produce(DOWN, r.cotf, r.hidden_ff, away),
        lambda: produce(DOWN, r.cotf, r.hidden_ff, home),
    )
    base += REDUCE_COPIES
    load("wv", r.wv, r.weights.at[0])
    norm_sums(r.upstream, r.gains[2:3, :], r.normed_two, r.inverse_two, r.cot, r.grad_middle, 2, r.stats, base)
    base += 3
    r.block[...] = r.grad_middle[...].astype(BF)
    together(
        spread_steps(sq, r.block, r.gmid, r.sends, r.receives, 0, r.local_sem.at[0]),
        lambda: produce(UP, r.mid, r.grad_pre, away),
        lambda: produce(UP, r.mid, r.grad_pre, home),
        lambda: back.collect(DOWN, 0),
    )

    ready("wo", "gated", "gate", "normed", "inverse")
    start(tile_copy(r.gmid, 0))
    for i in range(tile_count):
        if i + 1 < tile_count:
            start(tile_copy(r.gmid, i + 1))
        wait(tile_copy(r.gmid, i))
        rows = slice(i * TILE, (i + 1) * TILE)
        grad = mm(r.tiles[i % 2], r.weights[2])
        gate = r.gate[rows, :]
        normed = r.normed[rows, :]
        logistic = jax.nn.sigmoid(gate)
        swish = gate * logistic
        r.grad_gate[rows, :] = (grad * normed * (logistic + swish * (1.0 - logistic))).astype(BF)
        scaled = grad * swish
        r.grad_mixed[rows, :] = (
            r.inverse[rows, 0:1]
            * (
                scaled
                - jnp.mean(scaled, axis=1, keepdims=True)
                - normed * jnp.mean(scaled * normed, axis=1, keepdims=True)
            )
        ).astype(BF)
    load("wg", r.wg, r.weights.at[2])

    ready("q", "k", "v", "reach")
    decay_mask(r.mask, rate)
    weight_out = column_of(length, 1.0, 1.0, rate)
    for slot in range(2):
        rows = slice(slot * length, (slot + 1) * length)
        query = (r.q[rows, :].astype(F32) * weight_out).astype(BF)
        r.state[slot] = t_mm(query, r.grad_mixed[rows, :])
    carry = carried(
        plan, at, r.state, r.reach, r.low_buf, r.high_buf, rate, length, True, r.carry_send, r.carry_receive, 0
    )
    next(carry)
    produce(OUT, r.gmid, r.gated, away)
    back.collect(UP, 0)
    weight_in = column_of(length, 0.0, 1.0, rate)
    weight_back = column_of(length, length - 1.0, -1.0, rate)

    def rotated_back(value, slot):
        base_ = r.turn[slot]
        cosine = base_[0:1] * r.cos_off[...] - base_[1:2] * r.sin_off[...]
        sine = base_[1:2] * r.cos_off[...] + base_[0:1] * r.sin_off[...]
        return unrotate(value, cosine, sine)

    @pl.loop(0, 2)
    def _(slot):
        rows = pl.ds(pl.multiple_of(slot * length, length), length)
        weights = (mm_t(r.grad_mixed[rows, :], r.v[rows, :]) * r.mask[...]).astype(BF)
        value = mm(weights, r.k[rows, :]) + mm_t(r.grad_mixed[rows, :], r.in_bf[slot]) * weight_in
        r.grad_keys[rows, 0:key_size] = rotated_back(value, slot).astype(BF)
        r.gate[rows, 0:key_size] = t_mm(weights, r.q[rows, :])
        weights = (mm_t(r.q[rows, :], r.k[rows, :]) * r.mask[...]).astype(BF)
        r.normed[rows, :] = t_mm(weights, r.grad_mixed[rows, :])

    next(carry, None)
    back.collect(DOWN, 1)
    produce(OUT, r.gmid, r.gated, home)
    back.collect(UP, 1)
    for _ in carry:
        pass
    for slot in range(2):
        r.out_bf[slot] = r.reach[slot].astype(BF)

    @pl.loop(0, 2)
    def _(slot):
        rows = pl.ds(pl.multiple_of(slot * length, length), length)
        value = r.gate[rows, 0:key_size] + mm_t(r.v[rows, :], r.out_bf[slot]) * weight_back
        r.grad_keys[rows, key_size : 2 * key_size] = rotated_back(value, slot).astype(BF)
        value = r.normed[rows, :] + mm(r.k[rows, :], r.out_bf[slot]) * weight_back
        r.grad_pre[rows, :] = value.astype(BF)

    emit(DOWN)
    back.collect(OUT, 0)
    emit(UP)
    back.clear(UP)
    back.clear(DOWN)
    produce(GATE, r.hid, r.grad_gate, away)
    produce(VALUE, r.hid, r.grad_pre, away)
    produce(GATE, r.hid, r.grad_gate, home)
    back.collect(OUT, 1)
    produce(VALUE, r.hid, r.grad_pre, home)
    emit(OUT)
    back.clear(OUT)
    back.collect(GATE, 0)
    produce(KEYS, r.hid, r.grad_keys, away)
    produce(KEYS, r.hid, r.grad_keys, home)

    ready("middle")
    together(
        reduce([r.hidden_ff], [1], r.upstream, base),
        lambda: back.collect(GATE, 1),
        lambda: back.collect(VALUE, 0),
    )
    base += REDUCE_COPIES
    load("wk", r.wk, r.weights.at[1, :, pl.ds(key_size, key_size)])
    load("wq", r.wq, r.weights.at[1, :, pl.ds(0, key_size)])
    r.layer_out[...] += r.upstream[...]
    peers = (sq.S, sq.Y, sq.C)
    for number, peer in enumerate(peers):
        pl.semaphore_signal(r.again.at[number], inc=1, device_id=peer, device_id_type=MESH)
    for number in range(len(peers)):
        pl.semaphore_wait(r.again.at[number], 1)
    back.collect(KEYS, 0)

    ready("wv", "wg", "wk", "wq")
    together(
        reduce([r.grad_keys, r.grad_pre, r.grad_gate], [1, 0, 2], r.upstream, base),
        lambda: back.collect(VALUE, 1),
        lambda: back.collect(KEYS, 1),
    )
    base += REDUCE_COPIES
    norm_sums(r.upstream, r.gains[0:1, :], r.normed_one, r.inverse_one, r.grad_middle, r.grad_inputs, 0, r.stats_two, base)
    base += 3

    copies = []
    r.all_sums[back.me] = r.sums[...]
    for mask in range(1, back.size):
        copy = remote(r.sums, r.all_sums.at[back.me], r.sum_send, r.sum_receive, mask, flipped(plan, at, mask))
        copy.start()
        copies.append(copy)
    emit(GATE)
    emit(VALUE)
    for copy in copies:
        copy.wait_recv()
    total = r.all_sums[0]
    for i in range(1, back.size):
        total = total + r.all_sums[i]
    r.by_block[mine] = total
    for index, device in enumerate((sq.Y, sq.C, sq.X)):
        copy = remote(r.by_block.at[mine], r.by_block.at[mine], r.sends, r.receives, base + index, device)
        copy.start()
        copies.append(copy)
    for copy in copies[-3:]:
        copy.wait_recv()
    r.sums_out[...] = r.by_block[back.me * piece // width]
    for copy in copies:
        copy.wait_send()
    emit(KEYS)
    for unit in (GATE, VALUE, KEYS):
        back.clear(unit)
    for copy in emitted[-2:]:
        copy.wait()


def back_pass(plan, f, cot, rate, turn, cos_off, sin_off, rows, number):
    length, width = cot.shape
    size = 1 << len(plan.seq)
    model = f.wq_out.shape[0]
    key_size, value_size = f.q_out.shape[1], f.v_out.shape[1]
    hidden = f.wu_out.shape[1]
    both = 2 * length
    any_spec, vmem_spec = pl.BlockSpec(memory_space=pl.ANY), pl.BlockSpec(memory_space=pltpu.VMEM)

    def shape(dims, kind=F32):
        return jax.ShapeDtypeStruct(dims, kind)

    ins = [
        (n, a, any_spec)
        for n, a in (
            ("wq", f.wq_out),
            ("wk", f.wk_out),
            ("wv", f.wv_out),
            ("wg", f.wg_out),
            ("wo", f.wo_out),
            ("wu", f.wu_out),
            ("wd", f.wd_out),
            ("hid", f.hidden_out),
            ("mid", f.mid_out),
            ("cotf", f.cot_out),
            ("q_in", f.q_out),
            ("k_in", f.k_out),
            ("v_in", f.v_out),
            ("reach_in", f.reach_out),
            ("gate_in", f.gate_out),
            ("normed_in", f.normed_out),
            ("inverse_in", f.inverse_out),
            ("gated_in", f.gated_out),
            ("middle_in", f.middle),
        )
    ] + [
        (n, a, vmem_spec)
        for n, a in (
            ("cot", cot),
            ("normed_one", f.normed_one),
            ("inverse_one", f.inverse_one),
            ("normed_two", f.normed_two),
            ("inverse_two", f.inverse_two),
            ("gains", f.gains),
            ("rate", rate),
            ("turn", turn),
            ("cos_off", cos_off),
            ("sin_off", sin_off),
        )
    ]
    turned_out = rows % 128 == 0
    flat = [("gq", key_size), ("gk", key_size), ("gv", value_size), ("gg", value_size), ("gu", hidden)]
    outs = [(n, shape((rows, 2 * c)), any_spec) for n, c in flat]
    outs += [
        (n, shape((2 * c, rows) if turned_out else (rows, 2 * c)), any_spec) for n, c in (("go", value_size), ("gd", hidden))
    ]
    outs += [
        ("gmid", shape((2, length, model), BF), any_spec),
        ("layer_out", shape((length, width)), vmem_spec),
        ("grad_inputs", shape((length, width)), vmem_spec),
        ("sums_out", shape((8, width)), vmem_spec),
    ]
    carries = carry_buffers(plan, key_size, value_size)
    dma = pltpu.SemaphoreType.DMA
    count = SPREAD_COPIES + 3 * REDUCE_COPIES + 9
    strip = max(rows, 128)
    hand, near, _, arrived = reduce_room(length, width)
    scratch = [
        ("weights", pltpu.VMEM((3, model, value_size), BF)),
        ("tiles", pltpu.VMEM((2, TILE, model), BF)),
        ("strips", pltpu.VMEM((2, both, strip), BF)),
        ("q", pltpu.VMEM((both, key_size), BF)),
        ("k", pltpu.VMEM((both, key_size), BF)),
        ("v", pltpu.VMEM((both, value_size), BF)),
        ("gate", pltpu.VMEM((both, value_size), F32)),
        ("normed", pltpu.VMEM((both, value_size), F32)),
        ("inverse", pltpu.VMEM((both, 128), F32)),
        ("gated", pltpu.VMEM((both, value_size), BF)),
        ("in_bf", pltpu.VMEM((2, key_size, value_size), BF)),
        ("out_bf", pltpu.VMEM((2, key_size, value_size), BF)),
        ("mask", pltpu.VMEM((length, length), F32)),
        ("state", carries[0]),
        ("reach", carries[1]),
        ("low_buf", carries[2]),
        ("high_buf", carries[3]),
        ("hidden_ff", pltpu.VMEM((both, hidden), BF)),
        ("grad_pre", pltpu.VMEM((both, hidden), BF)),
        ("grad_gate", pltpu.VMEM((both, value_size), BF)),
        ("grad_mixed", pltpu.VMEM((both, value_size), BF)),
        ("grad_keys", pltpu.VMEM((both, 2 * key_size), BF)),
        ("upstream", pltpu.VMEM((length, width), F32)),
        ("grad_middle", pltpu.VMEM((length, width), F32)),
        ("block", pltpu.VMEM((length, width), BF)),
        ("hand", hand),
        ("near", near),
        ("arrived", arrived),
        ("totals", pltpu.VMEM((3, model, value_size), BF)),
        ("got", pltpu.VMEM((6, size - 1, rows, value_size), BF)),
        ("stats", pltpu.VMEM((4, 8, length), F32)),
        ("stats_two", pltpu.VMEM((4, 8, length), F32)),
        ("sums", pltpu.VMEM((8, width), F32)),
        ("all_sums", pltpu.VMEM((size, 8, width), F32)),
        ("by_block", pltpu.VMEM((4, 8, width), F32)),
        ("stage", pltpu.VMEM((2, rows, value_size), F32)),
        ("stage_t", pltpu.VMEM((2, value_size, rows) if turned_out else (2, 8, 128), F32)),
        ("whole_strip", pltpu.VMEM((strip, value_size) if strip > rows else (8, 128), F32)),
        ("bulk_send", dma((6 * size,))),
        ("bulk_receive", dma((6 * size,))),
        ("load_sem", dma((24,))),
        ("tile_sem", dma((2, 1 + model // value_size))),
        ("strip_sem", dma((2, 2))),
        ("emit_sem", dma((2,))),
        ("carry_send", dma((len(plan.seq),))),
        ("carry_receive", dma((len(plan.seq),))),
        ("sum_send", dma((size,))),
        ("sum_receive", dma((size,))),
        ("sends", dma((count,))),
        ("receives", dma((count,))),
        ("local_sem", dma((1,))),
        ("again", pltpu.SemaphoreType.REGULAR((3,))),
    ]
    names = [n for n, *_ in ins] + [n for n, *_ in outs] + [n for n, _ in scratch]

    def kernel(*refs):
        back_kernel(plan, names, *refs)

    results = pl.pallas_call(
        kernel,
        out_shape=tuple(s for _, s, _ in outs),
        in_specs=[s for *_, s in ins],
        out_specs=tuple(s for *_, s in outs),
        scratch_shapes=[s for _, s in scratch],
        compiler_params=pltpu.CompilerParams(
            collective_id=number, has_side_effects=True, vmem_limit_bytes=VMEM_LIMIT
        ),
        name="back",
    )(*[a for _, a, _ in ins])
    out = types.SimpleNamespace(**dict(zip([n for n, *_ in outs], results)))
    if not turned_out:
        out.go, out.gd = out.go.T, out.gd.T
    return out


def rotate(values, cosine, sine):
    half = values.shape[1] // 2
    first, second = values[:, :half], values[:, half:]
    return jnp.concatenate([first * cosine - second * sine, first * sine + second * cosine], axis=1)


def unrotate(values, cosine, sine):
    half = values.shape[1] // 2
    first, second = values[:, :half], values[:, half:]
    return jnp.concatenate([first * cosine + second * sine, second * cosine - first * sine], axis=1)


def on_device(
    plan,
    inputs,
    decay_exponent,
    first_gain,
    first_bias,
    query_weight,
    key_weight,
    value_weight,
    gate_weight,
    out_weight,
    second_gain,
    second_bias,
    up_weight,
    down_weight,
    cotangent,
):
    length, model = inputs.shape
    rows = query_weight.shape[0]
    pair_bit = lax.axis_index(plan.pair)
    column = lax.axis_index(plan.head_axes)
    width = cotangent.shape[1]

    key_size = query_weight.shape[1] // 2
    value_size = value_weight.shape[1] // 2
    hidden = up_weight.shape[1] // 2

    vec = jnp.stack([first_gain, first_bias, second_gain, second_bias] * 2).astype(F32)

    exponent = pick(decay_exponent, pair_bit, 0).astype(F32)
    lograte = jnp.log1p(-jnp.exp2(-exponent))
    offset = jnp.arange(length, dtype=F32)
    seq_index = lax.axis_index(plan.seq_axes)
    pair_weight = 2 ** plan.seq.index(plan.pair)
    first_slot = seq_index - pair_bit * pair_weight
    starts = jnp.stack([first_slot, first_slot + pair_weight]) * length
    frequency = np.exp(-math.log(10000.0) * np.arange(key_size // 2, dtype=np.float32) / (key_size // 2 - 1))
    frequency = frequency.astype(np.float32)
    angles = np.arange(length)[:, None] * frequency.astype(np.float64)[None, :]
    cos_off, sin_off = jnp.asarray(np.cos(angles), F32), jnp.asarray(np.sin(angles), F32)
    start_angles = starts.astype(F32)[:, None] * frequency[None, :]
    turn = jnp.stack([jnp.cos(start_angles), jnp.sin(start_angles)] * 4, axis=1)
    shards = [query_weight, key_weight, value_weight, gate_weight, out_weight.T, up_weight, down_weight.T]
    rate = jnp.full((8, 128), lograte, F32)
    f = front(plan, shards, inputs, cotangent.astype(BF), vec, rate, turn, cos_off, sin_off, 1)
    b = back_pass(plan, f, cotangent, rate, turn, cos_off, sin_off, rows, 2)
    place = seq_index % (width // rows) * rows
    mine = lax.dynamic_slice_in_dim(b.sums_out, place, rows, 1)
    return (
        b.layer_out,
        b.grad_inputs,
        mine[0],
        mine[1],
        b.gq,
        b.gk,
        b.gv,
        b.gg,
        b.go,
        mine[2],
        mine[3],
        b.gu,
        b.gd,
    )


def solution(mesh):
    seq_bits = (mesh.shape["seq"]).bit_length() - 1
    head_bits = (mesh.shape["head"]).bit_length() - 1
    plan = Plan(seq_bits, head_bits)
    seq, head = plan.seq_axes, plan.head_axes
    fine = Mesh(mesh.devices.reshape((2,) * (seq_bits + head_bits)), seq + head)
    in_specs = (
        P(seq, None),
        P(head),
        P(seq),
        P(seq),
        P(seq, head),
        P(seq, head),
        P(seq, head),
        P(seq, head),
        P(head, seq),
        P(seq),
        P(seq),
        P(seq, head),
        P(head, seq),
        P(seq, head),
    )
    out_specs = (
        P(seq, head),
        P(seq, head),
        P(seq),
        P(seq),
        P(seq, head),
        P(seq, head),
        P(seq, head),
        P(seq, head),
        P(head, seq),
        P(seq),
        P(seq),
        P(seq, head),
        P(head, seq),
    )

    def step(*args):
        return on_device(plan, *args)

    return jax.shard_map(step, mesh=fine, in_specs=in_specs, out_specs=out_specs, check_vma=False)
```

```python
import functools
import math
import types

import jax
import jax.numpy as jnp
import numpy as np
from jax import lax
from jax.experimental import pallas as pl
from jax.experimental.pallas import tpu as pltpu
from jax.sharding import Mesh, PartitionSpec as P

EPSILON = 1e-05
BF = jnp.bfloat16
F32 = jnp.float32
MESH = pl.DeviceIdType.MESH
VMEM_LIMIT = 67043328

def pick(array, index, axis):
    return lax.dynamic_index_in_dim(array, index, axis, keepdims=False)


def dot(left, right, contract):
    return lax.dot_general(left, right, (contract, ((), ())), preferred_element_type=F32)


def mm(left, right):
    return dot(left, right, ((1,), (0,)))


def mm_t(left, right):
    return dot(left, right, ((1,), (1,)))


def t_mm(left, right):
    return dot(left, right, ((0,), (0,)))


class Plan:
    def __init__(self, seq_bits, head_bits):
        self.seq = [f"s{i}" for i in range(seq_bits)]
        self.head = [f"h{i}" for i in range(head_bits)]
        self.names = tuple(reversed(self.seq)) + ()
        self.seq_axes = tuple(reversed(self.seq))
        self.head_axes = tuple(reversed(self.head))
        self.pair = "s1" if seq_bits > 1 else "s0"
        self.low = [a for a in self.seq if a < self.pair]
        self.high = [a for a in self.seq if a > self.pair]


class Square:
    def __init__(self, pair):
        self.pair = pair
        self.p = lax.axis_index(pair)
        self.y = lax.axis_index("h1")
        self.c = lax.axis_index("h0")
        self.S = {pair: 1 - self.p}
        self.Y = {"h1": 1 - self.y}
        self.C = {"h0": 1 - self.c}
        self.X = {"h1": 1 - self.y, "h0": 1 - self.c}

    def greet(self, cross=True):
        barrier = pltpu.get_barrier_semaphore()
        peers = [self.S, self.Y, self.C] + ([self.X] if cross else [])
        for peer in peers:
            pl.semaphore_signal(barrier, inc=1, device_id=peer, device_id_type=MESH)
        pl.semaphore_wait(barrier, len(peers))


def remote(source, target, sends, receives, index, device):
    return pltpu.make_async_remote_copy(
        src_ref=source,
        dst_ref=target,
        send_sem=sends.at[index],
        recv_sem=receives.at[index],
        device_id=device,
        device_id_type=MESH,
    )


def spread(sq, block, full, sends, receives, base, local_sem):
    rows, width = block.shape
    half = rows // 2

    def place(p, y, c, start, count):
        return full.at[p, pl.ds(start, count), pl.ds(pl.multiple_of((y * 2 + c) * width, width), width)]

    p, y, c = sq.p, sq.y, sq.c
    top, low = (0, half), (half, half)

    def own(part):
        return block.at[pl.ds(part[0], part[1]), :]

    def send(index, source, target, device):
        copy = remote(source, target, sends, receives, base + index, device)
        copy.start()
        return copy

    def relay(index, p_, y_, part, device):
        return send(index, place(p_, y_, c, *part), place(p_, y_, c, *part), device)

    k0 = send(0, own(top), place(p, y, c, *top), sq.S)
    k2 = send(2, own(low), place(p, y, c, *low), sq.Y)
    k6 = send(6, block, place(p, y, c, 0, rows), sq.C)
    k1 = send(1, own(low), place(p, y, c, *low), sq.S)
    k3 = send(3, own(top), place(p, y, c, *top), sq.Y)
    keep = pltpu.make_async_copy(block, place(p, y, c, 0, rows), local_sem)
    keep.start()
    k2.wait_recv()
    k4 = relay(4, p, 1 - y, low, sq.S)
    k9 = relay(9, p, 1 - y, low, sq.C)
    k0.wait_recv()
    k5 = relay(5, 1 - p, y, top, sq.Y)
    k7 = relay(7, 1 - p, y, top, sq.C)
    k1.wait_recv()
    k8 = relay(8, 1 - p, y, low, sq.C)
    k3.wait_recv()
    k10 = relay(10, p, 1 - y, top, sq.C)
    k5.wait_recv()
    k11 = relay(11, 1 - p, 1 - y, top, sq.C)
    k4.wait_recv()
    k12 = relay(12, 1 - p, 1 - y, low, sq.C)
    for copy in (k6, k7, k8, k9, k10, k11, k12):
        copy.wait_recv()
    for copy in (k0, k1, k2, k3, k4, k5, k6, k7, k8, k9, k10, k11, k12):
        copy.wait_send()
    keep.wait()


SPREAD_COPIES = 13
REDUCE_COPIES = 10


def exchange(sq, first, second, stats, sends, receives, base):
    rows = first.shape[0]
    lane = lax.broadcasted_iota(jnp.int32, (rows, 128), 1)
    packed = jnp.where(lane == 0, first, second).T
    mine = sq.y * 2 + sq.c
    stats[mine] = packed[:8]
    copies = []
    for index, device in enumerate((sq.Y, sq.C, sq.X)):
        copy = remote(stats.at[mine], stats.at[mine], sends, receives, base + index, device)
        copy.start()
        copies.append(copy)
    for copy in copies:
        copy.wait_recv()
    for copy in copies:
        copy.wait_send()
    return [stats[q][0:1] for q in range(4)], [stats[q][1:2] for q in range(4)]


def upright(first, second):
    rows = first.shape[1]
    line = lax.broadcasted_iota(jnp.int32, (128, rows), 0)
    turned = jnp.where(line == 0, first, second).T
    return turned[:, 0:1], turned[:, 1:2]


class Bulk:
    def __init__(self, plan, at, shards, wholes, sends, receives, local_sem):
        self.shards, self.wholes, self.at = shards, wholes, at
        self.sends, self.receives, self.local_sem = sends, receives, local_sem
        self.axes = [plan.pair] + plan.high + plan.low
        self.high, self.low, self.lows = plan.high, plan.low, len(plan.low)
        self.bit = {axis: 1 << plan.seq.index(axis) for axis in self.axes}
        self.me = sum(at[axis] * self.bit[axis] for axis in self.axes)
        self.size = 1 << len(self.axes)
        self.copies, self.kept, self.passed = [], {}, set()

    def piece(self, unit, mask):
        rows = self.shards[unit].shape[0]
        return self.wholes[unit].at[pl.ds(pl.multiple_of((self.me ^ mask) * rows, rows), rows), :]

    def half(self, unit, which):
        width = self.wholes[unit].shape[1]
        return self.shards[unit].at[:, pl.ds(pl.multiple_of(which * width, width), width)]

    def link(self, unit, source, held, axis):
        return remote(
            source,
            self.piece(unit, held),
            self.sends,
            self.receives,
            unit * self.size + (held | self.bit[axis]),
            {axis: 1 - self.at[axis]},
        )

    def send(self, unit, source, held, axis):
        copy = self.link(unit, source, held, axis)
        copy.start()
        self.copies.append(copy)

    def begin(self, unit, axes):
        own = self.at[self.axes[0]]
        for axis in axes:
            self.send(unit, self.half(unit, 1 - own if axis == self.axes[0] else own), 0, axis)
        if self.axes[0] in axes:
            keep = pltpu.make_async_copy(self.half(unit, own), self.piece(unit, 0), self.local_sem.at[unit])
            keep.start()
            self.kept[unit] = keep

    def held_before(self, stage):
        held = [0]
        for axis in self.axes[:stage]:
            held = held + [m | self.bit[axis] for m in held]
        return held

    def forward(self, unit, mask, axes):
        for later in axes:
            self.send(unit, self.piece(unit, mask), mask, later)

    def arrive(self, unit, stage, masks, axes=None):
        axis = self.axes[stage]
        for held in self.held_before(stage):
            mask = held | self.bit[axis]
            if not masks(mask):
                continue
            pltpu.make_async_remote_copy(
                src_ref=self.piece(unit, mask),
                dst_ref=self.piece(unit, mask),
                send_sem=self.sends.at[unit * self.size + mask],
                recv_sem=self.receives.at[unit * self.size + mask],
                device_id={axis: 1 - self.at[axis]},
                device_id_type=MESH,
            ).wait_recv()
            self.forward(unit, mask, self.axes[stage + 1 :] if axes is None else axes)

    def paired(self, unit, axes=None):
        self.arrive(unit, 0, lambda mask: True, axes)

    def first(self, unit):
        for stage in range(1, len(self.axes) - self.lows):
            self.arrive(unit, stage, lambda mask: not mask & self.bit[self.axes[0]])

    def second(self, unit):
        for stage in range(1, len(self.axes) - self.lows):
            self.arrive(unit, stage, lambda mask: mask & self.bit[self.axes[0]])

    def finish(self, unit):
        for stage in range(len(self.axes) - self.lows, len(self.axes)):
            self.arrive(unit, stage, lambda mask: True)
        self.kept[unit].wait()

    def drain(self):
        for copy in self.copies:
            copy.wait_send()


def together(process, *hooks):
    for number, _ in enumerate(process):
        if number < len(hooks):
            hooks[number]()


def carried(plan, at, state, reach, low_buf, high_buf, rate, length, reverse, sends, receives, base):
    index = base
    low_index = jnp.float32(0)
    span = 1.0
    copies = []

    def decay(count):
        return jnp.exp(rate * (count * float(length)))

    for slot in range(2):
        reach[slot] = jnp.zeros(reach.shape[1:], F32)
    for number, axis in enumerate(plan.low):
        bit = at[axis].astype(F32)
        late = 1.0 - bit if reverse else bit
        for slot in range(2):
            low_buf[2 * number, slot] = state[slot].astype(BF)
        copy = remote(low_buf.at[2 * number], low_buf.at[2 * number + 1], sends, receives, index, {axis: 1 - at[axis]})
        copy.start()
        copies.append(copy)
        index += 1
        yield
        copy.wait_recv()
        between = span - 1.0 - low_index if reverse else low_index
        step_decay = decay(span)
        take, keep = late * step_decay + (1.0 - late), late + (1.0 - late) * step_decay
        for slot in range(2):
            got = low_buf[2 * number + 1, slot].astype(F32)
            reach[slot] += got * (late * decay(between))
            state[slot] = got * take + state[slot] * keep
        low_index = low_index + bit * span
        span *= 2.0
    between = span - 1.0 - low_index if reverse else low_index
    early, later = (1, 0) if reverse else (0, 1)
    reach[later] += state[early] * decay(between)
    state[0] = state[early] * decay(span) + state[later]
    order = [low_index, low_index + span]
    span *= 2.0
    for number, axis in enumerate(plan.high):
        bit = at[axis].astype(F32)
        late = 1.0 - bit if reverse else bit
        high_buf[2 * number] = state[0].astype(BF)
        copy = remote(high_buf.at[2 * number], high_buf.at[2 * number + 1], sends, receives, index, {axis: 1 - at[axis]})
        copy.start()
        copies.append(copy)
        index += 1
        yield
        copy.wait_recv()
        step_decay = decay(span)
        take, keep = late * step_decay + (1.0 - late), late + (1.0 - late) * step_decay
        got = high_buf[2 * number + 1].astype(F32)
        for slot in range(2):
            between = span - 1.0 - order[slot] if reverse else order[slot]
            reach[slot] += got * (late * decay(between))
            order[slot] = order[slot] + bit * span
        state[0] = got * take + state[0] * keep
        span *= 2.0
    for copy in copies:
        copy.wait_send()


def carry_buffers(plan, key_size, value_size):
    return [
        pltpu.VMEM((2, key_size, value_size), F32),
        pltpu.VMEM((2, key_size, value_size), F32),
        pltpu.VMEM((2 * max(len(plan.low), 1), 2, key_size, value_size), BF),
        pltpu.VMEM((2 * max(len(plan.high), 1), key_size, value_size), BF),
    ]


def spread_steps(sq, block, full, sends, receives, base, local_sem):
    rows, width = block.shape
    half = rows // 2
    p, y, c = sq.p, sq.y, sq.c
    top, low = (0, half), (half, half)

    def place(p_, y_, c_, start, count):
        return full.at[p_, pl.ds(start, count), pl.ds(pl.multiple_of((y_ * 2 + c_) * width, width), width)]

    def own(part):
        return block.at[pl.ds(part[0], part[1]), :]

    def send(index, source, target, device):
        copy = remote(source, target, sends, receives, base + index, device)
        copy.start()
        return copy

    def relay(index, p_, y_, part, device):
        return send(index, place(p_, y_, c, *part), place(p_, y_, c, *part), device)

    k0 = send(0, own(top), place(p, y, c, *top), sq.S)
    k2 = send(2, own(low), place(p, y, c, *low), sq.Y)
    k6 = send(6, block, place(p, y, c, 0, rows), sq.C)
    k1 = send(1, own(low), place(p, y, c, *low), sq.S)
    k3 = send(3, own(top), place(p, y, c, *top), sq.Y)
    keep = pltpu.make_async_copy(block, place(p, y, c, 0, rows), local_sem)
    keep.start()
    yield
    k2.wait_recv()
    k4 = relay(4, p, 1 - y, low, sq.S)
    k9 = relay(9, p, 1 - y, low, sq.C)
    k0.wait_recv()
    k5 = relay(5, 1 - p, y, top, sq.Y)
    k7 = relay(7, 1 - p, y, top, sq.C)
    yield
    k1.wait_recv()
    k8 = relay(8, 1 - p, y, low, sq.C)
    k3.wait_recv()
    k10 = relay(10, p, 1 - y, top, sq.C)
    yield
    k5.wait_recv()
    k11 = relay(11, 1 - p, 1 - y, top, sq.C)
    k4.wait_recv()
    k12 = relay(12, 1 - p, 1 - y, low, sq.C)
    for copy in (k6, k7, k8, k9, k10, k11, k12):
        copy.wait_recv()
    for copy in (k0, k1, k2, k3, k4, k5, k6, k7, k8, k9, k10, k11, k12):
        copy.wait_send()
    keep.wait()


def pass_steps(sq, block, full, sends, receives, base, wide):
    rows = full.shape[1]
    width = full.shape[2] // 4
    half = rows // 2
    p, y, c = sq.p, sq.y, sq.c
    parts = ((0, half), (half, half))
    copies = []

    def place(p_, y_, part):
        columns = pl.ds(pl.multiple_of((y_ * 2 + c) * width, width), width)
        return full.at[p_, pl.ds(part[0], part[1]), columns]

    def send(index, source, p_, y_, part, device):
        copy = remote(source, place(p_, y_, part), sends, receives, base + index, device)
        copy.start()
        copies.append(copy)
        return copy

    def own(part):
        return block.at[pl.ds(part[0], part[1]), :]

    far = [send(i, own(part), p, y, part, sq.S) for i, part in enumerate(parts)]
    beside, near = [], []
    if wide:
        beside += [send(2 + i, own(part), p, y, part, sq.Y) for i, part in enumerate(parts)]
        near += [send(4 + i, own(part), p, y, part, sq.C) for i, part in enumerate(parts)]
    yield
    other = []
    for i, part in enumerate(parts):
        far[i].wait_recv()
        other.append(send(6 + i, place(1 - p, y, part), 1 - p, y, part, sq.Y))
        near.append(send(8 + i, place(1 - p, y, part), 1 - p, y, part, sq.C))
    yield
    for i, part in enumerate(parts):
        if wide:
            beside[i].wait_recv()
            near.append(send(10 + i, place(p, 1 - y, part), p, 1 - y, part, sq.C))
        other[i].wait_recv()
        near.append(send(12 + i, place(1 - p, 1 - y, part), 1 - p, 1 - y, part, sq.C))
    yield
    for copy in near:
        copy.wait_recv()
    for copy in copies:
        copy.wait_send()


PASS_COPIES = 14


def reduce_steps(sq, block_of, result, hand, near, total, arrived, sends, receives, base):
    rows, width = result.shape
    half = rows // 2
    p, y, c = sq.p, sq.y, sq.c
    top, low = pl.ds(0, half), pl.ds(half, half)

    def send(index, source, target, device):
        copy = remote(source, target, sends, receives, base + index, device)
        copy.start()
        return copy

    order = ((1 - p, 1 - y), (1 - p, y), (p, 1 - y), (p, y))

    def give(i, p_, y_):
        return remote(hand.at[p_, y_], near.at[p_, y_], sends, receives, base + i, sq.C)

    @pl.loop(0, 4)
    def _(i):
        p_, y_ = (1 - p + i // 2) % 2, (1 - y + i % 2) % 2
        hand[p_, y_] = block_of(p_, y_, 1 - c).astype(BF)
        give(i, p_, y_).start()

    given = [give(i, p_, y_) for i, (p_, y_) in enumerate(order)]

    def join(i):
        p_, y_ = order[i]
        own = block_of(p_, y_, c)
        given[i].wait_recv()
        return own + near[p_, y_].astype(F32)

    total[1 - p, 1 - y] = join(0).astype(BF)
    a = send(4, total.at[1 - p, 1 - y, low], arrived.at[0], sq.S)
    b = send(5, total.at[1 - p, 1 - y, top], arrived.at[1], sq.Y)
    total[1 - p, y] = join(1).astype(BF)
    e = send(6, total.at[1 - p, y, low], arrived.at[2], sq.S)
    total[p, 1 - y] = join(2).astype(BF)
    f = send(7, total.at[p, 1 - y, top], arrived.at[3], sq.Y)
    result[...] = join(3)
    yield
    b.wait_recv()
    total[1 - p, y, top] = (total[1 - p, y, top].astype(F32) + arrived[1].astype(F32)).astype(BF)
    g = send(8, total.at[1 - p, y, top], arrived.at[4], sq.S)
    a.wait_recv()
    total[p, 1 - y, low] = (total[p, 1 - y, low].astype(F32) + arrived[0].astype(F32)).astype(BF)
    d = send(9, total.at[p, 1 - y, low], arrived.at[5], sq.Y)
    yield
    e.wait_recv()
    f.wait_recv()
    g.wait_recv()
    result[top, :] += arrived[4].astype(F32) + arrived[3].astype(F32)
    d.wait_recv()
    result[low, :] += arrived[2].astype(F32) + arrived[5].astype(F32)
    for copy in given + [a, b, e, f, g, d]:
        copy.wait_send()


def reduce_room(rows, width):
    return [pltpu.VMEM((2, 2, rows, width), BF)] * 3 + [pltpu.VMEM((6, rows // 2, width), BF)]


def flipped(plan, at, mask):
    return {axis: 1 - at[axis] for i, axis in enumerate(plan.seq) if mask >> i & 1}


def greet_all(plan, at, sq):
    barrier = pltpu.get_barrier_semaphore()
    peers = [flipped(plan, at, mask) for mask in range(1, 1 << len(plan.seq))] + [sq.Y, sq.C, sq.X]
    for peer in peers:
        pl.semaphore_signal(barrier, inc=1, device_id=peer, device_id_type=MESH)
    pl.semaphore_wait(barrier, len(peers))


def column_of(rows, start, sign, rate):
    offset = lax.broadcasted_iota(jnp.int32, (rows, 1), 0).astype(F32)
    return jnp.exp((start + sign * offset) * rate)


def decay_mask(mask, rate):
    rows = mask.shape[0]

    @pl.loop(0, rows // 128)
    def _(i):
        start = pl.multiple_of(i * 128, 128)
        line = lax.broadcasted_iota(jnp.int32, (128, rows), 0) + start
        lane = lax.broadcasted_iota(jnp.int32, (128, rows), 1)
        distance = (line - lane).astype(F32)
        mask[pl.ds(start, 128), :] = jnp.where(distance >= 0, jnp.exp(jnp.maximum(distance, 0.0) * rate), 0.0)


TILE = 256


def row_tiles(full, body):
    rows = full.shape[1]
    each = rows // TILE

    @pl.loop(0, 2 * each)
    def _(i):
        body(i // each, pl.multiple_of(i % each * TILE, TILE), pl.multiple_of(i * TILE, TILE))


def turned(r, slot, start):
    base = r.turn[slot]
    cos_at, sin_at = base[0:1], base[1:2]
    cos_off, sin_off = r.cos_off[pl.ds(start, TILE), :], r.sin_off[pl.ds(start, TILE), :]
    return cos_at * cos_off - sin_at * sin_off, sin_at * cos_off + cos_at * sin_off


def front_kernel(plan, names, *refs):
    r = types.SimpleNamespace(**dict(zip(names, refs)))
    at = {axis: lax.axis_index(axis) for axis in plan.seq + plan.head}
    sq = Square(plan.pair)
    length, model = r.inputs.shape
    width = r.block.shape[1]
    mine = sq.y * 2 + sq.c
    column = pl.multiple_of(mine * width, width)
    rate = r.rate[0:1, 0:1]
    weights = [r.wq, r.wk, r.wv, r.wg, r.wo, r.wu, r.wd]
    key_size, value_size = r.wq.shape[1], r.wv.shape[1]
    saved = []

    def save(source, target):
        copy = pltpu.make_async_copy(source, target, r.save_sem.at[len(saved)])
        copy.start()
        saved.append(copy)

    greet_all(plan, at, sq)
    bulk = Bulk(plan, at, [r.sq, r.sk, r.sv, r.sg, r.so, r.su, r.sd], weights, r.bulk_send, r.bulk_receive, r.bulk_local)
    QUERY, KEY, VALUE, GATE, OUT, UP, DOWN = range(7)
    pair, high, low = [bulk.axes[0]], bulk.high, bulk.low

    size = 1 << len(plan.seq)
    copies = []
    for mask in range(1, size):
        copy = remote(r.vec, r.vecs.at[bulk.me], r.vec_send, r.vec_receive, mask, flipped(plan, at, mask))
        copy.start()
        copies.append(copy)
    r.vecs[bulk.me] = r.vec[...]
    bulk.begin(QUERY, bulk.axes)
    bulk.begin(KEY, bulk.axes)
    for unit in (VALUE, GATE, OUT):
        bulk.begin(unit, low)

    for copy in copies:
        copy.wait_recv()
    step = r.vec.shape[1]
    for j in range(size):
        r.all_gains[:, j * step : (j + 1) * step] = r.vecs[j]
    r.gains[...] = r.all_gains[:, pl.ds(column, width)]

    @pl.loop(0, length // 128)
    def _(i):
        rows = pl.ds(pl.multiple_of(i * 128, 128), 128)
        stream = r.inputs[rows, :]
        mean = jnp.mean(stream, axis=1, keepdims=True)
        inverse = lax.rsqrt(jnp.mean(jnp.square(stream - mean), axis=1, keepdims=True) + EPSILON)
        r.inverse_one[rows, :] = jnp.broadcast_to(inverse, (128, 128))
        normed = (stream - mean) * inverse
        hidden = (normed * r.all_gains[0:1, :] + r.all_gains[1:2, :]).astype(BF)
        r.hidden[sq.p, rows, :] = hidden
        own = (r.inputs[rows, pl.ds(column, width)] - mean) * inverse
        r.normed_one[rows, :] = own
        r.block[rows, :] = (own * r.gains[0:1, :] + r.gains[1:2, :]).astype(BF)

    gains = r.gains[...]
    hid = pass_steps(sq, r.block, r.hidden, r.hid_send, r.hid_receive, 0, False)
    cot = pass_steps(sq, r.cot, r.cot_out, r.cot_send, r.cot_receive, 0, True)
    keep_cot = pltpu.make_async_copy(r.cot, r.cot_out.at[sq.p, :, pl.ds(column, width)], r.local_sem.at[0])
    keep_cot.start()
    next(hid)
    bulk.begin(VALUE, pair + high)
    bulk.paired(QUERY)
    bulk.paired(KEY)
    bulk.first(QUERY)
    bulk.first(KEY)
    bulk.paired(VALUE)
    bulk.begin(GATE, pair + high)
    bulk.begin(OUT, pair + high)
    next(hid)
    decay_mask(r.mask, rate)
    bulk.second(QUERY)
    bulk.second(KEY)
    bulk.first(VALUE)
    next(hid)
    next(hid, None)
    save(r.hidden, r.hidden_out)

    bulk.finish(QUERY)
    bulk.finish(KEY)
    save(r.wq, r.wq_out)
    save(r.wk, r.wk_out)

    def project_keys(slot, start, row):
        hidden = r.hidden[slot, pl.ds(start, TILE), :]
        cosine, sine = turned(r, slot, start)
        for weight, target in ((r.wq, r.q), (r.wk, r.k)):
            value = mm(hidden, weight[...])
            target[pl.ds(row, TILE), :] = rotate(value, cosine, sine).astype(BF)

    row_tiles(r.hidden, project_keys)

    bulk.second(VALUE)
    bulk.paired(GATE)
    bulk.paired(OUT)
    bulk.finish(VALUE)
    save(r.wv, r.wv_out)

    def project_values(slot, start, row):
        r.v[pl.ds(row, TILE), :] = mm(r.hidden[slot, pl.ds(start, TILE), :], r.wv[...]).astype(BF)

    row_tiles(r.hidden, project_values)
    save(r.q, r.q_out)
    save(r.k, r.k_out)
    save(r.v, r.v_out)
    weight_out = column_of(length, float(length), -1.0, rate)
    for slot in range(2):
        rows = slice(slot * length, (slot + 1) * length)
        key = (r.k[rows, :].astype(F32) * weight_out).astype(BF)
        r.state[slot] = t_mm(key, r.v[rows, :])
    carry = carried(
        plan, at, r.state, r.reach, r.low_buf, r.high_buf, rate, length, False, r.carry_send, r.carry_receive, 0
    )
    next(carry)

    def inner(slot, start, row):
        scores = mm_t(r.q[pl.ds(row, TILE), :], r.k[pl.ds(pl.multiple_of(slot * length, length), length), :])
        weights_ = (scores * r.mask[pl.ds(start, TILE), :]).astype(BF)
        r.normed[pl.ds(row, TILE), :] = mm(weights_, r.v[pl.ds(pl.multiple_of(slot * length, length), length), :])

    row_tiles(r.hidden, inner)
    bulk.first(GATE)
    bulk.first(OUT)
    bulk.begin(UP, pair)
    bulk.begin(DOWN, pair)
    next(carry, None)
    bulk.second(GATE)
    bulk.second(OUT)
    bulk.begin(UP, high + low)
    bulk.begin(DOWN, low)
    bulk.finish(GATE)
    save(r.wg, r.wg_out)

    def gates(slot, start, row):
        r.gate[pl.ds(row, TILE), :] = mm(r.hidden[slot, pl.ds(start, TILE), :], r.wg[...])

    row_tiles(r.hidden, gates)
    save(r.gate, r.gate_out)
    bulk.paired(UP, low)
    bulk.paired(DOWN, low)
    for _ in carry:
        pass
    for slot in range(2):
        r.reach_bf[slot] = r.reach[slot].astype(BF)
    save(r.reach_bf, r.reach_out)

    def outer(slot, start, row):
        rows = pl.ds(row, TILE)
        offset = lax.broadcasted_iota(jnp.int32, (TILE, 1), 0) + start
        cross = mm(r.q[rows, :], r.reach_bf[slot]) * jnp.exp(offset.astype(F32) * rate)
        retained = r.normed[rows, :] + cross
        center = retained - jnp.mean(retained, axis=1, keepdims=True)
        inverse = lax.rsqrt(jnp.mean(center * center, axis=1, keepdims=True) + EPSILON)
        value = center * inverse
        r.normed[rows, :] = value
        r.inverse[rows, :] = jnp.broadcast_to(inverse, (TILE, 128))
        gate = r.gate[rows, :]
        r.gated[rows, :] = (gate * jax.nn.sigmoid(gate) * value).astype(BF)

    row_tiles(r.hidden, outer)
    save(r.normed, r.normed_out)
    save(r.inverse, r.inverse_out)
    save(r.gated, r.gated_out)
    bulk.finish(OUT)
    save(r.wo, r.wo_out)

    def out_block(p_, y_, c_):
        rows = pl.ds(pl.multiple_of(p_ * length, length), length)
        return mm_t(r.gated[rows, :], r.wo[pl.ds(pl.multiple_of((y_ * 2 + c_) * width, width), width), :])

    def nothing():
        pass

    def rest_of_up():
        bulk.forward(UP, bulk.bit[pair[0]], high)
        bulk.begin(DOWN, high)

    def rest_of_down():
        bulk.forward(DOWN, bulk.bit[pair[0]], high)
        next(cot)
        bulk.first(UP)

    def second_up():
        bulk.second(UP)
        bulk.first(DOWN)

    reduce = reduce_steps(
        sq, out_block, r.middle, r.hand, r.near, r.total, r.arrived, r.sends, r.receives, SPREAD_COPIES
    )
    together(reduce, nothing, rest_of_up)
    whole = r.middle[...] + r.inputs[:, pl.ds(column, width)]
    r.middle[...] = whole
    mean = jnp.mean(whole, axis=1, keepdims=True)
    deviation = jnp.mean(jnp.square(whole - mean), axis=1, keepdims=True)
    base = SPREAD_COPIES + REDUCE_COPIES
    means, spreads = exchange(sq, mean, deviation, r.stats, r.sends, r.receives, base)
    center = sum(means) * (1.0 / len(means))
    variance = sum(s + jnp.square(m - center) for m, s in zip(means, spreads)) * (1.0 / len(means))
    mean, scale = upright(center, lax.rsqrt(variance + EPSILON))
    r.inverse_two[...] = jnp.broadcast_to(scale, r.inverse_two.shape)
    value = (r.middle[...] - mean) * scale
    r.normed_two[...] = value
    r.block[...] = (value * gains[2:3] + gains[3:4]).astype(BF)
    spread = spread_steps(sq, r.block, r.mid_out, r.sends, r.receives, 0, r.local_sem.at[1])
    together(spread, nothing, rest_of_down, second_up)
    bulk.finish(UP)
    save(r.wu, r.wu_out)
    next(cot)
    bulk.second(DOWN)
    next(cot)
    next(cot, None)
    bulk.finish(DOWN)
    save(r.wd, r.wd_out)
    bulk.drain()
    keep_cot.wait()
    for copy in copies:
        copy.wait_send()
    for copy in saved:
        copy.wait()


def front(plan, shards, inputs, cot, vec, rate, turn, cos_off, sin_off, number):
    length, model = inputs.shape
    width = cot.shape[1]
    size = 1 << len(plan.seq)
    key_size, value_size, hidden = shards[0].shape[1] // 2, shards[2].shape[1] // 2, shards[5].shape[1] // 2
    any_spec, vmem_spec = pl.BlockSpec(memory_space=pl.ANY), pl.BlockSpec(memory_space=pltpu.VMEM)
    both = 2 * length

    def shape(dims, kind=BF):
        return jax.ShapeDtypeStruct(dims, kind)

    sq, sk, sv, sg, so, su, sd = shards
    far = dict(sq=sq, sk=sk, sv=sv, sg=sg, so=so, su=su, sd=sd)
    near = dict(inputs=inputs, cot=cot, vec=vec, rate=rate, turn=turn, cos_off=cos_off, sin_off=sin_off)
    wq, wk, wv, wg, wo, wu, wd = [(model, s.shape[1] // 2) for s in shards]
    far_outs = dict(
        wq_out=shape(wq),
        wk_out=shape(wk),
        wv_out=shape(wv),
        wg_out=shape(wg),
        wo_out=shape(wo),
        wu_out=shape(wu),
        wd_out=shape(wd),
        hidden_out=shape((2, length, model)),
        cot_out=shape((2, length, model)),
        mid_out=shape((2, length, model)),
        q_out=shape((both, key_size)),
        k_out=shape((both, key_size)),
        v_out=shape((both, value_size)),
        reach_out=shape((2, key_size, value_size)),
        gate_out=shape((both, value_size), F32),
        normed_out=shape((both, value_size), F32),
        inverse_out=shape((both, 128), F32),
        gated_out=shape((both, value_size)),
    )
    near_outs = dict(
        middle=shape((length, width), F32),
        normed_one=shape((length, width), F32),
        inverse_one=shape((length, 128), F32),
        normed_two=shape((length, width), F32),
        inverse_two=shape((length, 128), F32),
        gains=shape((8, width), F32),
    )
    carries = carry_buffers(plan, key_size, value_size)
    count = SPREAD_COPIES + REDUCE_COPIES + 3
    dma = pltpu.SemaphoreType.DMA
    hand, near_room, total, arrived = reduce_room(length, width)
    scratch = dict(
        wq=pltpu.VMEM(wq, BF),
        wk=pltpu.VMEM(wk, BF),
        wv=pltpu.VMEM(wv, BF),
        wg=pltpu.VMEM(wg, BF),
        wo=pltpu.VMEM(wo, BF),
        wu=pltpu.VMEM(wu, BF),
        wd=pltpu.VMEM(wd, BF),
        hidden=pltpu.VMEM((2, length, model), BF),
        block=pltpu.VMEM((length, width), BF),
        q=pltpu.VMEM((both, key_size), BF),
        k=pltpu.VMEM((both, key_size), BF),
        v=pltpu.VMEM((both, value_size), BF),
        gate=pltpu.VMEM((both, value_size), F32),
        normed=pltpu.VMEM((both, value_size), F32),
        inverse=pltpu.VMEM((both, 128), F32),
        gated=pltpu.VMEM((both, value_size), BF),
        mask=pltpu.VMEM((length, length), F32),
        state=carries[0],
        reach=carries[1],
        low_buf=carries[2],
        high_buf=carries[3],
        reach_bf=pltpu.VMEM((2, key_size, value_size), BF),
        vecs=pltpu.VMEM((size,) + vec.shape, F32),
        stats=pltpu.VMEM((4, 8, length), F32),
        hand=hand,
        near=near_room,
        total=total,
        arrived=arrived,
        bulk_send=dma((7 * size,)),
        bulk_receive=dma((7 * size,)),
        bulk_local=dma((7,)),
        vec_send=dma((size,)),
        vec_receive=dma((size,)),
        carry_send=dma((len(plan.seq),)),
        carry_receive=dma((len(plan.seq),)),
        all_gains=pltpu.VMEM((8, model), F32),
        hid_send=dma((PASS_COPIES,)),
        hid_receive=dma((PASS_COPIES,)),
        cot_send=dma((PASS_COPIES,)),
        cot_receive=dma((PASS_COPIES,)),
        sends=dma((count,)),
        receives=dma((count,)),
        local_sem=dma((3,)),
        save_sem=dma((32,)),
    )
    names = list(far) + list(near) + list(far_outs) + list(near_outs) + list(scratch)
    results = pl.pallas_call(
        functools.partial(front_kernel, plan, names),
        out_shape=tuple(far_outs.values()) + tuple(near_outs.values()),
        in_specs=[any_spec] * len(far) + [vmem_spec] * len(near),
        out_specs=(any_spec,) * len(far_outs) + (vmem_spec,) * len(near_outs),
        scratch_shapes=list(scratch.values()),
        compiler_params=pltpu.CompilerParams(
            collective_id=number, has_side_effects=True, vmem_limit_bytes=VMEM_LIMIT
        ),
        name="front",
    )(*far.values(), *near.values())
    return types.SimpleNamespace(**dict(zip(list(far_outs) + list(near_outs), results)))


SLOT = (1, 0, 2, 0, 3, None)


class Return:
    def __init__(self, plan, at, totals, spare, got, sends, receives):
        self.at, self.totals, self.spare, self.got = at, totals, spare, got
        self.sends, self.receives = sends, receives
        self.order = plan.low + list(reversed(plan.high)) + [plan.pair]
        self.bit = {axis: 1 << i for i, axis in enumerate(plan.seq)}
        self.size = 1 << len(plan.seq)
        self.me = sum(at[axis] * self.bit[axis] for axis in self.order)
        self.copies = {}

    def stage_of(self, mask):
        for stage, axis in enumerate(self.order):
            if mask & self.bit[axis]:
                return stage
        return len(self.order)

    def masks(self, stage):
        found = [m for m in range(1, self.size) if self.stage_of(m) == stage]
        return sorted(found, key=lambda m: (self.stage_of(m ^ self.bit[self.order[stage]]), m))

    def link(self, unit, mask, axis=None):
        axis = axis or self.order[self.stage_of(mask)]
        return remote(
            self.total(unit, mask),
            self.got.at[unit, mask - 1],
            self.sends,
            self.receives,
            unit * self.size + mask,
            {axis: 1 - self.at[axis]},
        )

    def total(self, unit, mask):
        rows, columns = self.got.shape[2:]
        if SLOT[unit] is None:
            across, down = self.spare.shape[2] // columns, self.spare.shape[1] // rows
            tile = self.spare.at[mask // (across * down)]
            return tile.at[pl.ds(mask // across % down * rows, rows), pl.ds(mask % across * columns, columns)]
        return self.totals.at[SLOT[unit], pl.ds(mask * rows, rows), :]

    def send(self, unit, mask):
        copy = self.link(unit, mask)
        copy.start()
        self.copies[unit, mask] = copy

    def made(self, unit, mask):
        if self.stage_of(mask) == 0:
            self.send(unit, mask)

    def ahead(self, stage):
        bit = self.bit[self.order[stage]]
        masks = self.masks(stage)
        first = [m for m in masks if m ^ bit and self.stage_of(m ^ bit) == stage + 1]
        return first, [m for m in masks if m not in first]

    def collect(self, unit, stage, masks):
        axis = self.order[stage]
        for mask in masks:
            target = mask ^ self.bit[axis]
            self.link(unit, mask).wait_recv()
            total = self.total(unit, target)
            total[...] = (total[...].astype(F32) + self.got[unit, mask - 1].astype(F32)).astype(BF)
            if self.stage_of(target) == stage + 1 and target:
                self.send(unit, target)

    def early(self, unit):
        self.collect(unit, 0, self.ahead(0)[0])

    def late(self, unit):
        self.collect(unit, 0, self.ahead(0)[1])

    def middle(self, unit):
        for stage in range(1, len(self.order) - 1):
            self.collect(unit, stage, self.masks(stage))

    def last(self, unit):
        return self.got.at[unit, self.bit[self.order[-1]] - 1]

    def last_arrived(self, unit):
        self.link(unit, self.bit[self.order[-1]]).wait_recv()

    def clear(self, unit):
        for (number, _), copy in self.copies.items():
            if number == unit:
                copy.wait_send()


def back_kernel(plan, names, *refs):
    r = types.SimpleNamespace(**dict(zip(names, refs)))
    at = {axis: lax.axis_index(axis) for axis in plan.seq + plan.head}
    sq = Square(plan.pair)
    length, width = r.cot.shape
    key_size, value_size = r.q.shape[1], r.v.shape[1]
    mine = sq.y * 2 + sq.c
    rate = r.rate[0:1, 0:1]
    UP, DOWN, OUT, GATE, VALUE, KEYS = range(6)
    back = Return(plan, at, r.totals, r.tiles, r.got, r.bulk_send, r.bulk_receive)
    piece, model = r.got.shape[2], r.mid.shape[2]
    strip = r.strips.shape[2]
    per_strip = strip // piece

    loads = {}

    def load(name, source, target):
        copy = pltpu.make_async_copy(source, target, r.load_sem.at[len(loads)])
        copy.start()
        loads[name] = copy

    def ready(*wanted):
        for name in wanted:
            loads[name].wait()

    load("wu", r.wu, r.weights.at[0])
    load("wd", r.wd, r.weights.at[1])

    parts = model // value_size

    def tile_copy(source, i):
        each = length // TILE
        rows = source.at[i // each, pl.ds(i % each * TILE, TILE), :]
        return [pltpu.make_async_copy(rows, r.tiles.at[i % 2], r.tile_sem.at[i % 2, 0])]

    def cot_tile(i, part):
        return r.totals.at[r.totals.shape[0] - 1, pl.ds((i % 2 * parts + part) * TILE, TILE), :]

    def cot_copy(i):
        each = length // TILE
        return [
            pltpu.make_async_copy(
                r.cotf.at[i // each, pl.ds(i % each * TILE, TILE), pl.ds(part * value_size, value_size)],
                cot_tile(i, part),
                r.tile_sem.at[i % 2, 1 + part],
            )
            for part in range(parts)
        ]

    def start(copies):
        for copy in copies:
            copy.start()

    def wait(copies):
        for copy in copies:
            copy.wait()

    tile_count = 2 * length // TILE
    start(tile_copy(r.mid, 0) + cot_copy(0))
    greet_all(plan, at, sq)
    load("wo", r.wo, r.weights.at[2])
    load("gated", r.gated_in, r.gated)
    load("gate", r.gate_in, r.gate)
    load("normed", r.normed_in, r.normed)
    load("inverse", r.inverse_in, r.inverse)
    load("q", r.q_in, r.q)
    load("k", r.k_in, r.k)
    load("v", r.v_in, r.v)
    load("reach", r.reach_in, r.in_bf)
    load("middle", r.middle_in, r.layer_out)
    ready("wu", "wd")

    for i in range(tile_count):
        if i + 1 < tile_count:
            start(tile_copy(r.mid, i + 1) + cot_copy(i + 1))
        wait(tile_copy(r.mid, i) + cot_copy(i))
        rows = slice(i * TILE, (i + 1) * TILE)
        preact = mm(r.tiles[i % 2], r.weights[0])
        cdf = 0.5 * (1.0 + lax.erf(preact * 0.7071067811865476))
        slope = cdf + preact * (jnp.exp(-0.5 * preact * preact) * 0.3989422804014327)
        r.hidden_ff[rows, :] = (preact * cdf).astype(BF)
        grad = sum(
            mm(cot_tile(i, part)[...], r.weights[1, part * value_size : (part + 1) * value_size, :])
            for part in range(parts)
        )
        r.grad_pre[rows, :] = (grad * slope).astype(BF)

    def strip_copy(source, mask, number):
        start = pl.multiple_of((back.me ^ mask) // per_strip * strip, strip)
        half = r.strips.at[number % 2]
        return [
            pltpu.make_async_copy(
                source.at[slot, :, pl.ds(start, strip)],
                half.at[pl.ds(slot * length, length), :],
                r.strip_sem.at[number % 2, slot],
            )
            for slot in range(2)
        ]

    def produce(unit, source, grads, masks):
        count = len(masks)
        step = masks[1] - masks[0] if count > 1 else 0
        even = all(mask == masks[0] + number * step for number, mask in enumerate(masks))

        def one(number, mask):
            for copy in strip_copy(source, mask, number):
                copy.wait()
            value = t_mm(r.strips[number % 2], grads[...])
            if per_strip > 1:
                r.whole_strip[...] = value
                inside = pl.multiple_of((back.me ^ mask) % per_strip * piece, piece)
                value = r.whole_strip[pl.ds(inside, piece), :]
            back.total(unit, mask)[...] = value.astype(BF)

        for copy in strip_copy(source, masks[0], 0):
            copy.start()
        if even:

            @pl.loop(0, count)
            def _(number):
                @pl.when(number + 1 < count)
                def _():
                    for copy in strip_copy(source, masks[0] + (number + 1) * step, number + 1):
                        copy.start()

                mask = masks[0] + number * step
                one(number, mask)
                if back.stage_of(masks[0]) == 0:
                    back.link(unit, mask, back.order[0]).start()

            for mask in masks:
                if back.stage_of(mask) == 0:
                    back.copies[unit, mask] = back.link(unit, mask)
        else:
            for number, mask in enumerate(masks):
                if number + 1 < count:
                    for copy in strip_copy(source, masks[number + 1], number + 1):
                        copy.start()
                one(number, mask)
                back.made(unit, mask)

    away_first, away_rest = back.ahead(0)
    low_bit = back.bit[back.order[0]]
    home_first, home_rest = ([m ^ low_bit for m in masks] for masks in (away_first, away_rest))

    def blocks(grads, weight):
        def block_of(p_, y_, c_):
            rows = pl.ds(pl.multiple_of(p_ * length, length), length)
            columns = pl.ds(pl.multiple_of((y_ * 2 + c_) * width, width), width)
            return sum(mm_t(g[rows, :], r.weights[w, columns, :]) for g, w in zip(grads, weight))

        return block_of

    def reduce(grads, weight, result, base):
        return reduce_steps(
            sq, blocks(grads, weight), result, r.hand, r.near, r.near, r.arrived, r.sends, r.receives, base
        )

    emitted = {}

    def emit(unit):
        own = at[plan.pair]
        back.last_arrived(unit)
        emitted[unit] = [
            pltpu.make_async_copy(source, r.halves.at[unit, half], r.emit_sem.at[unit, number])
            for number, (half, source) in enumerate(((own, back.total(unit, 0)), (1 - own, back.last(unit))))
        ]
        start(emitted[unit])

    def clear(unit):
        back.clear(unit)
        wait(emitted[unit])

    def norm_sums(upstream, gain, normed, inverse, base_stream, result, row, stats, base):
        value = upstream[...]
        product = value * normed[...]
        r.sums[row : row + 1, :] = jnp.sum(product, axis=0, keepdims=True)
        r.sums[row + 1 : row + 2, :] = jnp.sum(value, axis=0, keepdims=True)
        first = jnp.mean(value * gain, axis=1, keepdims=True)
        second = jnp.mean(product * gain, axis=1, keepdims=True)
        firsts, seconds = exchange(sq, first, second, stats, r.sends, r.receives, base)
        share = 1.0 / len(firsts)
        first, second = upright(sum(firsts) * share, sum(seconds) * share)
        result[...] = base_stream[...] + inverse[:, 0:1] * (upstream[...] * gain - first - normed[...] * second)

    def down_last():
        produce(DOWN, r.cotf, r.hidden_ff, away_rest)
        produce(DOWN, r.cotf, r.hidden_ff, home_first)
        produce(UP, r.mid, r.grad_pre, away_first)

    base = SPREAD_COPIES
    together(
        reduce([r.grad_pre], [0], r.upstream, base),
        lambda: produce(DOWN, r.cotf, r.hidden_ff, away_first),
        down_last,
    )
    base += REDUCE_COPIES
    back.early(DOWN)
    load("wv", r.wv, r.weights.at[0])
    norm_sums(r.upstream, r.gains[2:3, :], r.normed_two, r.inverse_two, r.cot, r.grad_middle, 2, r.stats, base)
    base += 3
    block = r.hand.at[0, 0]
    block[...] = r.grad_middle[...].astype(BF)

    def up_next():
        produce(UP, r.mid, r.grad_pre, away_rest)
        produce(DOWN, r.cotf, r.hidden_ff, home_rest)

    def up_last():
        back.late(DOWN)
        produce(UP, r.mid, r.grad_pre, home_rest)

    together(
        spread_steps(sq, block, r.gmid, r.sends, r.receives, 0, r.local_sem.at[0]),
        up_next,
        lambda: produce(UP, r.mid, r.grad_pre, home_first),
    )
    up_last()
    ready("wo", "gated", "gate", "normed", "inverse")
    back.early(UP)

    start(tile_copy(r.gmid, 0))
    for i in range(tile_count):
        if i + 1 < tile_count:
            start(tile_copy(r.gmid, i + 1))
        wait(tile_copy(r.gmid, i))
        rows = slice(i * TILE, (i + 1) * TILE)
        grad = mm(r.tiles[i % 2], r.weights[2])
        gate = r.gate[rows, :]
        normed = r.normed[rows, :]
        logistic = jax.nn.sigmoid(gate)
        swish = gate * logistic
        r.grad_gate[rows, :] = (grad * normed * (logistic + swish * (1.0 - logistic))).astype(BF)
        scaled = grad * swish
        r.grad_mixed[rows, :] = (
            r.inverse[rows, 0:1]
            * (
                scaled
                - jnp.mean(scaled, axis=1, keepdims=True)
                - normed * jnp.mean(scaled * normed, axis=1, keepdims=True)
            )
        ).astype(BF)
    load("wg", r.wg, r.weights.at[2])
    back.middle(DOWN)

    ready("q", "k", "v", "reach")
    decay_mask(r.mask, rate)
    weight_out = column_of(length, 1.0, 1.0, rate)
    for slot in range(2):
        rows = slice(slot * length, (slot + 1) * length)
        query = (r.q[rows, :].astype(F32) * weight_out).astype(BF)
        r.state[slot] = t_mm(query, r.grad_mixed[rows, :])
    carry = carried(
        plan, at, r.state, r.reach, r.low_buf, r.high_buf, rate, length, True, r.carry_send, r.carry_receive, 0
    )
    next(carry)
    produce(OUT, r.gmid, r.gated, away_first)
    weight_in = column_of(length, 0.0, 1.0, rate)
    weight_back = column_of(length, length - 1.0, -1.0, rate)

    def rotated_back(value, slot):
        base_ = r.turn[slot]
        cosine = base_[0:1] * r.cos_off[...] - base_[1:2] * r.sin_off[...]
        sine = base_[1:2] * r.cos_off[...] + base_[0:1] * r.sin_off[...]
        return unrotate(value, cosine, sine)

    @pl.loop(0, 2)
    def _(slot):
        rows = pl.ds(pl.multiple_of(slot * length, length), length)
        weights = (mm_t(r.grad_mixed[rows, :], r.v[rows, :]) * r.mask[...]).astype(BF)
        value = mm(weights, r.k[rows, :]) + mm_t(r.grad_mixed[rows, :], r.in_bf[slot]) * weight_in
        r.grad_keys[rows, 0:key_size] = rotated_back(value, slot).astype(BF)
        r.gate[rows, 0:key_size] = t_mm(weights, r.q[rows, :])
        weights = (mm_t(r.q[rows, :], r.k[rows, :]) * r.mask[...]).astype(BF)
        r.normed[rows, :] = t_mm(weights, r.grad_mixed[rows, :])

    produce(OUT, r.gmid, r.gated, away_rest)
    next(carry, None)
    feed = reduce([r.hidden_ff], [1], r.grad_inputs, base)
    base += REDUCE_COPIES
    next(feed)
    load("wk", r.wk, r.weights.at[1, :, pl.ds(key_size, key_size)])
    load("wq", r.wq, r.weights.at[1, :, pl.ds(0, key_size)])
    emit(DOWN)
    clear(DOWN)
    produce(GATE, r.hid, r.grad_gate, away_first)
    produce(OUT, r.gmid, r.gated, home_first)
    back.early(OUT)
    next(feed)
    produce(GATE, r.hid, r.grad_gate, away_rest)
    back.late(UP)
    for _ in carry:
        pass
    out_bf = r.low_buf.at[0]
    for slot in range(2):
        out_bf[slot] = r.reach[slot].astype(BF)

    @pl.loop(0, 2)
    def _(slot):
        rows = pl.ds(pl.multiple_of(slot * length, length), length)
        value = r.gate[rows, 0:key_size] + mm_t(r.v[rows, :], out_bf[slot]) * weight_back
        r.grad_keys[rows, key_size : 2 * key_size] = rotated_back(value, slot).astype(BF)
        value = r.normed[rows, :] + mm(r.k[rows, :], out_bf[slot]) * weight_back
        r.grad_pre[rows, :] = value.astype(BF)

    produce(VALUE, r.hid, r.grad_pre, away_first)
    produce(KEYS, r.hid, r.grad_keys, away_first)
    produce(VALUE, r.hid, r.grad_pre, away_rest)
    produce(KEYS, r.hid, r.grad_keys, away_rest)
    for _ in feed:
        pass
    normed_one = r.gate.at[pl.ds(0, length), :]
    load("normed_one", r.normed_one_in, normed_one)
    peers = (sq.S, sq.Y, sq.C)
    for number, peer in enumerate(peers):
        pl.semaphore_signal(r.again.at[number], inc=1, device_id=peer, device_id_type=MESH)
    ready("middle")
    r.layer_out[...] += r.grad_inputs[...]
    back.middle(UP)
    produce(GATE, r.hid, r.grad_gate, home_first)
    back.early(GATE)
    produce(OUT, r.gmid, r.gated, home_rest)
    back.late(OUT)
    back.middle(OUT)
    for number in range(len(peers)):
        pl.semaphore_wait(r.again.at[number], 1)

    ready("wv", "wg", "wk", "wq", "normed_one")

    def value_next():
        produce(VALUE, r.hid, r.grad_pre, home_first)
        back.early(VALUE)
        produce(KEYS, r.hid, r.grad_keys, home_first)

    def keys_next():
        back.early(KEYS)
        produce(GATE, r.hid, r.grad_gate, home_rest)
        back.late(GATE)
        back.middle(GATE)

    together(
        reduce([r.grad_keys, r.grad_pre, r.grad_gate], [1, 0, 2], r.upstream, base),
        value_next,
        keys_next,
    )
    base += REDUCE_COPIES
    norm_sums(r.upstream, r.gains[0:1, :], normed_one, r.inverse_one, r.grad_middle, r.grad_inputs, 0, r.stats_two, base)
    base += 3

    copies = []
    r.all_sums[back.me] = r.sums[...]
    for mask in range(1, back.size):
        copy = remote(r.sums, r.all_sums.at[back.me], r.sum_send, r.sum_receive, mask, flipped(plan, at, mask))
        copy.start()
        copies.append(copy)
    produce(VALUE, r.hid, r.grad_pre, home_rest)
    produce(KEYS, r.hid, r.grad_keys, home_rest)
    back.late(VALUE)
    back.late(KEYS)
    emit(UP)
    back.middle(VALUE)
    emit(OUT)
    back.middle(KEYS)
    emit(GATE)
    for copy in copies:
        copy.wait_recv()
    total = r.all_sums[0]
    for i in range(1, back.size):
        total = total + r.all_sums[i]
    r.by_block[mine] = total
    for index, device in enumerate((sq.Y, sq.C, sq.X)):
        copy = remote(r.by_block.at[mine], r.by_block.at[mine], r.sends, r.receives, base + index, device)
        copy.start()
        copies.append(copy)
    for copy in copies[-3:]:
        copy.wait_recv()
    r.sums_out[...] = r.by_block[back.me * piece // width]
    for copy in copies:
        copy.wait_send()
    emit(VALUE)
    emit(KEYS)
    for unit in (UP, OUT, GATE, VALUE, KEYS):
        clear(unit)


def back_pass(plan, f, cot, rate, turn, cos_off, sin_off, rows, number):
    length, width = cot.shape
    size = 1 << len(plan.seq)
    model = f.wq_out.shape[0]
    key_size, value_size = f.q_out.shape[1], f.v_out.shape[1]
    hidden = f.wu_out.shape[1]
    both = 2 * length
    any_spec, vmem_spec = pl.BlockSpec(memory_space=pl.ANY), pl.BlockSpec(memory_space=pltpu.VMEM)

    def shape(dims, kind=F32):
        return jax.ShapeDtypeStruct(dims, kind)

    far = dict(
        wq=f.wq_out,
        wk=f.wk_out,
        wv=f.wv_out,
        wg=f.wg_out,
        wo=f.wo_out,
        wu=f.wu_out,
        wd=f.wd_out,
        hid=f.hidden_out,
        mid=f.mid_out,
        cotf=f.cot_out,
        q_in=f.q_out,
        k_in=f.k_out,
        v_in=f.v_out,
        reach_in=f.reach_out,
        gate_in=f.gate_out,
        normed_in=f.normed_out,
        inverse_in=f.inverse_out,
        gated_in=f.gated_out,
        middle_in=f.middle,
        normed_one_in=f.normed_one,
    )
    near = dict(
        cot=cot,
        inverse_one=f.inverse_one,
        normed_two=f.normed_two,
        inverse_two=f.inverse_two,
        gains=f.gains,
        rate=rate,
        turn=turn,
        cos_off=cos_off,
        sin_off=sin_off,
    )
    far_outs = dict(halves=shape((6, 2, rows, value_size), BF), gmid=shape((2, length, model), BF))
    near_outs = dict(
        layer_out=shape((length, width)), grad_inputs=shape((length, width)), sums_out=shape((8, width))
    )
    carries = carry_buffers(plan, key_size, value_size)
    dma = pltpu.SemaphoreType.DMA
    count = SPREAD_COPIES + 3 * REDUCE_COPIES + 9
    strip = max(rows, 128)
    hand, near_room, _, arrived = reduce_room(length, width)
    scratch = dict(
        weights=pltpu.VMEM((3, model, value_size), BF),
        tiles=pltpu.VMEM((2, TILE, model), BF),
        strips=pltpu.VMEM((2, both, strip), BF),
        q=pltpu.VMEM((both, key_size), BF),
        k=pltpu.VMEM((both, key_size), BF),
        v=pltpu.VMEM((both, value_size), BF),
        gate=pltpu.VMEM((both, value_size), F32),
        normed=pltpu.VMEM((both, value_size), F32),
        inverse=pltpu.VMEM((both, 128), F32),
        gated=pltpu.VMEM((both, value_size), BF),
        in_bf=pltpu.VMEM((2, key_size, value_size), BF),
        mask=pltpu.VMEM((length, length), F32),
        state=carries[0],
        reach=carries[1],
        low_buf=carries[2],
        high_buf=carries[3],
        hidden_ff=pltpu.VMEM((both, hidden), BF),
        grad_pre=pltpu.VMEM((both, hidden), BF),
        grad_gate=pltpu.VMEM((both, value_size), BF),
        grad_mixed=pltpu.VMEM((both, value_size), BF),
        grad_keys=pltpu.VMEM((both, 2 * key_size), BF),
        upstream=pltpu.VMEM((length, width), F32),
        grad_middle=pltpu.VMEM((length, width), F32),
        hand=hand,
        near=near_room,
        arrived=arrived,
        totals=pltpu.VMEM((4, model, value_size), BF),
        got=pltpu.VMEM((6, size - 1, rows, value_size), BF),
        stats=pltpu.VMEM((4, 8, length), F32),
        stats_two=pltpu.VMEM((4, 8, length), F32),
        sums=pltpu.VMEM((8, width), F32),
        all_sums=pltpu.VMEM((size, 8, width), F32),
        by_block=pltpu.VMEM((4, 8, width), F32),
        whole_strip=pltpu.VMEM((strip, value_size) if strip > rows else (8, 128), F32),
        bulk_send=dma((6 * size,)),
        bulk_receive=dma((6 * size,)),
        load_sem=dma((24,)),
        tile_sem=dma((2, 1 + model // value_size)),
        strip_sem=dma((2, 2)),
        emit_sem=dma((6, 2)),
        carry_send=dma((len(plan.seq),)),
        carry_receive=dma((len(plan.seq),)),
        sum_send=dma((size,)),
        sum_receive=dma((size,)),
        sends=dma((count,)),
        receives=dma((count,)),
        local_sem=dma((1,)),
        again=pltpu.SemaphoreType.REGULAR((3,)),
    )
    names = list(far) + list(near) + list(far_outs) + list(near_outs) + list(scratch)

    def kernel(*refs):
        back_kernel(plan, names, *refs)

    results = pl.pallas_call(
        kernel,
        out_shape=tuple(far_outs.values()) + tuple(near_outs.values()),
        in_specs=[any_spec] * len(far) + [vmem_spec] * len(near),
        out_specs=(any_spec,) * len(far_outs) + (vmem_spec,) * len(near_outs),
        scratch_shapes=list(scratch.values()),
        compiler_params=pltpu.CompilerParams(
            collective_id=number, has_side_effects=True, vmem_limit_bytes=VMEM_LIMIT
        ),
        name="back",
    )(*far.values(), *near.values())
    out = types.SimpleNamespace(**dict(zip(list(far_outs) + list(near_outs), results)))
    return finish(out, key_size)


def finish_kernel(key_size, halves, layer_in, grad_in, *refs):
    *outs, layer_out, grad_out = refs[:9]
    *stages, layer, grad, sems = refs[9:]
    loads = [
        pltpu.make_async_copy(source, stage, sems.at[number])
        for number, (source, stage) in enumerate(((layer_in, layer), (grad_in, grad)))
    ]
    for copy in loads:
        copy.start()
    stores = []

    def store(stage, target):
        copy = pltpu.make_async_copy(stage, target, sems.at[2 + len(stores)])
        copy.start()
        stores.append(copy)

    rows, columns = halves.shape[2:]
    for out, stage, unit, first, width in zip(
        outs, stages, (5, 5, 4, 3, 0, 2, 1), (0, key_size, 0, 0, 0, 0, 0), (key_size,) * 2 + (columns,) * 5
    ):
        for half in range(2):
            value = halves[unit, half, :, first : first + width].astype(F32)
            if out.shape[0] == rows:
                stage[:, half * width : (half + 1) * width] = value
            else:
                stage[half * width : (half + 1) * width, :] = value.T
        store(stage, out)
    for copy, stage, out in zip(loads, (layer, grad), (layer_out, grad_out)):
        copy.wait()
        store(stage, out)
    for copy in stores:
        copy.wait()


def finish(b, key_size):
    rows, value_size = b.halves.shape[2:]
    turned = rows % 128 == 0
    flat = [(rows, 2 * w) for w in (key_size, key_size, value_size, value_size, value_size)]
    shapes = flat + [(2 * value_size, rows) if turned else (rows, 2 * value_size)] * 2 + [b.layer_out.shape] * 2
    any_spec = pl.BlockSpec(memory_space=pl.ANY)
    results = pl.pallas_call(
        functools.partial(finish_kernel, key_size),
        out_shape=tuple(jax.ShapeDtypeStruct(s, F32) for s in shapes),
        in_specs=[pl.BlockSpec(memory_space=pltpu.VMEM), any_spec, any_spec],
        out_specs=tuple([any_spec] * len(shapes)),
        scratch_shapes=[pltpu.VMEM(s, F32) for s in shapes] + [pltpu.SemaphoreType.DMA((2 + len(shapes),))],
        name="finish",
    )(b.halves, b.layer_out, b.grad_inputs)
    gq, gk, gv, gg, gu, go, gd, layer_out, grad_inputs = results
    if not turned:
        go, gd = go.T, gd.T
    return types.SimpleNamespace(
        gq=gq, gk=gk, gv=gv, gg=gg, gu=gu, go=go, gd=gd, layer_out=layer_out, grad_inputs=grad_inputs, sums_out=b.sums_out
    )


def rotate(values, cosine, sine):
    half = values.shape[1] // 2
    first, second = values[:, :half], values[:, half:]
    return jnp.concatenate([first * cosine - second * sine, first * sine + second * cosine], axis=1)


def unrotate(values, cosine, sine):
    half = values.shape[1] // 2
    first, second = values[:, :half], values[:, half:]
    return jnp.concatenate([first * cosine + second * sine, second * cosine - first * sine], axis=1)


def on_device(
    plan,
    inputs,
    decay_exponent,
    first_gain,
    first_bias,
    query_weight,
    key_weight,
    value_weight,
    gate_weight,
    out_weight,
    second_gain,
    second_bias,
    up_weight,
    down_weight,
    cotangent,
):
    length, model = inputs.shape
    rows = query_weight.shape[0]
    pair_bit = lax.axis_index(plan.pair)
    column = lax.axis_index(plan.head_axes)
    width = cotangent.shape[1]

    key_size = query_weight.shape[1] // 2
    value_size = value_weight.shape[1] // 2
    hidden = up_weight.shape[1] // 2

    vec = jnp.stack([first_gain, first_bias, second_gain, second_bias] * 2).astype(F32)

    exponent = pick(decay_exponent, pair_bit, 0).astype(F32)
    lograte = jnp.log1p(-jnp.exp2(-exponent))
    offset = jnp.arange(length, dtype=F32)
    seq_index = lax.axis_index(plan.seq_axes)
    pair_weight = 2 ** plan.seq.index(plan.pair)
    first_slot = seq_index - pair_bit * pair_weight
    starts = jnp.stack([first_slot, first_slot + pair_weight]) * length
    frequency = np.exp(-math.log(10000.0) * np.arange(key_size // 2, dtype=np.float32) / (key_size // 2 - 1))
    frequency = frequency.astype(np.float32)
    angles = np.arange(length)[:, None] * frequency.astype(np.float64)[None, :]
    cos_off, sin_off = jnp.asarray(np.cos(angles), F32), jnp.asarray(np.sin(angles), F32)
    start_angles = starts.astype(F32)[:, None] * frequency[None, :]
    turn = jnp.stack([jnp.cos(start_angles), jnp.sin(start_angles)] * 4, axis=1)
    shards = [query_weight, key_weight, value_weight, gate_weight, out_weight.T, up_weight, down_weight.T]
    rate = jnp.full((8, 128), lograte, F32)
    f = front(plan, shards, inputs, cotangent.astype(BF), vec, rate, turn, cos_off, sin_off, 1)
    b = back_pass(plan, f, cotangent, rate, turn, cos_off, sin_off, rows, 2)
    place = seq_index % (width // rows) * rows
    mine = lax.dynamic_slice_in_dim(b.sums_out, place, rows, 1)
    return (
        b.layer_out,
        b.grad_inputs,
        mine[0],
        mine[1],
        b.gq,
        b.gk,
        b.gv,
        b.gg,
        b.go,
        mine[2],
        mine[3],
        b.gu,
        b.gd,
    )


def solution(mesh):
    seq_bits = (mesh.shape["seq"]).bit_length() - 1
    head_bits = (mesh.shape["head"]).bit_length() - 1
    plan = Plan(seq_bits, head_bits)
    seq, head = plan.seq_axes, plan.head_axes
    fine = Mesh(mesh.devices.reshape((2,) * (seq_bits + head_bits)), seq + head)
    in_specs = (
        P(seq, None),
        P(head),
        P(seq),
        P(seq),
        P(seq, head),
        P(seq, head),
        P(seq, head),
        P(seq, head),
        P(head, seq),
        P(seq),
        P(seq),
        P(seq, head),
        P(head, seq),
        P(seq, head),
    )
    out_specs = (
        P(seq, head),
        P(seq, head),
        P(seq),
        P(seq),
        P(seq, head),
        P(seq, head),
        P(seq, head),
        P(seq, head),
        P(head, seq),
        P(seq),
        P(seq),
        P(seq, head),
        P(head, seq),
    )

    def step(*args):
        return on_device(plan, *args)

    return jax.shard_map(step, mesh=fine, in_specs=in_specs, out_specs=out_specs, check_vma=False)
```

```python
import functools
import math
import types

import jax
import jax.numpy as jnp
import numpy as np
from jax import lax
from jax.experimental import pallas as pl
from jax.experimental.pallas import tpu as pltpu
from jax.sharding import Mesh, PartitionSpec as P

EPSILON = 1e-05
BF = jnp.bfloat16
F32 = jnp.float32
MESH = pl.DeviceIdType.MESH
VMEM_LIMIT = 67043328

def pick(array, index, axis):
    return lax.dynamic_index_in_dim(array, index, axis, keepdims=False)


def dot(left, right, contract):
    return lax.dot_general(left, right, (contract, ((), ())), preferred_element_type=F32)


def mm(left, right):
    return dot(left, right, ((1,), (0,)))


def mm_t(left, right):
    return dot(left, right, ((1,), (1,)))


def t_mm(left, right):
    return dot(left, right, ((0,), (0,)))


class Plan:
    def __init__(self, seq_bits, head_bits):
        self.seq = [f"s{i}" for i in range(seq_bits)]
        self.head = [f"h{i}" for i in range(head_bits)]
        self.names = tuple(reversed(self.seq)) + ()
        self.seq_axes = tuple(reversed(self.seq))
        self.head_axes = tuple(reversed(self.head))
        self.pair = "s1" if seq_bits > 1 else "s0"
        self.low = [a for a in self.seq if a < self.pair]
        self.high = [a for a in self.seq if a > self.pair]


class Square:
    def __init__(self, pair):
        self.pair = pair
        self.p = lax.axis_index(pair)
        self.y = lax.axis_index("h1")
        self.c = lax.axis_index("h0")
        self.S = {pair: 1 - self.p}
        self.Y = {"h1": 1 - self.y}
        self.C = {"h0": 1 - self.c}
        self.X = {"h1": 1 - self.y, "h0": 1 - self.c}

    def greet(self, cross=True):
        barrier = pltpu.get_barrier_semaphore()
        peers = [self.S, self.Y, self.C] + ([self.X] if cross else [])
        for peer in peers:
            pl.semaphore_signal(barrier, inc=1, device_id=peer, device_id_type=MESH)
        pl.semaphore_wait(barrier, len(peers))


def remote(source, target, sends, receives, index, device):
    return pltpu.make_async_remote_copy(
        src_ref=source,
        dst_ref=target,
        send_sem=sends.at[index],
        recv_sem=receives.at[index],
        device_id=device,
        device_id_type=MESH,
    )


def spread(sq, block, full, sends, receives, base, local_sem):
    rows, width = block.shape
    half = rows // 2

    def place(p, y, c, start, count):
        return full.at[p, pl.ds(start, count), pl.ds(pl.multiple_of((y * 2 + c) * width, width), width)]

    p, y, c = sq.p, sq.y, sq.c
    top, low = (0, half), (half, half)

    def own(part):
        return block.at[pl.ds(part[0], part[1]), :]

    def send(index, source, target, device):
        copy = remote(source, target, sends, receives, base + index, device)
        copy.start()
        return copy

    def relay(index, p_, y_, part, device):
        return send(index, place(p_, y_, c, *part), place(p_, y_, c, *part), device)

    k0 = send(0, own(top), place(p, y, c, *top), sq.S)
    k2 = send(2, own(low), place(p, y, c, *low), sq.Y)
    k6 = send(6, block, place(p, y, c, 0, rows), sq.C)
    k1 = send(1, own(low), place(p, y, c, *low), sq.S)
    k3 = send(3, own(top), place(p, y, c, *top), sq.Y)
    keep = pltpu.make_async_copy(block, place(p, y, c, 0, rows), local_sem)
    keep.start()
    k2.wait_recv()
    k4 = relay(4, p, 1 - y, low, sq.S)
    k9 = relay(9, p, 1 - y, low, sq.C)
    k0.wait_recv()
    k5 = relay(5, 1 - p, y, top, sq.Y)
    k7 = relay(7, 1 - p, y, top, sq.C)
    k1.wait_recv()
    k8 = relay(8, 1 - p, y, low, sq.C)
    k3.wait_recv()
    k10 = relay(10, p, 1 - y, top, sq.C)
    k5.wait_recv()
    k11 = relay(11, 1 - p, 1 - y, top, sq.C)
    k4.wait_recv()
    k12 = relay(12, 1 - p, 1 - y, low, sq.C)
    for copy in (k6, k7, k8, k9, k10, k11, k12):
        copy.wait_recv()
    for copy in (k0, k1, k2, k3, k4, k5, k6, k7, k8, k9, k10, k11, k12):
        copy.wait_send()
    keep.wait()


SPREAD_COPIES = 13
REDUCE_COPIES = 10


def exchange(sq, first, second, stats, sends, receives, base):
    rows = first.shape[0]
    lane = lax.broadcasted_iota(jnp.int32, (rows, 128), 1)
    packed = jnp.where(lane == 0, first, second).T
    mine = sq.y * 2 + sq.c
    stats[mine] = packed[:8]
    copies = []
    for index, device in enumerate((sq.Y, sq.C, sq.X)):
        copy = remote(stats.at[mine], stats.at[mine], sends, receives, base + index, device)
        copy.start()
        copies.append(copy)
    for copy in copies:
        copy.wait_recv()
    for copy in copies:
        copy.wait_send()
    return [stats[q][0:1] for q in range(4)], [stats[q][1:2] for q in range(4)]


def upright(first, second):
    rows = first.shape[1]
    line = lax.broadcasted_iota(jnp.int32, (128, rows), 0)
    turned = jnp.where(line == 0, first, second).T
    return turned[:, 0:1], turned[:, 1:2]


class Bulk:
    def __init__(self, plan, at, shards, wholes, sends, receives, local_sem):
        self.shards, self.wholes, self.at = shards, wholes, at
        self.sends, self.receives, self.local_sem = sends, receives, local_sem
        self.axes = [plan.pair] + plan.high + plan.low
        self.high, self.low, self.lows = plan.high, plan.low, len(plan.low)
        self.bit = {axis: 1 << plan.seq.index(axis) for axis in self.axes}
        self.me = sum(at[axis] * self.bit[axis] for axis in self.axes)
        self.size = 1 << len(self.axes)
        self.copies, self.kept, self.passed = [], {}, set()

    def piece(self, unit, mask):
        rows = self.shards[unit].shape[0]
        return self.wholes[unit].at[pl.ds(pl.multiple_of((self.me ^ mask) * rows, rows), rows), :]

    def half(self, unit, which):
        width = self.wholes[unit].shape[1]
        return self.shards[unit].at[:, pl.ds(pl.multiple_of(which * width, width), width)]

    def link(self, unit, source, held, axis):
        return remote(
            source,
            self.piece(unit, held),
            self.sends,
            self.receives,
            unit * self.size + (held | self.bit[axis]),
            {axis: 1 - self.at[axis]},
        )

    def send(self, unit, source, held, axis):
        copy = self.link(unit, source, held, axis)
        copy.start()
        self.copies.append(copy)

    def begin(self, unit, axes):
        own = self.at[self.axes[0]]
        for axis in axes:
            self.send(unit, self.half(unit, 1 - own if axis == self.axes[0] else own), 0, axis)
        if self.axes[0] in axes:
            keep = pltpu.make_async_copy(self.half(unit, own), self.piece(unit, 0), self.local_sem.at[unit])
            keep.start()
            self.kept[unit] = keep

    def held_before(self, stage):
        held = [0]
        for axis in self.axes[:stage]:
            held = held + [m | self.bit[axis] for m in held]
        return held

    def forward(self, unit, mask, axes):
        for later in axes:
            self.send(unit, self.piece(unit, mask), mask, later)

    def arrive(self, unit, stage, masks, axes=None):
        axis = self.axes[stage]
        for held in self.held_before(stage):
            mask = held | self.bit[axis]
            if not masks(mask):
                continue
            pltpu.make_async_remote_copy(
                src_ref=self.piece(unit, mask),
                dst_ref=self.piece(unit, mask),
                send_sem=self.sends.at[unit * self.size + mask],
                recv_sem=self.receives.at[unit * self.size + mask],
                device_id={axis: 1 - self.at[axis]},
                device_id_type=MESH,
            ).wait_recv()
            self.forward(unit, mask, self.axes[stage + 1 :] if axes is None else axes)

    def paired(self, unit, axes=None):
        self.arrive(unit, 0, lambda mask: True, axes)

    def first(self, unit):
        for stage in range(1, len(self.axes) - self.lows):
            self.arrive(unit, stage, lambda mask: not mask & self.bit[self.axes[0]])

    def second(self, unit):
        for stage in range(1, len(self.axes) - self.lows):
            self.arrive(unit, stage, lambda mask: mask & self.bit[self.axes[0]])

    def finish(self, unit):
        for stage in range(len(self.axes) - self.lows, len(self.axes)):
            self.arrive(unit, stage, lambda mask: True)
        self.kept[unit].wait()

    def drain(self):
        for copy in self.copies:
            copy.wait_send()


def together(process, *hooks):
    for number, _ in enumerate(process):
        if number < len(hooks):
            hooks[number]()


def carried(plan, at, state, reach, low_buf, high_buf, rate, length, reverse, sends, receives, base):
    index = base
    low_index = jnp.float32(0)
    span = 1.0
    copies = []

    def decay(count):
        return jnp.exp(rate * (count * float(length)))

    for slot in range(2):
        reach[slot] = jnp.zeros(reach.shape[1:], F32)
    for number, axis in enumerate(plan.low):
        bit = at[axis].astype(F32)
        late = 1.0 - bit if reverse else bit
        for slot in range(2):
            low_buf[2 * number, slot] = state[slot].astype(BF)
        copy = remote(low_buf.at[2 * number], low_buf.at[2 * number + 1], sends, receives, index, {axis: 1 - at[axis]})
        copy.start()
        copies.append(copy)
        index += 1
        yield
        copy.wait_recv()
        between = span - 1.0 - low_index if reverse else low_index
        step_decay = decay(span)
        take, keep = late * step_decay + (1.0 - late), late + (1.0 - late) * step_decay
        for slot in range(2):
            got = low_buf[2 * number + 1, slot].astype(F32)
            reach[slot] += got * (late * decay(between))
            state[slot] = got * take + state[slot] * keep
        low_index = low_index + bit * span
        span *= 2.0
    between = span - 1.0 - low_index if reverse else low_index
    early, later = (1, 0) if reverse else (0, 1)
    reach[later] += state[early] * decay(between)
    state[0] = state[early] * decay(span) + state[later]
    order = [low_index, low_index + span]
    span *= 2.0
    for number, axis in enumerate(plan.high):
        bit = at[axis].astype(F32)
        late = 1.0 - bit if reverse else bit
        high_buf[2 * number] = state[0].astype(BF)
        copy = remote(high_buf.at[2 * number], high_buf.at[2 * number + 1], sends, receives, index, {axis: 1 - at[axis]})
        copy.start()
        copies.append(copy)
        index += 1
        yield
        copy.wait_recv()
        step_decay = decay(span)
        take, keep = late * step_decay + (1.0 - late), late + (1.0 - late) * step_decay
        got = high_buf[2 * number + 1].astype(F32)
        for slot in range(2):
            between = span - 1.0 - order[slot] if reverse else order[slot]
            reach[slot] += got * (late * decay(between))
            order[slot] = order[slot] + bit * span
        state[0] = got * take + state[0] * keep
        span *= 2.0
    for copy in copies:
        copy.wait_send()


def carry_buffers(plan, key_size, value_size):
    return [
        pltpu.VMEM((2, key_size, value_size), F32),
        pltpu.VMEM((2, key_size, value_size), F32),
        pltpu.VMEM((2 * max(len(plan.low), 1), 2, key_size, value_size), BF),
        pltpu.VMEM((2 * max(len(plan.high), 1), key_size, value_size), BF),
    ]


def spread_steps(sq, block, full, sends, receives, base, local_sem):
    rows, width = block.shape
    half = rows // 2
    p, y, c = sq.p, sq.y, sq.c
    top, low = (0, half), (half, half)

    def place(p_, y_, c_, start, count):
        return full.at[p_, pl.ds(start, count), pl.ds(pl.multiple_of((y_ * 2 + c_) * width, width), width)]

    def own(part):
        return block.at[pl.ds(part[0], part[1]), :]

    def send(index, source, target, device):
        copy = remote(source, target, sends, receives, base + index, device)
        copy.start()
        return copy

    def relay(index, p_, y_, part, device):
        return send(index, place(p_, y_, c, *part), place(p_, y_, c, *part), device)

    k0 = send(0, own(top), place(p, y, c, *top), sq.S)
    k2 = send(2, own(low), place(p, y, c, *low), sq.Y)
    k6 = send(6, block, place(p, y, c, 0, rows), sq.C)
    k1 = send(1, own(low), place(p, y, c, *low), sq.S)
    k3 = send(3, own(top), place(p, y, c, *top), sq.Y)
    keep = pltpu.make_async_copy(block, place(p, y, c, 0, rows), local_sem)
    keep.start()
    yield
    k2.wait_recv()
    k4 = relay(4, p, 1 - y, low, sq.S)
    k9 = relay(9, p, 1 - y, low, sq.C)
    k0.wait_recv()
    k5 = relay(5, 1 - p, y, top, sq.Y)
    k7 = relay(7, 1 - p, y, top, sq.C)
    yield
    k1.wait_recv()
    k8 = relay(8, 1 - p, y, low, sq.C)
    k3.wait_recv()
    k10 = relay(10, p, 1 - y, top, sq.C)
    yield
    k5.wait_recv()
    k11 = relay(11, 1 - p, 1 - y, top, sq.C)
    k4.wait_recv()
    k12 = relay(12, 1 - p, 1 - y, low, sq.C)
    for copy in (k6, k7, k8, k9, k10, k11, k12):
        copy.wait_recv()
    for copy in (k0, k1, k2, k3, k4, k5, k6, k7, k8, k9, k10, k11, k12):
        copy.wait_send()
    keep.wait()


def pass_steps(sq, block, full, sends, receives, base, wide):
    rows = full.shape[1]
    width = full.shape[2] // 4
    half = rows // 2
    p, y, c = sq.p, sq.y, sq.c
    parts = ((0, half), (half, half))
    copies = []

    def place(p_, y_, part):
        columns = pl.ds(pl.multiple_of((y_ * 2 + c) * width, width), width)
        return full.at[p_, pl.ds(part[0], part[1]), columns]

    def send(index, source, p_, y_, part, device):
        copy = remote(source, place(p_, y_, part), sends, receives, base + index, device)
        copy.start()
        copies.append(copy)
        return copy

    def own(part):
        return block.at[pl.ds(part[0], part[1]), :]

    far = [send(i, own(part), p, y, part, sq.S) for i, part in enumerate(parts)]
    beside, near = [], []
    if wide:
        beside += [send(2 + i, own(part), p, y, part, sq.Y) for i, part in enumerate(parts)]
        near += [send(4 + i, own(part), p, y, part, sq.C) for i, part in enumerate(parts)]
    yield
    other = []
    for i, part in enumerate(parts):
        far[i].wait_recv()
        other.append(send(6 + i, place(1 - p, y, part), 1 - p, y, part, sq.Y))
        near.append(send(8 + i, place(1 - p, y, part), 1 - p, y, part, sq.C))
    yield
    for i, part in enumerate(parts):
        if wide:
            beside[i].wait_recv()
            near.append(send(10 + i, place(p, 1 - y, part), p, 1 - y, part, sq.C))
        other[i].wait_recv()
        near.append(send(12 + i, place(1 - p, 1 - y, part), 1 - p, 1 - y, part, sq.C))
    yield
    for copy in near:
        copy.wait_recv()
    for copy in copies:
        copy.wait_send()


PASS_COPIES = 14


def reduce_steps(sq, block_of, result, hand, near, total, arrived, sends, receives, base):
    rows, width = result.shape
    half = rows // 2
    p, y, c = sq.p, sq.y, sq.c
    top, low = pl.ds(0, half), pl.ds(half, half)

    def send(index, source, target, device):
        copy = remote(source, target, sends, receives, base + index, device)
        copy.start()
        return copy

    order = ((1 - p, 1 - y), (1 - p, y), (p, 1 - y), (p, y))

    def give(i, p_, y_):
        return remote(hand.at[p_, y_], near.at[p_, y_], sends, receives, base + i, sq.C)

    @pl.loop(0, 4)
    def _(i):
        p_, y_ = (1 - p + i // 2) % 2, (1 - y + i % 2) % 2
        hand[p_, y_] = block_of(p_, y_, 1 - c).astype(BF)
        give(i, p_, y_).start()

    given = [give(i, p_, y_) for i, (p_, y_) in enumerate(order)]

    def join(i):
        p_, y_ = order[i]
        own = block_of(p_, y_, c)
        given[i].wait_recv()
        return own + near[p_, y_].astype(F32)

    total[1 - p, 1 - y] = join(0).astype(BF)
    a = send(4, total.at[1 - p, 1 - y, low], arrived.at[0], sq.S)
    b = send(5, total.at[1 - p, 1 - y, top], arrived.at[1], sq.Y)

    @pl.loop(0, 2)
    def _(i):
        p_, y_ = (1 - p + i) % 2, (y + i) % 2
        own = block_of(p_, y_, c)
        give(1 + i, p_, y_).wait_recv()
        total[p_, y_] = (own + near[p_, y_].astype(F32)).astype(BF)

    e = send(6, total.at[1 - p, y, low], arrived.at[2], sq.S)
    f = send(7, total.at[p, 1 - y, top], arrived.at[3], sq.Y)
    result[...] = join(3)
    yield
    b.wait_recv()
    total[1 - p, y, top] = (total[1 - p, y, top].astype(F32) + arrived[1].astype(F32)).astype(BF)
    g = send(8, total.at[1 - p, y, top], arrived.at[4], sq.S)
    a.wait_recv()
    total[p, 1 - y, low] = (total[p, 1 - y, low].astype(F32) + arrived[0].astype(F32)).astype(BF)
    d = send(9, total.at[p, 1 - y, low], arrived.at[5], sq.Y)
    yield
    e.wait_recv()
    f.wait_recv()
    g.wait_recv()
    result[top, :] += arrived[4].astype(F32) + arrived[3].astype(F32)
    d.wait_recv()
    result[low, :] += arrived[2].astype(F32) + arrived[5].astype(F32)
    for copy in given + [a, b, e, f, g, d]:
        copy.wait_send()


def reduce_room(rows, width):
    return [pltpu.VMEM((2, 2, rows, width), BF)] * 3 + [pltpu.VMEM((6, rows // 2, width), BF)]


def flipped(plan, at, mask):
    return {axis: 1 - at[axis] for i, axis in enumerate(plan.seq) if mask >> i & 1}


def greet_all(plan, at, sq):
    barrier = pltpu.get_barrier_semaphore()
    peers = [flipped(plan, at, mask) for mask in range(1, 1 << len(plan.seq))] + [sq.Y, sq.C, sq.X]
    for peer in peers:
        pl.semaphore_signal(barrier, inc=1, device_id=peer, device_id_type=MESH)
    pl.semaphore_wait(barrier, len(peers))


def column_of(rows, start, sign, rate):
    offset = lax.broadcasted_iota(jnp.int32, (rows, 1), 0).astype(F32)
    return jnp.exp((start + sign * offset) * rate)


def decay_mask(mask, rate):
    rows = mask.shape[0]

    @pl.loop(0, rows // 128)
    def _(i):
        start = pl.multiple_of(i * 128, 128)
        line = lax.broadcasted_iota(jnp.int32, (128, rows), 0) + start
        lane = lax.broadcasted_iota(jnp.int32, (128, rows), 1)
        distance = (line - lane).astype(F32)
        mask[pl.ds(start, 128), :] = jnp.where(distance >= 0, jnp.exp(jnp.maximum(distance, 0.0) * rate), 0.0)


TILE = 256


def row_tiles(full, body):
    rows = full.shape[1]
    each = rows // TILE

    @pl.loop(0, 2 * each)
    def _(i):
        body(i // each, pl.multiple_of(i % each * TILE, TILE), pl.multiple_of(i * TILE, TILE))


def turned(r, slot, start):
    base = r.turn[slot]
    cos_at, sin_at = base[0:1], base[1:2]
    cos_off, sin_off = r.cos_off[pl.ds(start, TILE), :], r.sin_off[pl.ds(start, TILE), :]
    return cos_at * cos_off - sin_at * sin_off, sin_at * cos_off + cos_at * sin_off


def front_kernel(plan, names, *refs):
    r = types.SimpleNamespace(**dict(zip(names, refs)))
    at = {axis: lax.axis_index(axis) for axis in plan.seq + plan.head}
    sq = Square(plan.pair)
    length, model = r.inputs.shape
    width = r.block.shape[1]
    mine = sq.y * 2 + sq.c
    column = pl.multiple_of(mine * width, width)
    rate = r.rate[0:1, 0:1]
    weights = [r.wq, r.wk, r.wv, r.wg, r.wo, r.wu, r.wd]
    key_size, value_size = r.wq.shape[1], r.wv.shape[1]
    saved = []

    def save(source, target):
        copy = pltpu.make_async_copy(source, target, r.save_sem.at[len(saved)])
        copy.start()
        saved.append(copy)

    greet_all(plan, at, sq)
    flip = r.so.shape[0] != r.sq.shape[0]
    outer_shards = [r.so_t, r.sd_t] if flip else [r.so, r.sd]
    shards = [r.sq, r.sk, r.sv, r.sg, outer_shards[0], r.su, outer_shards[1]]
    bulk = Bulk(plan, at, shards, weights, r.bulk_send, r.bulk_receive, r.bulk_local)
    QUERY, KEY, VALUE, GATE, OUT, UP, DOWN = range(7)
    pair, high, low = [bulk.axes[0]], bulk.high, bulk.low

    for row, vector in enumerate((r.gain_one, r.bias_one, r.gain_two, r.bias_two)):
        r.vec[row : row + 1, :] = vector[...].astype(F32)
    r.vec[4:8, :] = jnp.zeros((4, r.vec.shape[1]), F32)
    size = 1 << len(plan.seq)
    copies = []
    for mask in range(1, size):
        copy = remote(r.vec, r.vecs.at[bulk.me], r.vec_send, r.vec_receive, mask, flipped(plan, at, mask))
        copy.start()
        copies.append(copy)
    r.vecs[bulk.me] = r.vec[...]
    bulk.begin(QUERY, bulk.axes)
    bulk.begin(KEY, bulk.axes)
    if flip:
        r.so_t[...] = r.so[...].T
        r.sd_t[...] = r.sd[...].T
    r.cot_bf[...] = r.cot[...].astype(BF)
    for unit in (VALUE, GATE, OUT):
        bulk.begin(unit, low)

    for copy in copies:
        copy.wait_recv()
    step = r.vec.shape[1]
    for j in range(size):
        r.all_gains[:, j * step : (j + 1) * step] = r.vecs[j]
    r.gains[...] = r.all_gains[:, pl.ds(column, width)]

    @pl.loop(0, length // 128)
    def _(i):
        rows = pl.ds(pl.multiple_of(i * 128, 128), 128)
        stream = r.inputs[rows, :]
        mean = jnp.mean(stream, axis=1, keepdims=True)
        inverse = lax.rsqrt(jnp.mean(jnp.square(stream - mean), axis=1, keepdims=True) + EPSILON)
        r.inverse_one[rows, :] = jnp.broadcast_to(inverse, (128, 128))
        normed = (stream - mean) * inverse
        hidden = (normed * r.all_gains[0:1, :] + r.all_gains[1:2, :]).astype(BF)
        r.hidden[sq.p, rows, :] = hidden
        own = (r.inputs[rows, pl.ds(column, width)] - mean) * inverse
        r.normed_one[rows, :] = own
        r.block[rows, :] = (own * r.gains[0:1, :] + r.gains[1:2, :]).astype(BF)

    gains = r.gains[...]
    hid = pass_steps(sq, r.block, r.hidden, r.hid_send, r.hid_receive, 0, False)
    cot = pass_steps(sq, r.cot_bf, r.cot_out, r.cot_send, r.cot_receive, 0, True)
    keep_cot = pltpu.make_async_copy(r.cot_bf, r.cot_out.at[sq.p, :, pl.ds(column, width)], r.local_sem.at[0])
    keep_cot.start()
    next(hid)
    bulk.begin(VALUE, pair + high)
    bulk.paired(QUERY)
    bulk.paired(KEY)
    bulk.first(QUERY)
    bulk.first(KEY)
    bulk.paired(VALUE)
    bulk.begin(GATE, pair + high)
    bulk.begin(OUT, pair + high)
    next(hid)
    decay_mask(r.mask, rate)
    bulk.second(QUERY)
    bulk.second(KEY)
    bulk.first(VALUE)
    next(hid)
    next(hid, None)
    save(r.hidden, r.hidden_out)

    bulk.finish(QUERY)
    bulk.finish(KEY)
    save(r.wq, r.wq_out)
    save(r.wk, r.wk_out)

    def project_keys(slot, start, row):
        hidden = r.hidden[slot, pl.ds(start, TILE), :]
        cosine, sine = turned(r, slot, start)
        for weight, target in ((r.wq, r.q), (r.wk, r.k)):
            value = mm(hidden, weight[...])
            target[pl.ds(row, TILE), :] = rotate(value, cosine, sine).astype(BF)

    row_tiles(r.hidden, project_keys)

    bulk.second(VALUE)
    bulk.paired(GATE)
    bulk.paired(OUT)
    bulk.finish(VALUE)
    save(r.wv, r.wv_out)

    def project_values(slot, start, row):
        r.v[pl.ds(row, TILE), :] = mm(r.hidden[slot, pl.ds(start, TILE), :], r.wv[...]).astype(BF)

    row_tiles(r.hidden, project_values)
    save(r.q, r.q_out)
    save(r.k, r.k_out)
    save(r.v, r.v_out)
    weight_out = column_of(length, float(length), -1.0, rate)
    for slot in range(2):
        rows = slice(slot * length, (slot + 1) * length)
        key = (r.k[rows, :].astype(F32) * weight_out).astype(BF)
        r.state[slot] = t_mm(key, r.v[rows, :])
    carry = carried(
        plan, at, r.state, r.reach, r.low_buf, r.high_buf, rate, length, False, r.carry_send, r.carry_receive, 0
    )
    next(carry)

    def inner(slot, start, row):
        scores = mm_t(r.q[pl.ds(row, TILE), :], r.k[pl.ds(pl.multiple_of(slot * length, length), length), :])
        weights_ = (scores * r.mask[pl.ds(start, TILE), :]).astype(BF)
        r.normed[pl.ds(row, TILE), :] = mm(weights_, r.v[pl.ds(pl.multiple_of(slot * length, length), length), :])

    row_tiles(r.hidden, inner)
    bulk.first(GATE)
    bulk.first(OUT)
    bulk.begin(UP, pair)
    bulk.begin(DOWN, pair)
    next(carry, None)
    bulk.second(GATE)
    bulk.second(OUT)
    bulk.begin(UP, high + low)
    bulk.begin(DOWN, low)
    bulk.finish(GATE)
    save(r.wg, r.wg_out)

    def gates(slot, start, row):
        r.gate[pl.ds(row, TILE), :] = mm(r.hidden[slot, pl.ds(start, TILE), :], r.wg[...])

    row_tiles(r.hidden, gates)
    save(r.gate, r.gate_out)
    bulk.paired(UP, low)
    bulk.paired(DOWN, low)
    for _ in carry:
        pass
    for slot in range(2):
        r.reach_bf[slot] = r.reach[slot].astype(BF)
    save(r.reach_bf, r.reach_out)

    def outer(slot, start, row):
        rows = pl.ds(row, TILE)
        offset = lax.broadcasted_iota(jnp.int32, (TILE, 1), 0) + start
        cross = mm(r.q[rows, :], r.reach_bf[slot]) * jnp.exp(offset.astype(F32) * rate)
        retained = r.normed[rows, :] + cross
        center = retained - jnp.mean(retained, axis=1, keepdims=True)
        inverse = lax.rsqrt(jnp.mean(center * center, axis=1, keepdims=True) + EPSILON)
        value = center * inverse
        r.normed[rows, :] = value
        r.inverse[rows, :] = jnp.broadcast_to(inverse, (TILE, 128))
        gate = r.gate[rows, :]
        r.gated[rows, :] = (gate * jax.nn.sigmoid(gate) * value).astype(BF)

    row_tiles(r.hidden, outer)
    save(r.normed, r.normed_out)
    save(r.inverse, r.inverse_out)
    save(r.gated, r.gated_out)
    bulk.finish(OUT)
    save(r.wo, r.wo_out)

    def out_block(p_, y_, c_):
        rows = pl.ds(pl.multiple_of(p_ * length, length), length)
        return mm_t(r.gated[rows, :], r.wo[pl.ds(pl.multiple_of((y_ * 2 + c_) * width, width), width), :])

    def nothing():
        pass

    def rest_of_up():
        bulk.forward(UP, bulk.bit[pair[0]], high)
        bulk.begin(DOWN, high)

    def rest_of_down():
        bulk.forward(DOWN, bulk.bit[pair[0]], high)
        next(cot)
        bulk.first(UP)

    def second_up():
        bulk.second(UP)
        bulk.first(DOWN)

    reduce = reduce_steps(
        sq, out_block, r.middle, r.hand, r.near, r.total, r.arrived, r.sends, r.receives, SPREAD_COPIES
    )
    together(reduce, nothing, rest_of_up)
    whole = r.middle[...] + r.inputs[:, pl.ds(column, width)]
    r.middle[...] = whole
    mean = jnp.mean(whole, axis=1, keepdims=True)
    deviation = jnp.mean(jnp.square(whole - mean), axis=1, keepdims=True)
    base = SPREAD_COPIES + REDUCE_COPIES
    means, spreads = exchange(sq, mean, deviation, r.stats, r.sends, r.receives, base)
    center = sum(means) * (1.0 / len(means))
    variance = sum(s + jnp.square(m - center) for m, s in zip(means, spreads)) * (1.0 / len(means))
    mean, scale = upright(center, lax.rsqrt(variance + EPSILON))
    r.inverse_two[...] = jnp.broadcast_to(scale, r.inverse_two.shape)
    value = (r.middle[...] - mean) * scale
    r.normed_two[...] = value
    r.block[...] = (value * gains[2:3] + gains[3:4]).astype(BF)
    spread = spread_steps(sq, r.block, r.mid_out, r.sends, r.receives, 0, r.local_sem.at[1])
    together(spread, nothing, rest_of_down, second_up)
    bulk.finish(UP)
    save(r.wu, r.wu_out)
    next(cot)
    bulk.second(DOWN)
    next(cot)
    next(cot, None)
    bulk.finish(DOWN)
    save(r.wd, r.wd_out)
    bulk.drain()
    keep_cot.wait()
    for copy in copies:
        copy.wait_send()
    for copy in saved:
        copy.wait()


def front(plan, shards, inputs, cot, vectors, rate, turn, cos_off, sin_off, number):
    length, model = inputs.shape
    width = cot.shape[1]
    size = 1 << len(plan.seq)
    key_size, value_size, hidden = shards[0].shape[1] // 2, shards[2].shape[1] // 2, shards[5].shape[1] // 2
    any_spec, vmem_spec = pl.BlockSpec(memory_space=pl.ANY), pl.BlockSpec(memory_space=pltpu.VMEM)
    both = 2 * length

    def shape(dims, kind=BF):
        return jax.ShapeDtypeStruct(dims, kind)

    sq, sk, sv, sg, so, su, sd = shards
    rows = sq.shape[0]
    flip = rows % 128 == 0
    if not flip:
        so, sd = so.T, sd.T
    far = dict(sq=sq, sk=sk, sv=sv, sg=sg, su=su)
    near = dict(so=so, sd=sd, inputs=inputs, cot=cot, rate=rate, turn=turn, cos_off=cos_off, sin_off=sin_off)
    gain_one, bias_one, gain_two, bias_two = [v[None] for v in vectors]
    near.update(gain_one=gain_one, bias_one=bias_one, gain_two=gain_two, bias_two=bias_two)
    wq, wk, wv, wg, wu = [(model, s.shape[1] // 2) for s in far.values()]
    wo, wd = (model, value_size), (model, hidden)
    far_outs = dict(
        wq_out=shape(wq),
        wk_out=shape(wk),
        wv_out=shape(wv),
        wg_out=shape(wg),
        wo_out=shape(wo),
        wu_out=shape(wu),
        wd_out=shape(wd),
        hidden_out=shape((2, length, model)),
        cot_out=shape((2, length, model)),
        mid_out=shape((2, length, model)),
        q_out=shape((both, key_size)),
        k_out=shape((both, key_size)),
        v_out=shape((both, value_size)),
        reach_out=shape((2, key_size, value_size)),
        gate_out=shape((both, value_size), F32),
        normed_out=shape((both, value_size), F32),
        inverse_out=shape((both, 128), F32),
        gated_out=shape((both, value_size)),
    )
    near_outs = dict(
        middle=shape((length, width), F32),
        normed_one=shape((length, width), F32),
        inverse_one=shape((length, 128), F32),
        normed_two=shape((length, width), F32),
        inverse_two=shape((length, 128), F32),
        gains=shape((8, width), F32),
    )
    carries = carry_buffers(plan, key_size, value_size)
    count = SPREAD_COPIES + REDUCE_COPIES + 3
    dma = pltpu.SemaphoreType.DMA
    hand, near_room, total, arrived = reduce_room(length, width)
    scratch = dict(
        so_t=pltpu.VMEM((rows, 2 * value_size) if flip else (16, 128), BF),
        sd_t=pltpu.VMEM((rows, 2 * hidden) if flip else (16, 128), BF),
        cot_bf=pltpu.VMEM((length, width), BF),
        wq=pltpu.VMEM(wq, BF),
        wk=pltpu.VMEM(wk, BF),
        wv=pltpu.VMEM(wv, BF),
        wg=pltpu.VMEM(wg, BF),
        wo=pltpu.VMEM(wo, BF),
        wu=pltpu.VMEM(wu, BF),
        wd=pltpu.VMEM(wd, BF),
        hidden=pltpu.VMEM((2, length, model), BF),
        block=pltpu.VMEM((length, width), BF),
        q=pltpu.VMEM((both, key_size), BF),
        k=pltpu.VMEM((both, key_size), BF),
        v=pltpu.VMEM((both, value_size), BF),
        gate=pltpu.VMEM((both, value_size), F32),
        normed=pltpu.VMEM((both, value_size), F32),
        inverse=pltpu.VMEM((both, 128), F32),
        gated=pltpu.VMEM((both, value_size), BF),
        mask=pltpu.VMEM((length, length), F32),
        state=carries[0],
        reach=carries[1],
        low_buf=carries[2],
        high_buf=carries[3],
        reach_bf=pltpu.VMEM((2, key_size, value_size), BF),
        vec=pltpu.VMEM((8, rows), F32),
        vecs=pltpu.VMEM((size, 8, rows), F32),
        stats=pltpu.VMEM((4, 8, length), F32),
        hand=hand,
        near=near_room,
        total=total,
        arrived=arrived,
        bulk_send=dma((7 * size,)),
        bulk_receive=dma((7 * size,)),
        bulk_local=dma((7,)),
        vec_send=dma((size,)),
        vec_receive=dma((size,)),
        carry_send=dma((len(plan.seq),)),
        carry_receive=dma((len(plan.seq),)),
        all_gains=pltpu.VMEM((8, model), F32),
        hid_send=dma((PASS_COPIES,)),
        hid_receive=dma((PASS_COPIES,)),
        cot_send=dma((PASS_COPIES,)),
        cot_receive=dma((PASS_COPIES,)),
        sends=dma((count,)),
        receives=dma((count,)),
        local_sem=dma((3,)),
        save_sem=dma((32,)),
    )
    names = list(far) + list(near) + list(far_outs) + list(near_outs) + list(scratch)
    results = pl.pallas_call(
        functools.partial(front_kernel, plan, names),
        out_shape=tuple(far_outs.values()) + tuple(near_outs.values()),
        in_specs=[any_spec] * len(far) + [vmem_spec] * len(near),
        out_specs=(any_spec,) * len(far_outs) + (vmem_spec,) * len(near_outs),
        scratch_shapes=list(scratch.values()),
        compiler_params=pltpu.CompilerParams(
            collective_id=number, has_side_effects=True, vmem_limit_bytes=VMEM_LIMIT
        ),
        name="front",
    )(*far.values(), *near.values())
    return types.SimpleNamespace(**dict(zip(list(far_outs) + list(near_outs), results)))


SLOT = (1, 0, 2, 0, 3, None)


class Return:
    def __init__(self, plan, at, totals, spare, got, sends, receives):
        self.at, self.totals, self.spare, self.got = at, totals, spare, got
        self.sends, self.receives = sends, receives
        self.order = plan.low + list(reversed(plan.high)) + [plan.pair]
        self.bit = {axis: 1 << i for i, axis in enumerate(plan.seq)}
        self.size = 1 << len(plan.seq)
        self.me = sum(at[axis] * self.bit[axis] for axis in self.order)
        self.copies = {}

    def stage_of(self, mask):
        for stage, axis in enumerate(self.order):
            if mask & self.bit[axis]:
                return stage
        return len(self.order)

    def masks(self, stage):
        found = [m for m in range(1, self.size) if self.stage_of(m) == stage]
        return sorted(found, key=lambda m: (self.stage_of(m ^ self.bit[self.order[stage]]), m))

    def link(self, unit, mask, axis=None):
        axis = axis or self.order[self.stage_of(mask)]
        return remote(
            self.total(unit, mask),
            self.got.at[unit, mask - 1],
            self.sends,
            self.receives,
            unit * self.size + mask,
            {axis: 1 - self.at[axis]},
        )

    def total(self, unit, mask):
        rows, columns = self.got.shape[2:]
        if SLOT[unit] is None:
            across, down = self.spare.shape[2] // columns, self.spare.shape[1] // rows
            tile = self.spare.at[mask // (across * down)]
            return tile.at[pl.ds(mask // across % down * rows, rows), pl.ds(mask % across * columns, columns)]
        return self.totals.at[SLOT[unit], pl.ds(mask * rows, rows), :]

    def send(self, unit, mask):
        copy = self.link(unit, mask)
        copy.start()
        self.copies[unit, mask] = copy

    def made(self, unit, mask):
        if self.stage_of(mask) == 0:
            self.send(unit, mask)

    def ahead(self, stage):
        bit = self.bit[self.order[stage]]
        masks = self.masks(stage)
        first = [m for m in masks if m ^ bit and self.stage_of(m ^ bit) == stage + 1]
        return first, [m for m in masks if m not in first]

    def collect(self, unit, stage, masks):
        axis = self.order[stage]
        for mask in masks:
            target = mask ^ self.bit[axis]
            self.link(unit, mask).wait_recv()
            total, got = self.total(unit, target), self.got.at[unit, mask - 1]

            @pl.loop(0, total.shape[0] // 64)
            def _(i, total=total, got=got):
                rows = pl.ds(pl.multiple_of(i * 64, 64), 64)
                total[rows, :] = (total[rows, :].astype(F32) + got[rows, :].astype(F32)).astype(BF)

            if self.stage_of(target) == stage + 1 and target:
                self.send(unit, target)

    def early(self, unit):
        self.collect(unit, 0, self.ahead(0)[0])

    def late(self, unit):
        self.collect(unit, 0, self.ahead(0)[1])

    def middle(self, unit):
        for stage in range(1, len(self.order) - 1):
            self.collect(unit, stage, self.masks(stage))

    def last(self, unit):
        return self.got.at[unit, self.bit[self.order[-1]] - 1]

    def last_arrived(self, unit):
        self.link(unit, self.bit[self.order[-1]]).wait_recv()

    def clear(self, unit):
        for (number, _), copy in self.copies.items():
            if number == unit:
                copy.wait_send()


def back_kernel(plan, names, *refs):
    r = types.SimpleNamespace(**dict(zip(names, refs)))
    at = {axis: lax.axis_index(axis) for axis in plan.seq + plan.head}
    sq = Square(plan.pair)
    length, width = r.cot.shape
    key_size, value_size = r.q.shape[1], r.v.shape[1]
    mine = sq.y * 2 + sq.c
    rate = r.rate[0:1, 0:1]
    UP, DOWN, OUT, GATE, VALUE, KEYS = range(6)
    back = Return(plan, at, r.totals, r.tiles, r.got, r.bulk_send, r.bulk_receive)
    piece, model = r.got.shape[2], r.mid.shape[2]
    strip = r.strips.shape[2]
    per_strip = strip // piece

    loads = {}

    def load(name, source, target):
        copy = pltpu.make_async_copy(source, target, r.load_sem.at[len(loads)])
        copy.start()
        loads[name] = copy

    def ready(*wanted):
        for name in wanted:
            loads[name].wait()

    load("wu", r.wu, r.weights.at[0])
    load("wd", r.wd, r.weights.at[1])

    parts = model // value_size

    def tile_copy(source, i):
        each = length // TILE
        rows = source.at[i // each, pl.ds(i % each * TILE, TILE), :]
        return [pltpu.make_async_copy(rows, r.tiles.at[i % 2], r.tile_sem.at[i % 2, 0])]

    def cot_tile(i, part):
        rows = pl.ds(pl.multiple_of((i % 2 * parts + part) * TILE, TILE), TILE)
        return r.totals.at[r.totals.shape[0] - 1, rows, :]

    def cot_copy(i):
        each = length // TILE
        return [
            pltpu.make_async_copy(
                r.cotf.at[i // each, pl.ds(i % each * TILE, TILE), pl.ds(part * value_size, value_size)],
                cot_tile(i, part),
                r.tile_sem.at[i % 2, 1 + part],
            )
            for part in range(parts)
        ]

    def start(copies):
        for copy in copies:
            copy.start()

    def wait(copies):
        for copy in copies:
            copy.wait()

    tile_count = 2 * length // TILE
    start(tile_copy(r.mid, 0) + cot_copy(0))
    greet_all(plan, at, sq)
    load("wo", r.wo, r.weights.at[2])
    load("gated", r.gated_in, r.gated)
    load("gate", r.gate_in, r.gate)
    load("normed", r.normed_in, r.normed)
    load("inverse", r.inverse_in, r.inverse)
    load("q", r.q_in, r.q)
    load("k", r.k_in, r.k)
    load("v", r.v_in, r.v)
    load("reach", r.reach_in, r.in_bf)
    load("middle", r.middle_in, r.layer_out)
    ready("wu", "wd")

    @pl.loop(0, tile_count)
    def _(i):
        @pl.when(i + 1 < tile_count)
        def _():
            start(tile_copy(r.mid, i + 1) + cot_copy(i + 1))

        wait(tile_copy(r.mid, i) + cot_copy(i))
        rows = pl.ds(pl.multiple_of(i * TILE, TILE), TILE)
        preact = mm(r.tiles[i % 2], r.weights[0])
        cdf = 0.5 * (1.0 + lax.erf(preact * 0.7071067811865476))
        slope = cdf + preact * (jnp.exp(-0.5 * preact * preact) * 0.3989422804014327)
        r.hidden_ff[rows, :] = (preact * cdf).astype(BF)
        grad = sum(
            mm(cot_tile(i, part)[...], r.weights[1, part * value_size : (part + 1) * value_size, :])
            for part in range(parts)
        )
        r.grad_pre[rows, :] = (grad * slope).astype(BF)

    def strip_copy(source, mask, number):
        start = pl.multiple_of((back.me ^ mask) // per_strip * strip, strip)
        half = r.strips.at[number % 2]
        return [
            pltpu.make_async_copy(
                source.at[slot, :, pl.ds(start, strip)],
                half.at[pl.ds(slot * length, length), :],
                r.strip_sem.at[number % 2, slot],
            )
            for slot in range(2)
        ]

    def produce(unit, source, grads, masks):
        count = len(masks)
        step = masks[1] - masks[0] if count > 1 else 0
        even = all(mask == masks[0] + number * step for number, mask in enumerate(masks))

        def one(number, mask):
            for copy in strip_copy(source, mask, number):
                copy.wait()
            value = t_mm(r.strips[number % 2], grads[...])
            if per_strip > 1:
                r.whole_strip[...] = value
                inside = pl.multiple_of((back.me ^ mask) % per_strip * piece, piece)
                value = r.whole_strip[pl.ds(inside, piece), :]
            back.total(unit, mask)[...] = value.astype(BF)

        for copy in strip_copy(source, masks[0], 0):
            copy.start()
        if even:

            @pl.loop(0, count)
            def _(number):
                @pl.when(number + 1 < count)
                def _():
                    for copy in strip_copy(source, masks[0] + (number + 1) * step, number + 1):
                        copy.start()

                mask = masks[0] + number * step
                one(number, mask)
                if back.stage_of(masks[0]) == 0:
                    back.link(unit, mask, back.order[0]).start()

            for mask in masks:
                if back.stage_of(mask) == 0:
                    back.copies[unit, mask] = back.link(unit, mask)
        else:
            for number, mask in enumerate(masks):
                if number + 1 < count:
                    for copy in strip_copy(source, masks[number + 1], number + 1):
                        copy.start()
                one(number, mask)
                back.made(unit, mask)

    away_first, away_rest = back.ahead(0)
    low_bit = back.bit[back.order[0]]
    home_first, home_rest = ([m ^ low_bit for m in masks] for masks in (away_first, away_rest))

    def blocks(grads, weight):
        def block_of(p_, y_, c_):
            rows = pl.ds(pl.multiple_of(p_ * length, length), length)
            columns = pl.ds(pl.multiple_of((y_ * 2 + c_) * width, width), width)
            return sum(mm_t(g[rows, :], r.weights[w, columns, :]) for g, w in zip(grads, weight))

        return block_of

    def reduce(grads, weight, result, base):
        return reduce_steps(
            sq, blocks(grads, weight), result, r.hand, r.near, r.near, r.arrived, r.sends, r.receives, base
        )

    emitted = {}

    def emit(unit):
        own = at[plan.pair]
        back.last_arrived(unit)
        emitted[unit] = [
            pltpu.make_async_copy(source, r.halves.at[unit, half], r.emit_sem.at[unit, number])
            for number, (half, source) in enumerate(((own, back.total(unit, 0)), (1 - own, back.last(unit))))
        ]
        start(emitted[unit])

    def clear(unit):
        back.clear(unit)
        wait(emitted[unit])

    def norm_sums(upstream, gain, normed, inverse, base_stream, result, row, stats, base):
        value = upstream[...]
        product = value * normed[...]
        r.sums[row : row + 1, :] = jnp.sum(product, axis=0, keepdims=True)
        r.sums[row + 1 : row + 2, :] = jnp.sum(value, axis=0, keepdims=True)
        first = jnp.mean(value * gain, axis=1, keepdims=True)
        second = jnp.mean(product * gain, axis=1, keepdims=True)
        firsts, seconds = exchange(sq, first, second, stats, r.sends, r.receives, base)
        share = 1.0 / len(firsts)
        first, second = upright(sum(firsts) * share, sum(seconds) * share)
        result[...] = base_stream[...] + inverse[:, 0:1] * (upstream[...] * gain - first - normed[...] * second)

    def down_last():
        produce(DOWN, r.cotf, r.hidden_ff, away_rest)
        produce(DOWN, r.cotf, r.hidden_ff, home_first)
        produce(UP, r.mid, r.grad_pre, away_first)

    base = SPREAD_COPIES
    together(
        reduce([r.grad_pre], [0], r.upstream, base),
        lambda: produce(DOWN, r.cotf, r.hidden_ff, away_first),
        down_last,
    )
    base += REDUCE_COPIES
    back.early(DOWN)
    load("wv", r.wv, r.weights.at[0])
    norm_sums(r.upstream, r.gains[2:3, :], r.normed_two, r.inverse_two, r.cot, r.grad_middle, 2, r.stats, base)
    base += 3
    block = r.hand.at[0, 0]
    block[...] = r.grad_middle[...].astype(BF)

    def up_next():
        produce(UP, r.mid, r.grad_pre, away_rest)
        produce(DOWN, r.cotf, r.hidden_ff, home_rest)

    def up_last():
        back.late(DOWN)
        produce(UP, r.mid, r.grad_pre, home_rest)

    together(
        spread_steps(sq, block, r.gmid, r.sends, r.receives, 0, r.local_sem.at[0]),
        up_next,
        lambda: produce(UP, r.mid, r.grad_pre, home_first),
    )
    up_last()
    ready("wo", "gated", "gate", "normed", "inverse")
    back.early(UP)

    start(tile_copy(r.gmid, 0))
    @pl.loop(0, tile_count)
    def _(i):
        @pl.when(i + 1 < tile_count)
        def _():
            start(tile_copy(r.gmid, i + 1))

        wait(tile_copy(r.gmid, i))
        rows = pl.ds(pl.multiple_of(i * TILE, TILE), TILE)
        grad = mm(r.tiles[i % 2], r.weights[2])
        gate = r.gate[rows, :]
        normed = r.normed[rows, :]
        logistic = jax.nn.sigmoid(gate)
        swish = gate * logistic
        r.grad_gate[rows, :] = (grad * normed * (logistic + swish * (1.0 - logistic))).astype(BF)
        scaled = grad * swish
        r.grad_mixed[rows, :] = (
            r.inverse[rows, 0:1]
            * (
                scaled
                - jnp.mean(scaled, axis=1, keepdims=True)
                - normed * jnp.mean(scaled * normed, axis=1, keepdims=True)
            )
        ).astype(BF)
    load("wg", r.wg, r.weights.at[2])
    back.middle(DOWN)

    ready("q", "k", "v", "reach")
    decay_mask(r.mask, rate)
    weight_out = column_of(length, 1.0, 1.0, rate)
    for slot in range(2):
        rows = slice(slot * length, (slot + 1) * length)
        query = (r.q[rows, :].astype(F32) * weight_out).astype(BF)
        r.state[slot] = t_mm(query, r.grad_mixed[rows, :])
    carry = carried(
        plan, at, r.state, r.reach, r.low_buf, r.high_buf, rate, length, True, r.carry_send, r.carry_receive, 0
    )
    next(carry)
    produce(OUT, r.gmid, r.gated, away_first)
    weight_in = column_of(length, 0.0, 1.0, rate)
    weight_back = column_of(length, length - 1.0, -1.0, rate)

    def rotated_back(value, slot):
        base_ = r.turn[slot]
        cosine = base_[0:1] * r.cos_off[...] - base_[1:2] * r.sin_off[...]
        sine = base_[1:2] * r.cos_off[...] + base_[0:1] * r.sin_off[...]
        return unrotate(value, cosine, sine)

    @pl.loop(0, 2)
    def _(slot):
        rows = pl.ds(pl.multiple_of(slot * length, length), length)
        weights = (mm_t(r.grad_mixed[rows, :], r.v[rows, :]) * r.mask[...]).astype(BF)
        value = mm(weights, r.k[rows, :]) + mm_t(r.grad_mixed[rows, :], r.in_bf[slot]) * weight_in
        r.grad_keys[rows, 0:key_size] = rotated_back(value, slot).astype(BF)
        r.gate[rows, 0:key_size] = t_mm(weights, r.q[rows, :])
        weights = (mm_t(r.q[rows, :], r.k[rows, :]) * r.mask[...]).astype(BF)
        r.normed[rows, :] = t_mm(weights, r.grad_mixed[rows, :])

    produce(OUT, r.gmid, r.gated, away_rest)
    next(carry, None)
    feed = reduce([r.hidden_ff], [1], r.grad_inputs, base)
    base += REDUCE_COPIES
    next(feed)
    load("wk", r.wk, r.weights.at[1, :, pl.ds(key_size, key_size)])
    load("wq", r.wq, r.weights.at[1, :, pl.ds(0, key_size)])
    emit(DOWN)
    clear(DOWN)
    produce(GATE, r.hid, r.grad_gate, away_first)
    produce(OUT, r.gmid, r.gated, home_first)
    back.early(OUT)
    next(feed)
    produce(GATE, r.hid, r.grad_gate, away_rest)
    back.late(UP)
    for _ in carry:
        pass
    out_bf = r.low_buf.at[0]
    for slot in range(2):
        out_bf[slot] = r.reach[slot].astype(BF)

    @pl.loop(0, 2)
    def _(slot):
        rows = pl.ds(pl.multiple_of(slot * length, length), length)
        value = r.gate[rows, 0:key_size] + mm_t(r.v[rows, :], out_bf[slot]) * weight_back
        r.grad_keys[rows, key_size : 2 * key_size] = rotated_back(value, slot).astype(BF)
        value = r.normed[rows, :] + mm(r.k[rows, :], out_bf[slot]) * weight_back
        r.grad_pre[rows, :] = value.astype(BF)

    produce(VALUE, r.hid, r.grad_pre, away_first)
    produce(KEYS, r.hid, r.grad_keys, away_first)
    produce(VALUE, r.hid, r.grad_pre, away_rest)
    produce(KEYS, r.hid, r.grad_keys, away_rest)
    for _ in feed:
        pass
    normed_one = r.gate.at[pl.ds(0, length), :]
    load("normed_one", r.normed_one_in, normed_one)
    peers = (sq.S, sq.Y, sq.C)
    for number, peer in enumerate(peers):
        pl.semaphore_signal(r.again.at[number], inc=1, device_id=peer, device_id_type=MESH)
    ready("middle")
    r.layer_out[...] += r.grad_inputs[...]
    back.middle(UP)
    produce(GATE, r.hid, r.grad_gate, home_first)
    back.early(GATE)
    produce(OUT, r.gmid, r.gated, home_rest)
    back.late(OUT)
    back.middle(OUT)
    for number in range(len(peers)):
        pl.semaphore_wait(r.again.at[number], 1)

    ready("wv", "wg", "wk", "wq", "normed_one")

    def value_next():
        produce(VALUE, r.hid, r.grad_pre, home_first)
        back.early(VALUE)
        produce(KEYS, r.hid, r.grad_keys, home_first)

    def keys_next():
        back.early(KEYS)
        produce(GATE, r.hid, r.grad_gate, home_rest)
        back.late(GATE)
        back.middle(GATE)

    together(
        reduce([r.grad_keys, r.grad_pre, r.grad_gate], [1, 0, 2], r.upstream, base),
        value_next,
        keys_next,
    )
    base += REDUCE_COPIES
    norm_sums(r.upstream, r.gains[0:1, :], normed_one, r.inverse_one, r.grad_middle, r.grad_inputs, 0, r.stats_two, base)
    base += 3

    copies = []
    r.all_sums[back.me] = r.sums[...]
    for mask in range(1, back.size):
        copy = remote(r.sums, r.all_sums.at[back.me], r.sum_send, r.sum_receive, mask, flipped(plan, at, mask))
        copy.start()
        copies.append(copy)
    produce(VALUE, r.hid, r.grad_pre, home_rest)
    produce(KEYS, r.hid, r.grad_keys, home_rest)
    back.late(VALUE)
    back.late(KEYS)
    emit(UP)
    back.middle(VALUE)
    emit(OUT)
    back.middle(KEYS)
    emit(GATE)
    for copy in copies:
        copy.wait_recv()
    total = r.all_sums[0]
    for i in range(1, back.size):
        total = total + r.all_sums[i]
    r.by_block[mine] = total
    for index, device in enumerate((sq.Y, sq.C, sq.X)):
        copy = remote(r.by_block.at[mine], r.by_block.at[mine], r.sends, r.receives, base + index, device)
        copy.start()
        copies.append(copy)
    for copy in copies[-3:]:
        copy.wait_recv()
    r.sums_out[...] = r.by_block[back.me * piece // width]
    for copy in copies:
        copy.wait_send()
    emit(VALUE)
    emit(KEYS)
    for unit in (UP, OUT, GATE, VALUE, KEYS):
        clear(unit)


def back_pass(plan, f, cot, rate, turn, cos_off, sin_off, rows, number):
    length, width = cot.shape
    size = 1 << len(plan.seq)
    model = f.wq_out.shape[0]
    key_size, value_size = f.q_out.shape[1], f.v_out.shape[1]
    hidden = f.wu_out.shape[1]
    both = 2 * length
    any_spec, vmem_spec = pl.BlockSpec(memory_space=pl.ANY), pl.BlockSpec(memory_space=pltpu.VMEM)

    def shape(dims, kind=F32):
        return jax.ShapeDtypeStruct(dims, kind)

    far = dict(
        wq=f.wq_out,
        wk=f.wk_out,
        wv=f.wv_out,
        wg=f.wg_out,
        wo=f.wo_out,
        wu=f.wu_out,
        wd=f.wd_out,
        hid=f.hidden_out,
        mid=f.mid_out,
        cotf=f.cot_out,
        q_in=f.q_out,
        k_in=f.k_out,
        v_in=f.v_out,
        reach_in=f.reach_out,
        gate_in=f.gate_out,
        normed_in=f.normed_out,
        inverse_in=f.inverse_out,
        gated_in=f.gated_out,
        middle_in=f.middle,
        normed_one_in=f.normed_one,
    )
    near = dict(
        cot=cot,
        inverse_one=f.inverse_one,
        normed_two=f.normed_two,
        inverse_two=f.inverse_two,
        gains=f.gains,
        rate=rate,
        turn=turn,
        cos_off=cos_off,
        sin_off=sin_off,
    )
    far_outs = dict(halves=shape((6, 2, rows, value_size), BF), gmid=shape((2, length, model), BF))
    near_outs = dict(
        layer_out=shape((length, width)), grad_inputs=shape((length, width)), sums_out=shape((8, width))
    )
    carries = carry_buffers(plan, key_size, value_size)
    dma = pltpu.SemaphoreType.DMA
    count = SPREAD_COPIES + 3 * REDUCE_COPIES + 9
    strip = max(rows, 128)
    hand, near_room, _, arrived = reduce_room(length, width)
    scratch = dict(
        weights=pltpu.VMEM((3, model, value_size), BF),
        tiles=pltpu.VMEM((2, TILE, model), BF),
        strips=pltpu.VMEM((2, both, strip), BF),
        q=pltpu.VMEM((both, key_size), BF),
        k=pltpu.VMEM((both, key_size), BF),
        v=pltpu.VMEM((both, value_size), BF),
        gate=pltpu.VMEM((both, value_size), F32),
        normed=pltpu.VMEM((both, value_size), F32),
        inverse=pltpu.VMEM((both, 128), F32),
        gated=pltpu.VMEM((both, value_size), BF),
        in_bf=pltpu.VMEM((2, key_size, value_size), BF),
        mask=pltpu.VMEM((length, length), F32),
        state=carries[0],
        reach=carries[1],
        low_buf=carries[2],
        high_buf=carries[3],
        hidden_ff=pltpu.VMEM((both, hidden), BF),
        grad_pre=pltpu.VMEM((both, hidden), BF),
        grad_gate=pltpu.VMEM((both, value_size), BF),
        grad_mixed=pltpu.VMEM((both, value_size), BF),
        grad_keys=pltpu.VMEM((both, 2 * key_size), BF),
        upstream=pltpu.VMEM((length, width), F32),
        grad_middle=pltpu.VMEM((length, width), F32),
        hand=hand,
        near=near_room,
        arrived=arrived,
        totals=pltpu.VMEM((4, model, value_size), BF),
        got=pltpu.VMEM((6, size - 1, rows, value_size), BF),
        stats=pltpu.VMEM((4, 8, length), F32),
        stats_two=pltpu.VMEM((4, 8, length), F32),
        sums=pltpu.VMEM((8, width), F32),
        all_sums=pltpu.VMEM((size, 8, width), F32),
        by_block=pltpu.VMEM((4, 8, width), F32),
        whole_strip=pltpu.VMEM((strip, value_size) if strip > rows else (8, 128), F32),
        bulk_send=dma((6 * size,)),
        bulk_receive=dma((6 * size,)),
        load_sem=dma((24,)),
        tile_sem=dma((2, 1 + model // value_size)),
        strip_sem=dma((2, 2)),
        emit_sem=dma((6, 2)),
        carry_send=dma((len(plan.seq),)),
        carry_receive=dma((len(plan.seq),)),
        sum_send=dma((size,)),
        sum_receive=dma((size,)),
        sends=dma((count,)),
        receives=dma((count,)),
        local_sem=dma((1,)),
        again=pltpu.SemaphoreType.REGULAR((3,)),
    )
    names = list(far) + list(near) + list(far_outs) + list(near_outs) + list(scratch)

    def kernel(*refs):
        back_kernel(plan, names, *refs)

    results = pl.pallas_call(
        kernel,
        out_shape=tuple(far_outs.values()) + tuple(near_outs.values()),
        in_specs=[any_spec] * len(far) + [vmem_spec] * len(near),
        out_specs=(any_spec,) * len(far_outs) + (vmem_spec,) * len(near_outs),
        scratch_shapes=list(scratch.values()),
        compiler_params=pltpu.CompilerParams(
            collective_id=number, has_side_effects=True, vmem_limit_bytes=VMEM_LIMIT
        ),
        name="back",
    )(*far.values(), *near.values())
    out = types.SimpleNamespace(**dict(zip(list(far_outs) + list(near_outs), results)))
    return finish(out, key_size)


def finish_kernel(key_size, halves, layer_in, grad_in, *refs):
    *outs, layer_out, grad_out = refs[:9]
    *stages, layer, grad, sems = refs[9:]
    loads = [
        pltpu.make_async_copy(source, stage, sems.at[number])
        for number, (source, stage) in enumerate(((layer_in, layer), (grad_in, grad)))
    ]
    for copy in loads:
        copy.start()
    stores = []

    def store(stage, target):
        copy = pltpu.make_async_copy(stage, target, sems.at[2 + len(stores)])
        copy.start()
        stores.append(copy)

    rows, columns = halves.shape[2:]
    for out, stage, unit, first, width in zip(
        outs, stages, (5, 5, 4, 3, 0, 2, 1), (0, key_size, 0, 0, 0, 0, 0), (key_size,) * 2 + (columns,) * 5
    ):
        for half in range(2):
            value = halves[unit, half, :, first : first + width].astype(F32)
            if out.shape[0] == rows:
                stage[:, half * width : (half + 1) * width] = value
            else:
                stage[half * width : (half + 1) * width, :] = value.T
        store(stage, out)
    for copy, stage, out in zip(loads, (layer, grad), (layer_out, grad_out)):
        copy.wait()
        store(stage, out)
    for copy in stores:
        copy.wait()


def finish(b, key_size):
    rows, value_size = b.halves.shape[2:]
    turned = rows % 128 == 0
    flat = [(rows, 2 * w) for w in (key_size, key_size, value_size, value_size, value_size)]
    shapes = flat + [(2 * value_size, rows) if turned else (rows, 2 * value_size)] * 2 + [b.layer_out.shape] * 2
    any_spec = pl.BlockSpec(memory_space=pl.ANY)
    results = pl.pallas_call(
        functools.partial(finish_kernel, key_size),
        out_shape=tuple(jax.ShapeDtypeStruct(s, F32) for s in shapes),
        in_specs=[pl.BlockSpec(memory_space=pltpu.VMEM), any_spec, any_spec],
        out_specs=tuple([any_spec] * len(shapes)),
        scratch_shapes=[pltpu.VMEM(s, F32) for s in shapes] + [pltpu.SemaphoreType.DMA((2 + len(shapes),))],
        name="finish",
    )(b.halves, b.layer_out, b.grad_inputs)
    gq, gk, gv, gg, gu, go, gd, layer_out, grad_inputs = results
    if not turned:
        go, gd = go.T, gd.T
    return types.SimpleNamespace(
        gq=gq, gk=gk, gv=gv, gg=gg, gu=gu, go=go, gd=gd, layer_out=layer_out, grad_inputs=grad_inputs, sums_out=b.sums_out
    )


def rotate(values, cosine, sine):
    half = values.shape[1] // 2
    first, second = values[:, :half], values[:, half:]
    return jnp.concatenate([first * cosine - second * sine, first * sine + second * cosine], axis=1)


def unrotate(values, cosine, sine):
    half = values.shape[1] // 2
    first, second = values[:, :half], values[:, half:]
    return jnp.concatenate([first * cosine + second * sine, second * cosine - first * sine], axis=1)


def on_device(
    plan,
    inputs,
    decay_exponent,
    first_gain,
    first_bias,
    query_weight,
    key_weight,
    value_weight,
    gate_weight,
    out_weight,
    second_gain,
    second_bias,
    up_weight,
    down_weight,
    cotangent,
):
    length, model = inputs.shape
    rows = query_weight.shape[0]
    pair_bit = lax.axis_index(plan.pair)
    column = lax.axis_index(plan.head_axes)
    width = cotangent.shape[1]

    key_size = query_weight.shape[1] // 2
    value_size = value_weight.shape[1] // 2
    hidden = up_weight.shape[1] // 2

    vectors = (first_gain, first_bias, second_gain, second_bias)

    exponent = jnp.where(pair_bit == 0, decay_exponent[0], decay_exponent[1]).astype(F32)
    lograte = jnp.log1p(-jnp.exp2(-exponent))
    offset = jnp.arange(length, dtype=F32)
    seq_index = lax.axis_index(plan.seq_axes)
    pair_weight = 2 ** plan.seq.index(plan.pair)
    first_slot = seq_index - pair_bit * pair_weight
    starts = jnp.stack([first_slot, first_slot + pair_weight]) * length
    frequency = np.exp(-math.log(10000.0) * np.arange(key_size // 2, dtype=np.float32) / (key_size // 2 - 1))
    frequency = frequency.astype(np.float32)
    angles = np.arange(length)[:, None] * frequency.astype(np.float64)[None, :]
    cos_off, sin_off = jnp.asarray(np.cos(angles), F32), jnp.asarray(np.sin(angles), F32)
    start_angles = starts.astype(F32)[:, None] * frequency[None, :]
    turn = jnp.stack([jnp.cos(start_angles), jnp.sin(start_angles)] * 4, axis=1)
    shards = [query_weight, key_weight, value_weight, gate_weight, out_weight, up_weight, down_weight]
    rate = jnp.full((8, 128), lograte, F32)
    f = front(plan, shards, inputs, cotangent, vectors, rate, turn, cos_off, sin_off, 1)
    b = back_pass(plan, f, cotangent, rate, turn, cos_off, sin_off, rows, 2)
    place = seq_index % (width // rows) * rows
    mine = lax.dynamic_slice_in_dim(b.sums_out, place, rows, 1)
    return (
        b.layer_out,
        b.grad_inputs,
        mine[0],
        mine[1],
        b.gq,
        b.gk,
        b.gv,
        b.gg,
        b.go,
        mine[2],
        mine[3],
        b.gu,
        b.gd,
    )


def solution(mesh):
    seq_bits = (mesh.shape["seq"]).bit_length() - 1
    head_bits = (mesh.shape["head"]).bit_length() - 1
    plan = Plan(seq_bits, head_bits)
    seq, head = plan.seq_axes, plan.head_axes
    fine = Mesh(mesh.devices.reshape((2,) * (seq_bits + head_bits)), seq + head)
    in_specs = (
        P(seq, None),
        P(head),
        P(seq),
        P(seq),
        P(seq, head),
        P(seq, head),
        P(seq, head),
        P(seq, head),
        P(head, seq),
        P(seq),
        P(seq),
        P(seq, head),
        P(head, seq),
        P(seq, head),
    )
    out_specs = (
        P(seq, head),
        P(seq, head),
        P(seq),
        P(seq),
        P(seq, head),
        P(seq, head),
        P(seq, head),
        P(seq, head),
        P(head, seq),
        P(seq),
        P(seq),
        P(seq, head),
        P(head, seq),
    )

    def step(*args):
        return on_device(plan, *args)

    return jax.shard_map(step, mesh=fine, in_specs=in_specs, out_specs=out_specs, check_vma=False)
```

```python
import functools
import math
import types

import jax
import jax.numpy as jnp
import numpy as np
from jax import lax
from jax.experimental import pallas as pl
from jax.experimental.pallas import tpu as pltpu
from jax.sharding import Mesh, PartitionSpec as P

EPSILON = 1e-05
BF = jnp.bfloat16
F32 = jnp.float32
MESH = pl.DeviceIdType.MESH
VMEM_LIMIT = 67043328

def pick(array, index, axis):
    return lax.dynamic_index_in_dim(array, index, axis, keepdims=False)


def dot(left, right, contract):
    return lax.dot_general(left, right, (contract, ((), ())), preferred_element_type=F32)


def mm(left, right):
    return dot(left, right, ((1,), (0,)))


def mm_t(left, right):
    return dot(left, right, ((1,), (1,)))


def t_mm(left, right):
    return dot(left, right, ((0,), (0,)))


class Plan:
    def __init__(self, seq_bits, head_bits):
        self.seq = [f"s{i}" for i in range(seq_bits)]
        self.head = [f"h{i}" for i in range(head_bits)]
        self.names = tuple(reversed(self.seq)) + ()
        self.seq_axes = tuple(reversed(self.seq))
        self.head_axes = tuple(reversed(self.head))
        self.pair = "s1" if seq_bits > 1 else "s0"
        self.low = [a for a in self.seq if a < self.pair]
        self.high = [a for a in self.seq if a > self.pair]


class Square:
    def __init__(self, pair):
        self.pair = pair
        self.p = lax.axis_index(pair)
        self.y = lax.axis_index("h1")
        self.c = lax.axis_index("h0")
        self.S = {pair: 1 - self.p}
        self.Y = {"h1": 1 - self.y}
        self.C = {"h0": 1 - self.c}
        self.X = {"h1": 1 - self.y, "h0": 1 - self.c}

    def greet(self, cross=True):
        barrier = pltpu.get_barrier_semaphore()
        peers = [self.S, self.Y, self.C] + ([self.X] if cross else [])
        for peer in peers:
            pl.semaphore_signal(barrier, inc=1, device_id=peer, device_id_type=MESH)
        pl.semaphore_wait(barrier, len(peers))


def remote(source, target, sends, receives, index, device):
    return pltpu.make_async_remote_copy(
        src_ref=source,
        dst_ref=target,
        send_sem=sends.at[index],
        recv_sem=receives.at[index],
        device_id=device,
        device_id_type=MESH,
    )


def spread(sq, block, full, sends, receives, base, local_sem):
    rows, width = block.shape
    half = rows // 2

    def place(p, y, c, start, count):
        return full.at[p, pl.ds(start, count), pl.ds(pl.multiple_of((y * 2 + c) * width, width), width)]

    p, y, c = sq.p, sq.y, sq.c
    top, low = (0, half), (half, half)

    def own(part):
        return block.at[pl.ds(part[0], part[1]), :]

    def send(index, source, target, device):
        copy = remote(source, target, sends, receives, base + index, device)
        copy.start()
        return copy

    def relay(index, p_, y_, part, device):
        return send(index, place(p_, y_, c, *part), place(p_, y_, c, *part), device)

    k0 = send(0, own(top), place(p, y, c, *top), sq.S)
    k2 = send(2, own(low), place(p, y, c, *low), sq.Y)
    k6 = send(6, block, place(p, y, c, 0, rows), sq.C)
    k1 = send(1, own(low), place(p, y, c, *low), sq.S)
    k3 = send(3, own(top), place(p, y, c, *top), sq.Y)
    keep = pltpu.make_async_copy(block, place(p, y, c, 0, rows), local_sem)
    keep.start()
    k2.wait_recv()
    k4 = relay(4, p, 1 - y, low, sq.S)
    k9 = relay(9, p, 1 - y, low, sq.C)
    k0.wait_recv()
    k5 = relay(5, 1 - p, y, top, sq.Y)
    k7 = relay(7, 1 - p, y, top, sq.C)
    k1.wait_recv()
    k8 = relay(8, 1 - p, y, low, sq.C)
    k3.wait_recv()
    k10 = relay(10, p, 1 - y, top, sq.C)
    k5.wait_recv()
    k11 = relay(11, 1 - p, 1 - y, top, sq.C)
    k4.wait_recv()
    k12 = relay(12, 1 - p, 1 - y, low, sq.C)
    for copy in (k6, k7, k8, k9, k10, k11, k12):
        copy.wait_recv()
    for copy in (k0, k1, k2, k3, k4, k5, k6, k7, k8, k9, k10, k11, k12):
        copy.wait_send()
    keep.wait()


SPREAD_COPIES = 13
REDUCE_COPIES = 10


def exchange(sq, first, second, stats, sends, receives, base):
    rows = first.shape[0]
    lane = lax.broadcasted_iota(jnp.int32, (rows, 128), 1)
    packed = jnp.where(lane == 0, first, second).T
    mine = sq.y * 2 + sq.c
    stats[mine] = packed[:8]
    copies = []
    for index, device in enumerate((sq.Y, sq.C, sq.X)):
        copy = remote(stats.at[mine], stats.at[mine], sends, receives, base + index, device)
        copy.start()
        copies.append(copy)
    for copy in copies:
        copy.wait_recv()
    for copy in copies:
        copy.wait_send()
    return [stats[q][0:1] for q in range(4)], [stats[q][1:2] for q in range(4)]


def upright(first, second):
    rows = first.shape[1]
    line = lax.broadcasted_iota(jnp.int32, (128, rows), 0)
    turned = jnp.where(line == 0, first, second).T
    return turned[:, 0:1], turned[:, 1:2]


class Bulk:
    def __init__(self, plan, at, shards, wholes, sends, receives, local_sem):
        self.shards, self.wholes, self.at = shards, wholes, at
        self.sends, self.receives, self.local_sem = sends, receives, local_sem
        self.axes = [plan.pair] + plan.high + plan.low
        self.high, self.low, self.lows = plan.high, plan.low, len(plan.low)
        self.bit = {axis: 1 << plan.seq.index(axis) for axis in self.axes}
        self.me = sum(at[axis] * self.bit[axis] for axis in self.axes)
        self.size = 1 << len(self.axes)
        self.copies, self.kept, self.passed = [], {}, set()

    def piece(self, unit, mask):
        rows = self.shards[unit].shape[0]
        return self.wholes[unit].at[pl.ds(pl.multiple_of((self.me ^ mask) * rows, rows), rows), :]

    def half(self, unit, which):
        width = self.wholes[unit].shape[1]
        return self.shards[unit].at[:, pl.ds(pl.multiple_of(which * width, width), width)]

    def link(self, unit, source, held, axis):
        return remote(
            source,
            self.piece(unit, held),
            self.sends,
            self.receives,
            unit * self.size + (held | self.bit[axis]),
            {axis: 1 - self.at[axis]},
        )

    def send(self, unit, source, held, axis):
        copy = self.link(unit, source, held, axis)
        copy.start()
        self.copies.append(copy)

    def begin(self, unit, axes):
        own = self.at[self.axes[0]]
        for axis in axes:
            self.send(unit, self.half(unit, 1 - own if axis == self.axes[0] else own), 0, axis)
        if self.axes[0] in axes:
            keep = pltpu.make_async_copy(self.half(unit, own), self.piece(unit, 0), self.local_sem.at[unit])
            keep.start()
            self.kept[unit] = keep

    def held_before(self, stage):
        held = [0]
        for axis in self.axes[:stage]:
            held = held + [m | self.bit[axis] for m in held]
        return held

    def forward(self, unit, mask, axes):
        for later in axes:
            self.send(unit, self.piece(unit, mask), mask, later)

    def arrive(self, unit, stage, masks, axes=None):
        axis = self.axes[stage]
        for held in self.held_before(stage):
            mask = held | self.bit[axis]
            if not masks(mask):
                continue
            pltpu.make_async_remote_copy(
                src_ref=self.piece(unit, mask),
                dst_ref=self.piece(unit, mask),
                send_sem=self.sends.at[unit * self.size + mask],
                recv_sem=self.receives.at[unit * self.size + mask],
                device_id={axis: 1 - self.at[axis]},
                device_id_type=MESH,
            ).wait_recv()
            self.forward(unit, mask, self.axes[stage + 1 :] if axes is None else axes)

    def paired(self, unit, axes=None):
        self.arrive(unit, 0, lambda mask: True, axes)

    def first(self, unit):
        for stage in range(1, len(self.axes) - self.lows):
            self.arrive(unit, stage, lambda mask: not mask & self.bit[self.axes[0]])

    def second(self, unit):
        for stage in range(1, len(self.axes) - self.lows):
            self.arrive(unit, stage, lambda mask: mask & self.bit[self.axes[0]])

    def finish(self, unit):
        for stage in range(len(self.axes) - self.lows, len(self.axes)):
            self.arrive(unit, stage, lambda mask: True)
        self.kept[unit].wait()

    def drain(self):
        for copy in self.copies:
            copy.wait_send()


def together(process, *hooks):
    for number, _ in enumerate(process):
        if number < len(hooks):
            hooks[number]()


def carried(plan, at, state, reach, low_buf, high_buf, rate, length, reverse, sends, receives, base):
    index = base
    low_index = jnp.float32(0)
    span = 1.0
    copies = []

    def decay(count):
        return jnp.exp(rate * (count * float(length)))

    for slot in range(2):
        reach[slot] = jnp.zeros(reach.shape[1:], F32)
    for number, axis in enumerate(plan.low):
        bit = at[axis].astype(F32)
        late = 1.0 - bit if reverse else bit
        for slot in range(2):
            low_buf[2 * number, slot] = state[slot].astype(BF)
        copy = remote(low_buf.at[2 * number], low_buf.at[2 * number + 1], sends, receives, index, {axis: 1 - at[axis]})
        copy.start()
        copies.append(copy)
        index += 1
        yield
        copy.wait_recv()
        between = span - 1.0 - low_index if reverse else low_index
        step_decay = decay(span)
        take, keep = late * step_decay + (1.0 - late), late + (1.0 - late) * step_decay
        for slot in range(2):
            got = low_buf[2 * number + 1, slot].astype(F32)
            reach[slot] += got * (late * decay(between))
            state[slot] = got * take + state[slot] * keep
        low_index = low_index + bit * span
        span *= 2.0
    between = span - 1.0 - low_index if reverse else low_index
    early, later = (1, 0) if reverse else (0, 1)
    reach[later] += state[early] * decay(between)
    state[0] = state[early] * decay(span) + state[later]
    order = [low_index, low_index + span]
    span *= 2.0
    for number, axis in enumerate(plan.high):
        bit = at[axis].astype(F32)
        late = 1.0 - bit if reverse else bit
        high_buf[2 * number] = state[0].astype(BF)
        copy = remote(high_buf.at[2 * number], high_buf.at[2 * number + 1], sends, receives, index, {axis: 1 - at[axis]})
        copy.start()
        copies.append(copy)
        index += 1
        yield
        copy.wait_recv()
        step_decay = decay(span)
        take, keep = late * step_decay + (1.0 - late), late + (1.0 - late) * step_decay
        got = high_buf[2 * number + 1].astype(F32)
        for slot in range(2):
            between = span - 1.0 - order[slot] if reverse else order[slot]
            reach[slot] += got * (late * decay(between))
            order[slot] = order[slot] + bit * span
        state[0] = got * take + state[0] * keep
        span *= 2.0
    for copy in copies:
        copy.wait_send()


def carry_buffers(plan, key_size, value_size):
    return [
        pltpu.VMEM((2, key_size, value_size), F32),
        pltpu.VMEM((2, key_size, value_size), F32),
        pltpu.VMEM((2 * max(len(plan.low), 1), 2, key_size, value_size), BF),
        pltpu.VMEM((2 * max(len(plan.high), 1), key_size, value_size), BF),
    ]


def spread_steps(sq, block, full, sends, receives, base, local_sem):
    rows, width = block.shape
    half = rows // 2
    p, y, c = sq.p, sq.y, sq.c
    top, low = (0, half), (half, half)

    def place(p_, y_, c_, start, count):
        return full.at[p_, pl.ds(start, count), pl.ds(pl.multiple_of((y_ * 2 + c_) * width, width), width)]

    def own(part):
        return block.at[pl.ds(part[0], part[1]), :]

    def send(index, source, target, device):
        copy = remote(source, target, sends, receives, base + index, device)
        copy.start()
        return copy

    def relay(index, p_, y_, part, device):
        return send(index, place(p_, y_, c, *part), place(p_, y_, c, *part), device)

    k0 = send(0, own(top), place(p, y, c, *top), sq.S)
    k2 = send(2, own(low), place(p, y, c, *low), sq.Y)
    k6 = send(6, block, place(p, y, c, 0, rows), sq.C)
    k1 = send(1, own(low), place(p, y, c, *low), sq.S)
    k3 = send(3, own(top), place(p, y, c, *top), sq.Y)
    keep = pltpu.make_async_copy(block, place(p, y, c, 0, rows), local_sem)
    keep.start()
    yield
    k2.wait_recv()
    k4 = relay(4, p, 1 - y, low, sq.S)
    k9 = relay(9, p, 1 - y, low, sq.C)
    k0.wait_recv()
    k5 = relay(5, 1 - p, y, top, sq.Y)
    k7 = relay(7, 1 - p, y, top, sq.C)
    yield
    k1.wait_recv()
    k8 = relay(8, 1 - p, y, low, sq.C)
    k3.wait_recv()
    k10 = relay(10, p, 1 - y, top, sq.C)
    yield
    k5.wait_recv()
    k11 = relay(11, 1 - p, 1 - y, top, sq.C)
    k4.wait_recv()
    k12 = relay(12, 1 - p, 1 - y, low, sq.C)
    for copy in (k6, k7, k8, k9, k10, k11, k12):
        copy.wait_recv()
    for copy in (k0, k1, k2, k3, k4, k5, k6, k7, k8, k9, k10, k11, k12):
        copy.wait_send()
    keep.wait()


def pass_steps(sq, block, full, sends, receives, base, wide):
    rows = full.shape[1]
    width = full.shape[2] // 4
    half = rows // 2
    p, y, c = sq.p, sq.y, sq.c
    parts = ((0, half), (half, half))
    copies = []

    def place(p_, y_, part):
        columns = pl.ds(pl.multiple_of((y_ * 2 + c) * width, width), width)
        return full.at[p_, pl.ds(part[0], part[1]), columns]

    def send(index, source, p_, y_, part, device):
        copy = remote(source, place(p_, y_, part), sends, receives, base + index, device)
        copy.start()
        copies.append(copy)
        return copy

    def own(part):
        return block.at[pl.ds(part[0], part[1]), :]

    far = [send(i, own(part), p, y, part, sq.S) for i, part in enumerate(parts)]
    beside, near = [], []
    if wide:
        beside += [send(2 + i, own(part), p, y, part, sq.Y) for i, part in enumerate(parts)]
        near += [send(4 + i, own(part), p, y, part, sq.C) for i, part in enumerate(parts)]
    yield
    other = []
    for i, part in enumerate(parts):
        far[i].wait_recv()
        other.append(send(6 + i, place(1 - p, y, part), 1 - p, y, part, sq.Y))
        near.append(send(8 + i, place(1 - p, y, part), 1 - p, y, part, sq.C))
    yield
    for i, part in enumerate(parts):
        if wide:
            beside[i].wait_recv()
            near.append(send(10 + i, place(p, 1 - y, part), p, 1 - y, part, sq.C))
        other[i].wait_recv()
        near.append(send(12 + i, place(1 - p, 1 - y, part), 1 - p, 1 - y, part, sq.C))
    yield
    for copy in near:
        copy.wait_recv()
    for copy in copies:
        copy.wait_send()


PASS_COPIES = 14


def reduce_steps(sq, block_of, result, hand, near, total, arrived, sends, receives, base):
    rows, width = result.shape
    half = rows // 2
    p, y, c = sq.p, sq.y, sq.c
    top, low = pl.ds(0, half), pl.ds(half, half)

    def send(index, source, target, device):
        copy = remote(source, target, sends, receives, base + index, device)
        copy.start()
        return copy

    order = ((1 - p, 1 - y), (1 - p, y), (p, 1 - y), (p, y))

    def give(i, p_, y_):
        return remote(hand.at[p_, y_], near.at[p_, y_], sends, receives, base + i, sq.C)

    @pl.loop(0, 4)
    def _(i):
        p_, y_ = (1 - p + i // 2) % 2, (1 - y + i % 2) % 2
        hand[p_, y_] = block_of(p_, y_, 1 - c).astype(BF)
        give(i, p_, y_).start()

    given = [give(i, p_, y_) for i, (p_, y_) in enumerate(order)]

    def join(i):
        p_, y_ = order[i]
        own = block_of(p_, y_, c)
        given[i].wait_recv()
        return own + near[p_, y_].astype(F32)

    total[1 - p, 1 - y] = join(0).astype(BF)
    a = send(4, total.at[1 - p, 1 - y, low], arrived.at[0], sq.S)
    b = send(5, total.at[1 - p, 1 - y, top], arrived.at[1], sq.Y)

    @pl.loop(0, 2)
    def _(i):
        p_, y_ = (1 - p + i) % 2, (y + i) % 2
        own = block_of(p_, y_, c)
        give(1 + i, p_, y_).wait_recv()
        total[p_, y_] = (own + near[p_, y_].astype(F32)).astype(BF)

    e = send(6, total.at[1 - p, y, low], arrived.at[2], sq.S)
    f = send(7, total.at[p, 1 - y, top], arrived.at[3], sq.Y)
    result[...] = join(3)
    yield
    b.wait_recv()
    total[1 - p, y, top] = (total[1 - p, y, top].astype(F32) + arrived[1].astype(F32)).astype(BF)
    g = send(8, total.at[1 - p, y, top], arrived.at[4], sq.S)
    a.wait_recv()
    total[p, 1 - y, low] = (total[p, 1 - y, low].astype(F32) + arrived[0].astype(F32)).astype(BF)
    d = send(9, total.at[p, 1 - y, low], arrived.at[5], sq.Y)
    yield
    e.wait_recv()
    f.wait_recv()
    g.wait_recv()
    result[top, :] += arrived[4].astype(F32) + arrived[3].astype(F32)
    d.wait_recv()
    result[low, :] += arrived[2].astype(F32) + arrived[5].astype(F32)
    for copy in given + [a, b, e, f, g, d]:
        copy.wait_send()


def reduce_room(rows, width):
    return [pltpu.VMEM((2, 2, rows, width), BF)] * 3 + [pltpu.VMEM((6, rows // 2, width), BF)]


def flipped(plan, at, mask):
    return {axis: 1 - at[axis] for i, axis in enumerate(plan.seq) if mask >> i & 1}


def greet_all(plan, at, sq):
    barrier = pltpu.get_barrier_semaphore()
    peers = [flipped(plan, at, mask) for mask in range(1, 1 << len(plan.seq))] + [sq.Y, sq.C, sq.X]
    for peer in peers:
        pl.semaphore_signal(barrier, inc=1, device_id=peer, device_id_type=MESH)
    pl.semaphore_wait(barrier, len(peers))


def column_of(rows, start, sign, rate):
    offset = lax.broadcasted_iota(jnp.int32, (rows, 1), 0).astype(F32)
    return jnp.exp((start + sign * offset) * rate)


def decay_mask(mask, rate):
    rows = mask.shape[0]

    @pl.loop(0, rows // 128)
    def _(i):
        start = pl.multiple_of(i * 128, 128)
        line = lax.broadcasted_iota(jnp.int32, (128, rows), 0) + start
        lane = lax.broadcasted_iota(jnp.int32, (128, rows), 1)
        distance = (line - lane).astype(F32)
        mask[pl.ds(start, 128), :] = jnp.where(distance >= 0, jnp.exp(jnp.maximum(distance, 0.0) * rate), 0.0)


TILE = 256


def row_tiles(full, body):
    rows = full.shape[1]
    each = rows // TILE

    @pl.loop(0, 2 * each)
    def _(i):
        body(i // each, pl.multiple_of(i % each * TILE, TILE), pl.multiple_of(i * TILE, TILE))


def turned(r, slot, start):
    base = r.turn[slot]
    cos_at, sin_at = base[0:1], base[1:2]
    cos_off, sin_off = r.cos_off[pl.ds(start, TILE), :], r.sin_off[pl.ds(start, TILE), :]
    return cos_at * cos_off - sin_at * sin_off, sin_at * cos_off + cos_at * sin_off


def front_kernel(plan, names, *refs):
    r = types.SimpleNamespace(**dict(zip(names, refs)))
    at = {axis: lax.axis_index(axis) for axis in plan.seq + plan.head}
    sq = Square(plan.pair)
    length, model = r.inputs.shape
    width = r.block.shape[1]
    mine = sq.y * 2 + sq.c
    column = pl.multiple_of(mine * width, width)
    rate = r.rate[0:1, 0:1]
    weights = [r.wq, r.wk, r.wv, r.wg, r.wo, r.wu, r.wd]
    key_size, value_size = r.wq.shape[1], r.wv.shape[1]
    saved = []

    def save(source, target):
        copy = pltpu.make_async_copy(source, target, r.save_sem.at[len(saved)])
        copy.start()
        saved.append(copy)

    greet_all(plan, at, sq)
    flip = r.so.shape[0] != r.sq.shape[0]
    outer_shards = [r.so_t, r.sd_t] if flip else [r.so, r.sd]
    shards = [r.sq, r.sk, r.sv, r.sg, outer_shards[0], r.su, outer_shards[1]]
    bulk = Bulk(plan, at, shards, weights, r.bulk_send, r.bulk_receive, r.bulk_local)
    QUERY, KEY, VALUE, GATE, OUT, UP, DOWN = range(7)
    pair, high, low = [bulk.axes[0]], bulk.high, bulk.low

    size = 1 << len(plan.seq)
    copies = []
    for mask in range(1, size):
        copy = remote(r.vec, r.vecs.at[bulk.me], r.vec_send, r.vec_receive, mask, flipped(plan, at, mask))
        copy.start()
        copies.append(copy)
    r.vecs[bulk.me] = r.vec[...]
    bulk.begin(QUERY, bulk.axes)
    bulk.begin(KEY, bulk.axes)
    if flip:
        r.so_t[...] = r.so[...].T
        r.sd_t[...] = r.sd[...].T
    r.cot_bf[...] = r.cot[...].astype(BF)
    for unit in (VALUE, GATE, OUT):
        bulk.begin(unit, low)

    for copy in copies:
        copy.wait_recv()
    step = r.vec.shape[1]
    for j in range(size):
        r.all_gains[:, j * step : (j + 1) * step] = r.vecs[j]
    r.gains[...] = r.all_gains[:, pl.ds(column, width)]

    @pl.loop(0, length // 128)
    def _(i):
        rows = pl.ds(pl.multiple_of(i * 128, 128), 128)
        stream = r.inputs[rows, :]
        mean = jnp.mean(stream, axis=1, keepdims=True)
        inverse = lax.rsqrt(jnp.mean(jnp.square(stream - mean), axis=1, keepdims=True) + EPSILON)
        r.inverse_one[rows, :] = jnp.broadcast_to(inverse, (128, 128))
        normed = (stream - mean) * inverse
        hidden = (normed * r.all_gains[0:1, :] + r.all_gains[1:2, :]).astype(BF)
        r.hidden[sq.p, rows, :] = hidden
        own = (r.inputs[rows, pl.ds(column, width)] - mean) * inverse
        r.normed_one[rows, :] = own
        r.block[rows, :] = (own * r.gains[0:1, :] + r.gains[1:2, :]).astype(BF)

    gains = r.gains[...]
    hid = pass_steps(sq, r.block, r.hidden, r.hid_send, r.hid_receive, 0, False)
    cot = pass_steps(sq, r.cot_bf, r.cot_out, r.cot_send, r.cot_receive, 0, True)
    keep_cot = pltpu.make_async_copy(r.cot_bf, r.cot_out.at[sq.p, :, pl.ds(column, width)], r.local_sem.at[0])
    keep_cot.start()
    next(hid)
    bulk.begin(VALUE, pair + high)
    bulk.paired(QUERY)
    bulk.paired(KEY)
    bulk.first(QUERY)
    bulk.first(KEY)
    bulk.paired(VALUE)
    bulk.begin(GATE, pair + high)
    bulk.begin(OUT, pair + high)
    next(hid)
    decay_mask(r.mask, rate)
    bulk.second(QUERY)
    bulk.second(KEY)
    bulk.first(VALUE)
    next(hid)
    next(hid, None)
    save(r.hidden, r.hidden_out)

    bulk.finish(QUERY)
    bulk.finish(KEY)
    save(r.wq, r.wq_out)
    save(r.wk, r.wk_out)

    def project_keys(slot, start, row):
        hidden = r.hidden[slot, pl.ds(start, TILE), :]
        cosine, sine = turned(r, slot, start)
        for weight, target in ((r.wq, r.q), (r.wk, r.k)):
            value = mm(hidden, weight[...])
            target[pl.ds(row, TILE), :] = rotate(value, cosine, sine).astype(BF)

    row_tiles(r.hidden, project_keys)

    bulk.second(VALUE)
    bulk.paired(GATE)
    bulk.paired(OUT)
    bulk.finish(VALUE)
    save(r.wv, r.wv_out)

    def project_values(slot, start, row):
        r.v[pl.ds(row, TILE), :] = mm(r.hidden[slot, pl.ds(start, TILE), :], r.wv[...]).astype(BF)

    row_tiles(r.hidden, project_values)
    save(r.q, r.q_out)
    save(r.k, r.k_out)
    save(r.v, r.v_out)
    weight_out = column_of(length, float(length), -1.0, rate)
    for slot in range(2):
        rows = slice(slot * length, (slot + 1) * length)
        key = (r.k[rows, :].astype(F32) * weight_out).astype(BF)
        r.state[slot] = t_mm(key, r.v[rows, :])
    carry = carried(
        plan, at, r.state, r.reach, r.low_buf, r.high_buf, rate, length, False, r.carry_send, r.carry_receive, 0
    )
    next(carry)

    def inner(slot, start, row):
        scores = mm_t(r.q[pl.ds(row, TILE), :], r.k[pl.ds(pl.multiple_of(slot * length, length), length), :])
        weights_ = (scores * r.mask[pl.ds(start, TILE), :]).astype(BF)
        r.normed[pl.ds(row, TILE), :] = mm(weights_, r.v[pl.ds(pl.multiple_of(slot * length, length), length), :])

    row_tiles(r.hidden, inner)
    bulk.first(GATE)
    bulk.first(OUT)
    bulk.begin(UP, pair)
    bulk.begin(DOWN, pair)
    next(carry, None)
    bulk.second(GATE)
    bulk.second(OUT)
    bulk.begin(UP, high + low)
    bulk.begin(DOWN, low)
    bulk.finish(GATE)
    save(r.wg, r.wg_out)

    def gates(slot, start, row):
        r.gate[pl.ds(row, TILE), :] = mm(r.hidden[slot, pl.ds(start, TILE), :], r.wg[...])

    row_tiles(r.hidden, gates)
    save(r.gate, r.gate_out)
    bulk.paired(UP, low)
    bulk.paired(DOWN, low)
    for _ in carry:
        pass
    for slot in range(2):
        r.reach_bf[slot] = r.reach[slot].astype(BF)
    save(r.reach_bf, r.reach_out)

    def outer(slot, start, row):
        rows = pl.ds(row, TILE)
        offset = lax.broadcasted_iota(jnp.int32, (TILE, 1), 0) + start
        cross = mm(r.q[rows, :], r.reach_bf[slot]) * jnp.exp(offset.astype(F32) * rate)
        retained = r.normed[rows, :] + cross
        center = retained - jnp.mean(retained, axis=1, keepdims=True)
        inverse = lax.rsqrt(jnp.mean(center * center, axis=1, keepdims=True) + EPSILON)
        value = center * inverse
        r.normed[rows, :] = value
        r.inverse[rows, :] = jnp.broadcast_to(inverse, (TILE, 128))
        gate = r.gate[rows, :]
        r.gated[rows, :] = (gate * jax.nn.sigmoid(gate) * value).astype(BF)

    row_tiles(r.hidden, outer)
    save(r.normed, r.normed_out)
    save(r.inverse, r.inverse_out)
    save(r.gated, r.gated_out)
    bulk.finish(OUT)
    save(r.wo, r.wo_out)

    def out_block(p_, y_, c_):
        rows = pl.ds(pl.multiple_of(p_ * length, length), length)
        return mm_t(r.gated[rows, :], r.wo[pl.ds(pl.multiple_of((y_ * 2 + c_) * width, width), width), :])

    def nothing():
        pass

    def rest_of_up():
        bulk.forward(UP, bulk.bit[pair[0]], high)
        bulk.begin(DOWN, high)

    def rest_of_down():
        bulk.forward(DOWN, bulk.bit[pair[0]], high)
        next(cot)
        bulk.first(UP)

    def second_up():
        bulk.second(UP)
        bulk.first(DOWN)

    reduce = reduce_steps(
        sq, out_block, r.middle, r.hand, r.near, r.total, r.arrived, r.sends, r.receives, SPREAD_COPIES
    )
    together(reduce, nothing, rest_of_up)
    whole = r.middle[...] + r.inputs[:, pl.ds(column, width)]
    r.middle[...] = whole
    mean = jnp.mean(whole, axis=1, keepdims=True)
    deviation = jnp.mean(jnp.square(whole - mean), axis=1, keepdims=True)
    base = SPREAD_COPIES + REDUCE_COPIES
    means, spreads = exchange(sq, mean, deviation, r.stats, r.sends, r.receives, base)
    center = sum(means) * (1.0 / len(means))
    variance = sum(s + jnp.square(m - center) for m, s in zip(means, spreads)) * (1.0 / len(means))
    mean, scale = upright(center, lax.rsqrt(variance + EPSILON))
    r.inverse_two[...] = jnp.broadcast_to(scale, r.inverse_two.shape)
    value = (r.middle[...] - mean) * scale
    r.normed_two[...] = value
    r.block[...] = (value * gains[2:3] + gains[3:4]).astype(BF)
    spread = spread_steps(sq, r.block, r.mid_out, r.sends, r.receives, 0, r.local_sem.at[1])
    together(spread, nothing, rest_of_down, second_up)
    bulk.finish(UP)
    save(r.wu, r.wu_out)
    next(cot)
    bulk.second(DOWN)
    next(cot)
    next(cot, None)
    bulk.finish(DOWN)
    save(r.wd, r.wd_out)
    bulk.drain()
    keep_cot.wait()
    for copy in copies:
        copy.wait_send()
    for copy in saved:
        copy.wait()


def front(plan, shards, inputs, cot, vec, rate, turn, cos_off, sin_off, number):
    length, model = inputs.shape
    width = cot.shape[1]
    size = 1 << len(plan.seq)
    key_size, value_size, hidden = shards[0].shape[1] // 2, shards[2].shape[1] // 2, shards[5].shape[1] // 2
    any_spec, vmem_spec = pl.BlockSpec(memory_space=pl.ANY), pl.BlockSpec(memory_space=pltpu.VMEM)
    both = 2 * length

    def shape(dims, kind=BF):
        return jax.ShapeDtypeStruct(dims, kind)

    sq, sk, sv, sg, so, su, sd = shards
    rows = sq.shape[0]
    flip = rows % 128 == 0
    if not flip:
        so, sd = so.T, sd.T
    far = dict(sq=sq, sk=sk, sv=sv, sg=sg, su=su)
    near = dict(so=so, sd=sd, inputs=inputs, cot=cot, vec=vec, rate=rate, turn=turn, cos_off=cos_off, sin_off=sin_off)
    wq, wk, wv, wg, wu = [(model, s.shape[1] // 2) for s in far.values()]
    wo, wd = (model, value_size), (model, hidden)
    far_outs = dict(
        wq_out=shape(wq),
        wk_out=shape(wk),
        wv_out=shape(wv),
        wg_out=shape(wg),
        wo_out=shape(wo),
        wu_out=shape(wu),
        wd_out=shape(wd),
        hidden_out=shape((2, length, model)),
        cot_out=shape((2, length, model)),
        mid_out=shape((2, length, model)),
        q_out=shape((both, key_size)),
        k_out=shape((both, key_size)),
        v_out=shape((both, value_size)),
        reach_out=shape((2, key_size, value_size)),
        gate_out=shape((both, value_size), F32),
        normed_out=shape((both, value_size), F32),
        inverse_out=shape((both, 128), F32),
        gated_out=shape((both, value_size)),
    )
    near_outs = dict(
        middle=shape((length, width), F32),
        normed_one=shape((length, width), F32),
        inverse_one=shape((length, 128), F32),
        normed_two=shape((length, width), F32),
        inverse_two=shape((length, 128), F32),
        gains=shape((8, width), F32),
    )
    carries = carry_buffers(plan, key_size, value_size)
    count = SPREAD_COPIES + REDUCE_COPIES + 3
    dma = pltpu.SemaphoreType.DMA
    hand, near_room, total, arrived = reduce_room(length, width)
    scratch = dict(
        so_t=pltpu.VMEM((rows, 2 * value_size) if flip else (16, 128), BF),
        sd_t=pltpu.VMEM((rows, 2 * hidden) if flip else (16, 128), BF),
        cot_bf=pltpu.VMEM((length, width), BF),
        wq=pltpu.VMEM(wq, BF),
        wk=pltpu.VMEM(wk, BF),
        wv=pltpu.VMEM(wv, BF),
        wg=pltpu.VMEM(wg, BF),
        wo=pltpu.VMEM(wo, BF),
        wu=pltpu.VMEM(wu, BF),
        wd=pltpu.VMEM(wd, BF),
        hidden=pltpu.VMEM((2, length, model), BF),
        block=pltpu.VMEM((length, width), BF),
        q=pltpu.VMEM((both, key_size), BF),
        k=pltpu.VMEM((both, key_size), BF),
        v=pltpu.VMEM((both, value_size), BF),
        gate=pltpu.VMEM((both, value_size), F32),
        normed=pltpu.VMEM((both, value_size), F32),
        inverse=pltpu.VMEM((both, 128), F32),
        gated=pltpu.VMEM((both, value_size), BF),
        mask=pltpu.VMEM((length, length), F32),
        state=carries[0],
        reach=carries[1],
        low_buf=carries[2],
        high_buf=carries[3],
        reach_bf=pltpu.VMEM((2, key_size, value_size), BF),
        vecs=pltpu.VMEM((size, 8, rows), F32),
        stats=pltpu.VMEM((4, 8, length), F32),
        hand=hand,
        near=near_room,
        total=total,
        arrived=arrived,
        bulk_send=dma((7 * size,)),
        bulk_receive=dma((7 * size,)),
        bulk_local=dma((7,)),
        vec_send=dma((size,)),
        vec_receive=dma((size,)),
        carry_send=dma((len(plan.seq),)),
        carry_receive=dma((len(plan.seq),)),
        all_gains=pltpu.VMEM((8, model), F32),
        hid_send=dma((PASS_COPIES,)),
        hid_receive=dma((PASS_COPIES,)),
        cot_send=dma((PASS_COPIES,)),
        cot_receive=dma((PASS_COPIES,)),
        sends=dma((count,)),
        receives=dma((count,)),
        local_sem=dma((3,)),
        save_sem=dma((32,)),
    )
    names = list(far) + list(near) + list(far_outs) + list(near_outs) + list(scratch)
    results = pl.pallas_call(
        functools.partial(front_kernel, plan, names),
        out_shape=tuple(far_outs.values()) + tuple(near_outs.values()),
        in_specs=[any_spec] * len(far) + [vmem_spec] * len(near),
        out_specs=(any_spec,) * len(far_outs) + (vmem_spec,) * len(near_outs),
        scratch_shapes=list(scratch.values()),
        compiler_params=pltpu.CompilerParams(
            collective_id=number, has_side_effects=True, vmem_limit_bytes=VMEM_LIMIT
        ),
        name="front",
    )(*far.values(), *near.values())
    return types.SimpleNamespace(**dict(zip(list(far_outs) + list(near_outs), results)))


SLOT = (1, 0, 2, 0, 3, None)


class Return:
    def __init__(self, plan, at, totals, spare, got, sends, receives):
        self.at, self.totals, self.spare, self.got = at, totals, spare, got
        self.sends, self.receives = sends, receives
        self.order = plan.low + list(reversed(plan.high)) + [plan.pair]
        self.bit = {axis: 1 << i for i, axis in enumerate(plan.seq)}
        self.size = 1 << len(plan.seq)
        self.me = sum(at[axis] * self.bit[axis] for axis in self.order)
        self.copies = {}

    def stage_of(self, mask):
        for stage, axis in enumerate(self.order):
            if mask & self.bit[axis]:
                return stage
        return len(self.order)

    def masks(self, stage):
        found = [m for m in range(1, self.size) if self.stage_of(m) == stage]
        return sorted(found, key=lambda m: (self.stage_of(m ^ self.bit[self.order[stage]]), m))

    def link(self, unit, mask, axis=None):
        axis = axis or self.order[self.stage_of(mask)]
        return remote(
            self.total(unit, mask),
            self.got.at[unit, mask - 1],
            self.sends,
            self.receives,
            unit * self.size + mask,
            {axis: 1 - self.at[axis]},
        )

    def total(self, unit, mask):
        rows, columns = self.got.shape[2:]
        if SLOT[unit] is None:
            across, down = self.spare.shape[2] // columns, self.spare.shape[1] // rows
            tile = self.spare.at[mask // (across * down)]
            return tile.at[pl.ds(mask // across % down * rows, rows), pl.ds(mask % across * columns, columns)]
        return self.totals.at[SLOT[unit], pl.ds(mask * rows, rows), :]

    def send(self, unit, mask):
        copy = self.link(unit, mask)
        copy.start()
        self.copies[unit, mask] = copy

    def made(self, unit, mask):
        if self.stage_of(mask) == 0:
            self.send(unit, mask)

    def ahead(self, stage):
        bit = self.bit[self.order[stage]]
        masks = self.masks(stage)
        first = [m for m in masks if m ^ bit and self.stage_of(m ^ bit) == stage + 1]
        return first, [m for m in masks if m not in first]

    def collect(self, unit, stage, masks):
        axis = self.order[stage]
        for mask in masks:
            target = mask ^ self.bit[axis]
            self.link(unit, mask).wait_recv()
            total, got = self.total(unit, target), self.got.at[unit, mask - 1]

            @pl.loop(0, total.shape[0] // 64)
            def _(i, total=total, got=got):
                rows = pl.ds(pl.multiple_of(i * 64, 64), 64)
                total[rows, :] = (total[rows, :].astype(F32) + got[rows, :].astype(F32)).astype(BF)

            if self.stage_of(target) == stage + 1 and target:
                self.send(unit, target)

    def early(self, unit):
        self.collect(unit, 0, self.ahead(0)[0])

    def late(self, unit):
        self.collect(unit, 0, self.ahead(0)[1])

    def middle(self, unit):
        for stage in range(1, len(self.order) - 1):
            self.collect(unit, stage, self.masks(stage))

    def last(self, unit):
        return self.got.at[unit, self.bit[self.order[-1]] - 1]

    def last_arrived(self, unit):
        self.link(unit, self.bit[self.order[-1]]).wait_recv()

    def clear(self, unit):
        for (number, _), copy in self.copies.items():
            if number == unit:
                copy.wait_send()


def back_kernel(plan, names, *refs):
    r = types.SimpleNamespace(**dict(zip(names, refs)))
    at = {axis: lax.axis_index(axis) for axis in plan.seq + plan.head}
    sq = Square(plan.pair)
    length, width = r.cot.shape
    key_size, value_size = r.q.shape[1], r.v.shape[1]
    mine = sq.y * 2 + sq.c
    rate = r.rate[0:1, 0:1]
    UP, DOWN, OUT, GATE, VALUE, KEYS = range(6)
    back = Return(plan, at, r.totals, r.tiles, r.got, r.bulk_send, r.bulk_receive)
    piece, model = r.got.shape[2], r.mid.shape[2]
    strip = r.strips.shape[2]
    per_strip = strip // piece

    loads = {}

    def load(name, source, target):
        copy = pltpu.make_async_copy(source, target, r.load_sem.at[len(loads)])
        copy.start()
        loads[name] = copy

    def ready(*wanted):
        for name in wanted:
            loads[name].wait()

    load("wu", r.wu, r.weights.at[0])
    load("wd", r.wd, r.weights.at[1])

    parts = model // value_size

    def tile_copy(source, i):
        each = length // TILE
        rows = source.at[i // each, pl.ds(i % each * TILE, TILE), :]
        return [pltpu.make_async_copy(rows, r.tiles.at[i % 2], r.tile_sem.at[i % 2, 0])]

    def cot_tile(i, part):
        rows = pl.ds(pl.multiple_of((i % 2 * parts + part) * TILE, TILE), TILE)
        return r.totals.at[r.totals.shape[0] - 1, rows, :]

    def cot_copy(i):
        each = length // TILE
        return [
            pltpu.make_async_copy(
                r.cotf.at[i // each, pl.ds(i % each * TILE, TILE), pl.ds(part * value_size, value_size)],
                cot_tile(i, part),
                r.tile_sem.at[i % 2, 1 + part],
            )
            for part in range(parts)
        ]

    def start(copies):
        for copy in copies:
            copy.start()

    def wait(copies):
        for copy in copies:
            copy.wait()

    tile_count = 2 * length // TILE
    start(tile_copy(r.mid, 0) + cot_copy(0))
    greet_all(plan, at, sq)
    load("wo", r.wo, r.weights.at[2])
    load("gated", r.gated_in, r.gated)
    load("gate", r.gate_in, r.gate)
    load("normed", r.normed_in, r.normed)
    load("inverse", r.inverse_in, r.inverse)
    load("q", r.q_in, r.q)
    load("k", r.k_in, r.k)
    load("v", r.v_in, r.v)
    load("reach", r.reach_in, r.in_bf)
    load("middle", r.middle_in, r.layer_out)
    ready("wu", "wd")

    @pl.loop(0, tile_count)
    def _(i):
        @pl.when(i + 1 < tile_count)
        def _():
            start(tile_copy(r.mid, i + 1) + cot_copy(i + 1))

        wait(tile_copy(r.mid, i) + cot_copy(i))
        rows = pl.ds(pl.multiple_of(i * TILE, TILE), TILE)
        preact = mm(r.tiles[i % 2], r.weights[0])
        cdf = 0.5 * (1.0 + lax.erf(preact * 0.7071067811865476))
        slope = cdf + preact * (jnp.exp(-0.5 * preact * preact) * 0.3989422804014327)
        r.hidden_ff[rows, :] = (preact * cdf).astype(BF)
        grad = sum(
            mm(cot_tile(i, part)[...], r.weights[1, part * value_size : (part + 1) * value_size, :])
            for part in range(parts)
        )
        r.grad_pre[rows, :] = (grad * slope).astype(BF)

    def strip_copy(source, mask, number):
        start = pl.multiple_of((back.me ^ mask) // per_strip * strip, strip)
        half = r.strips.at[number % 2]
        return [
            pltpu.make_async_copy(
                source.at[slot, :, pl.ds(start, strip)],
                half.at[pl.ds(slot * length, length), :],
                r.strip_sem.at[number % 2, slot],
            )
            for slot in range(2)
        ]

    def produce(unit, source, grads, masks):
        count = len(masks)
        step = masks[1] - masks[0] if count > 1 else 0
        even = all(mask == masks[0] + number * step for number, mask in enumerate(masks))

        def one(number, mask):
            for copy in strip_copy(source, mask, number):
                copy.wait()
            value = t_mm(r.strips[number % 2], grads[...])
            if per_strip > 1:
                r.whole_strip[...] = value
                inside = pl.multiple_of((back.me ^ mask) % per_strip * piece, piece)
                value = r.whole_strip[pl.ds(inside, piece), :]
            back.total(unit, mask)[...] = value.astype(BF)

        for copy in strip_copy(source, masks[0], 0):
            copy.start()
        if even:

            @pl.loop(0, count)
            def _(number):
                @pl.when(number + 1 < count)
                def _():
                    for copy in strip_copy(source, masks[0] + (number + 1) * step, number + 1):
                        copy.start()

                mask = masks[0] + number * step
                one(number, mask)
                if back.stage_of(masks[0]) == 0:
                    back.link(unit, mask, back.order[0]).start()

            for mask in masks:
                if back.stage_of(mask) == 0:
                    back.copies[unit, mask] = back.link(unit, mask)
        else:
            for number, mask in enumerate(masks):
                if number + 1 < count:
                    for copy in strip_copy(source, masks[number + 1], number + 1):
                        copy.start()
                one(number, mask)
                back.made(unit, mask)

    away_first, away_rest = back.ahead(0)
    low_bit = back.bit[back.order[0]]
    home_first, home_rest = ([m ^ low_bit for m in masks] for masks in (away_first, away_rest))

    def blocks(grads, weight):
        def block_of(p_, y_, c_):
            rows = pl.ds(pl.multiple_of(p_ * length, length), length)
            columns = pl.ds(pl.multiple_of((y_ * 2 + c_) * width, width), width)
            return sum(mm_t(g[rows, :], r.weights[w, columns, :]) for g, w in zip(grads, weight))

        return block_of

    def reduce(grads, weight, result, base):
        return reduce_steps(
            sq, blocks(grads, weight), result, r.hand, r.near, r.near, r.arrived, r.sends, r.receives, base
        )

    emitted = {}

    def emit(unit):
        own = at[plan.pair]
        back.last_arrived(unit)
        emitted[unit] = [
            pltpu.make_async_copy(source, r.halves.at[unit, half], r.emit_sem.at[unit, number])
            for number, (half, source) in enumerate(((own, back.total(unit, 0)), (1 - own, back.last(unit))))
        ]
        start(emitted[unit])

    def clear(unit):
        back.clear(unit)
        wait(emitted[unit])

    def norm_sums(upstream, gain, normed, inverse, base_stream, result, row, stats, base):
        value = upstream[...]
        product = value * normed[...]
        r.sums[row : row + 1, :] = jnp.sum(product, axis=0, keepdims=True)
        r.sums[row + 1 : row + 2, :] = jnp.sum(value, axis=0, keepdims=True)
        first = jnp.mean(value * gain, axis=1, keepdims=True)
        second = jnp.mean(product * gain, axis=1, keepdims=True)
        firsts, seconds = exchange(sq, first, second, stats, r.sends, r.receives, base)
        share = 1.0 / len(firsts)
        first, second = upright(sum(firsts) * share, sum(seconds) * share)
        result[...] = base_stream[...] + inverse[:, 0:1] * (upstream[...] * gain - first - normed[...] * second)

    def down_last():
        produce(DOWN, r.cotf, r.hidden_ff, away_rest)
        produce(DOWN, r.cotf, r.hidden_ff, home_first)
        produce(UP, r.mid, r.grad_pre, away_first)

    base = SPREAD_COPIES
    together(
        reduce([r.grad_pre], [0], r.upstream, base),
        lambda: produce(DOWN, r.cotf, r.hidden_ff, away_first),
        down_last,
    )
    base += REDUCE_COPIES
    back.early(DOWN)
    load("wv", r.wv, r.weights.at[0])
    norm_sums(r.upstream, r.gains[2:3, :], r.normed_two, r.inverse_two, r.cot, r.grad_middle, 2, r.stats, base)
    base += 3
    block = r.hand.at[0, 0]
    block[...] = r.grad_middle[...].astype(BF)

    def up_next():
        produce(UP, r.mid, r.grad_pre, away_rest)
        produce(DOWN, r.cotf, r.hidden_ff, home_rest)

    def up_last():
        back.late(DOWN)
        produce(UP, r.mid, r.grad_pre, home_rest)

    together(
        spread_steps(sq, block, r.gmid, r.sends, r.receives, 0, r.local_sem.at[0]),
        up_next,
        lambda: produce(UP, r.mid, r.grad_pre, home_first),
    )
    up_last()
    ready("wo", "gated", "gate", "normed", "inverse")
    back.early(UP)

    start(tile_copy(r.gmid, 0))
    @pl.loop(0, tile_count)
    def _(i):
        @pl.when(i + 1 < tile_count)
        def _():
            start(tile_copy(r.gmid, i + 1))

        wait(tile_copy(r.gmid, i))
        rows = pl.ds(pl.multiple_of(i * TILE, TILE), TILE)
        grad = mm(r.tiles[i % 2], r.weights[2])
        gate = r.gate[rows, :]
        normed = r.normed[rows, :]
        logistic = jax.nn.sigmoid(gate)
        swish = gate * logistic
        r.grad_gate[rows, :] = (grad * normed * (logistic + swish * (1.0 - logistic))).astype(BF)
        scaled = grad * swish
        r.grad_mixed[rows, :] = (
            r.inverse[rows, 0:1]
            * (
                scaled
                - jnp.mean(scaled, axis=1, keepdims=True)
                - normed * jnp.mean(scaled * normed, axis=1, keepdims=True)
            )
        ).astype(BF)
    load("wg", r.wg, r.weights.at[2])
    back.middle(DOWN)

    ready("q", "k", "v", "reach")
    decay_mask(r.mask, rate)
    weight_out = column_of(length, 1.0, 1.0, rate)
    for slot in range(2):
        rows = slice(slot * length, (slot + 1) * length)
        query = (r.q[rows, :].astype(F32) * weight_out).astype(BF)
        r.state[slot] = t_mm(query, r.grad_mixed[rows, :])
    carry = carried(
        plan, at, r.state, r.reach, r.low_buf, r.high_buf, rate, length, True, r.carry_send, r.carry_receive, 0
    )
    next(carry)
    produce(OUT, r.gmid, r.gated, away_first)
    weight_in = column_of(length, 0.0, 1.0, rate)
    weight_back = column_of(length, length - 1.0, -1.0, rate)

    def rotated_back(value, slot):
        base_ = r.turn[slot]
        cosine = base_[0:1] * r.cos_off[...] - base_[1:2] * r.sin_off[...]
        sine = base_[1:2] * r.cos_off[...] + base_[0:1] * r.sin_off[...]
        return unrotate(value, cosine, sine)

    @pl.loop(0, 2)
    def _(slot):
        rows = pl.ds(pl.multiple_of(slot * length, length), length)
        weights = (mm_t(r.grad_mixed[rows, :], r.v[rows, :]) * r.mask[...]).astype(BF)
        value = mm(weights, r.k[rows, :]) + mm_t(r.grad_mixed[rows, :], r.in_bf[slot]) * weight_in
        r.grad_keys[rows, 0:key_size] = rotated_back(value, slot).astype(BF)
        r.gate[rows, 0:key_size] = t_mm(weights, r.q[rows, :])
        weights = (mm_t(r.q[rows, :], r.k[rows, :]) * r.mask[...]).astype(BF)
        r.normed[rows, :] = t_mm(weights, r.grad_mixed[rows, :])

    produce(OUT, r.gmid, r.gated, away_rest)
    next(carry, None)
    feed = reduce([r.hidden_ff], [1], r.grad_inputs, base)
    base += REDUCE_COPIES
    next(feed)
    load("wk", r.wk, r.weights.at[1, :, pl.ds(key_size, key_size)])
    load("wq", r.wq, r.weights.at[1, :, pl.ds(0, key_size)])
    emit(DOWN)
    clear(DOWN)
    produce(GATE, r.hid, r.grad_gate, away_first)
    produce(OUT, r.gmid, r.gated, home_first)
    back.early(OUT)
    next(feed)
    produce(GATE, r.hid, r.grad_gate, away_rest)
    back.late(UP)
    for _ in carry:
        pass
    out_bf = r.low_buf.at[0]
    for slot in range(2):
        out_bf[slot] = r.reach[slot].astype(BF)

    @pl.loop(0, 2)
    def _(slot):
        rows = pl.ds(pl.multiple_of(slot * length, length), length)
        value = r.gate[rows, 0:key_size] + mm_t(r.v[rows, :], out_bf[slot]) * weight_back
        r.grad_keys[rows, key_size : 2 * key_size] = rotated_back(value, slot).astype(BF)
        value = r.normed[rows, :] + mm(r.k[rows, :], out_bf[slot]) * weight_back
        r.grad_pre[rows, :] = value.astype(BF)

    produce(VALUE, r.hid, r.grad_pre, away_first)
    produce(KEYS, r.hid, r.grad_keys, away_first)
    produce(VALUE, r.hid, r.grad_pre, away_rest)
    produce(KEYS, r.hid, r.grad_keys, away_rest)
    for _ in feed:
        pass
    normed_one = r.gate.at[pl.ds(0, length), :]
    load("normed_one", r.normed_one_in, normed_one)
    peers = (sq.S, sq.Y, sq.C)
    for number, peer in enumerate(peers):
        pl.semaphore_signal(r.again.at[number], inc=1, device_id=peer, device_id_type=MESH)
    ready("middle")
    r.layer_out[...] += r.grad_inputs[...]
    back.middle(UP)
    produce(GATE, r.hid, r.grad_gate, home_first)
    back.early(GATE)
    produce(OUT, r.gmid, r.gated, home_rest)
    back.late(OUT)
    back.middle(OUT)
    for number in range(len(peers)):
        pl.semaphore_wait(r.again.at[number], 1)

    ready("wv", "wg", "wk", "wq", "normed_one")

    def value_next():
        produce(VALUE, r.hid, r.grad_pre, home_first)
        back.early(VALUE)
        produce(KEYS, r.hid, r.grad_keys, home_first)

    def keys_next():
        back.early(KEYS)
        produce(GATE, r.hid, r.grad_gate, home_rest)
        back.late(GATE)
        back.middle(GATE)

    together(
        reduce([r.grad_keys, r.grad_pre, r.grad_gate], [1, 0, 2], r.upstream, base),
        value_next,
        keys_next,
    )
    base += REDUCE_COPIES
    norm_sums(r.upstream, r.gains[0:1, :], normed_one, r.inverse_one, r.grad_middle, r.grad_inputs, 0, r.stats_two, base)
    base += 3

    copies = []
    r.all_sums[back.me] = r.sums[...]
    for mask in range(1, back.size):
        copy = remote(r.sums, r.all_sums.at[back.me], r.sum_send, r.sum_receive, mask, flipped(plan, at, mask))
        copy.start()
        copies.append(copy)
    produce(VALUE, r.hid, r.grad_pre, home_rest)
    produce(KEYS, r.hid, r.grad_keys, home_rest)
    back.late(VALUE)
    back.late(KEYS)
    emit(UP)
    back.middle(VALUE)
    emit(OUT)
    back.middle(KEYS)
    emit(GATE)
    for copy in copies:
        copy.wait_recv()
    total = r.all_sums[0]
    for i in range(1, back.size):
        total = total + r.all_sums[i]
    r.by_block[mine] = total
    for index, device in enumerate((sq.Y, sq.C, sq.X)):
        copy = remote(r.by_block.at[mine], r.by_block.at[mine], r.sends, r.receives, base + index, device)
        copy.start()
        copies.append(copy)
    for copy in copies[-3:]:
        copy.wait_recv()
    r.sums_out[...] = r.by_block[back.me * piece // width]
    for copy in copies:
        copy.wait_send()
    emit(VALUE)
    emit(KEYS)
    for unit in (UP, OUT, GATE, VALUE, KEYS):
        clear(unit)


def back_pass(plan, f, cot, rate, turn, cos_off, sin_off, rows, number):
    length, width = cot.shape
    size = 1 << len(plan.seq)
    model = f.wq_out.shape[0]
    key_size, value_size = f.q_out.shape[1], f.v_out.shape[1]
    hidden = f.wu_out.shape[1]
    both = 2 * length
    any_spec, vmem_spec = pl.BlockSpec(memory_space=pl.ANY), pl.BlockSpec(memory_space=pltpu.VMEM)

    def shape(dims, kind=F32):
        return jax.ShapeDtypeStruct(dims, kind)

    far = dict(
        wq=f.wq_out,
        wk=f.wk_out,
        wv=f.wv_out,
        wg=f.wg_out,
        wo=f.wo_out,
        wu=f.wu_out,
        wd=f.wd_out,
        hid=f.hidden_out,
        mid=f.mid_out,
        cotf=f.cot_out,
        q_in=f.q_out,
        k_in=f.k_out,
        v_in=f.v_out,
        reach_in=f.reach_out,
        gate_in=f.gate_out,
        normed_in=f.normed_out,
        inverse_in=f.inverse_out,
        gated_in=f.gated_out,
        middle_in=f.middle,
        normed_one_in=f.normed_one,
    )
    near = dict(
        cot=cot,
        inverse_one=f.inverse_one,
        normed_two=f.normed_two,
        inverse_two=f.inverse_two,
        gains=f.gains,
        rate=rate,
        turn=turn,
        cos_off=cos_off,
        sin_off=sin_off,
    )
    far_outs = dict(halves=shape((6, 2, rows, value_size), BF), gmid=shape((2, length, model), BF))
    near_outs = dict(
        layer_out=shape((length, width)), grad_inputs=shape((length, width)), sums_out=shape((8, width))
    )
    carries = carry_buffers(plan, key_size, value_size)
    dma = pltpu.SemaphoreType.DMA
    count = SPREAD_COPIES + 3 * REDUCE_COPIES + 9
    strip = max(rows, 128)
    hand, near_room, _, arrived = reduce_room(length, width)
    scratch = dict(
        weights=pltpu.VMEM((3, model, value_size), BF),
        tiles=pltpu.VMEM((2, TILE, model), BF),
        strips=pltpu.VMEM((2, both, strip), BF),
        q=pltpu.VMEM((both, key_size), BF),
        k=pltpu.VMEM((both, key_size), BF),
        v=pltpu.VMEM((both, value_size), BF),
        gate=pltpu.VMEM((both, value_size), F32),
        normed=pltpu.VMEM((both, value_size), F32),
        inverse=pltpu.VMEM((both, 128), F32),
        gated=pltpu.VMEM((both, value_size), BF),
        in_bf=pltpu.VMEM((2, key_size, value_size), BF),
        mask=pltpu.VMEM((length, length), F32),
        state=carries[0],
        reach=carries[1],
        low_buf=carries[2],
        high_buf=carries[3],
        hidden_ff=pltpu.VMEM((both, hidden), BF),
        grad_pre=pltpu.VMEM((both, hidden), BF),
        grad_gate=pltpu.VMEM((both, value_size), BF),
        grad_mixed=pltpu.VMEM((both, value_size), BF),
        grad_keys=pltpu.VMEM((both, 2 * key_size), BF),
        upstream=pltpu.VMEM((length, width), F32),
        grad_middle=pltpu.VMEM((length, width), F32),
        hand=hand,
        near=near_room,
        arrived=arrived,
        totals=pltpu.VMEM((4, model, value_size), BF),
        got=pltpu.VMEM((6, size - 1, rows, value_size), BF),
        stats=pltpu.VMEM((4, 8, length), F32),
        stats_two=pltpu.VMEM((4, 8, length), F32),
        sums=pltpu.VMEM((8, width), F32),
        all_sums=pltpu.VMEM((size, 8, width), F32),
        by_block=pltpu.VMEM((4, 8, width), F32),
        whole_strip=pltpu.VMEM((strip, value_size) if strip > rows else (8, 128), F32),
        bulk_send=dma((6 * size,)),
        bulk_receive=dma((6 * size,)),
        load_sem=dma((24,)),
        tile_sem=dma((2, 1 + model // value_size)),
        strip_sem=dma((2, 2)),
        emit_sem=dma((6, 2)),
        carry_send=dma((len(plan.seq),)),
        carry_receive=dma((len(plan.seq),)),
        sum_send=dma((size,)),
        sum_receive=dma((size,)),
        sends=dma((count,)),
        receives=dma((count,)),
        local_sem=dma((1,)),
        again=pltpu.SemaphoreType.REGULAR((3,)),
    )
    names = list(far) + list(near) + list(far_outs) + list(near_outs) + list(scratch)

    def kernel(*refs):
        back_kernel(plan, names, *refs)

    results = pl.pallas_call(
        kernel,
        out_shape=tuple(far_outs.values()) + tuple(near_outs.values()),
        in_specs=[any_spec] * len(far) + [vmem_spec] * len(near),
        out_specs=(any_spec,) * len(far_outs) + (vmem_spec,) * len(near_outs),
        scratch_shapes=list(scratch.values()),
        compiler_params=pltpu.CompilerParams(
            collective_id=number, has_side_effects=True, vmem_limit_bytes=VMEM_LIMIT
        ),
        name="back",
    )(*far.values(), *near.values())
    out = types.SimpleNamespace(**dict(zip(list(far_outs) + list(near_outs), results)))
    return finish(out, key_size)


def finish_kernel(key_size, halves, layer_in, grad_in, *refs):
    *outs, layer_out, grad_out = refs[:9]
    *stages, layer, grad, sems = refs[9:]
    loads = [
        pltpu.make_async_copy(source, stage, sems.at[number])
        for number, (source, stage) in enumerate(((layer_in, layer), (grad_in, grad)))
    ]
    for copy in loads:
        copy.start()
    stores = []

    def store(stage, target):
        copy = pltpu.make_async_copy(stage, target, sems.at[2 + len(stores)])
        copy.start()
        stores.append(copy)

    rows, columns = halves.shape[2:]
    for out, stage, unit, first, width in zip(
        outs, stages, (5, 5, 4, 3, 0, 2, 1), (0, key_size, 0, 0, 0, 0, 0), (key_size,) * 2 + (columns,) * 5
    ):
        for half in range(2):
            value = halves[unit, half, :, first : first + width].astype(F32)
            if out.shape[0] == rows:
                stage[:, half * width : (half + 1) * width] = value
            else:
                stage[half * width : (half + 1) * width, :] = value.T
        store(stage, out)
    for copy, stage, out in zip(loads, (layer, grad), (layer_out, grad_out)):
        copy.wait()
        store(stage, out)
    for copy in stores:
        copy.wait()


def finish(b, key_size):
    rows, value_size = b.halves.shape[2:]
    turned = rows % 128 == 0
    flat = [(rows, 2 * w) for w in (key_size, key_size, value_size, value_size, value_size)]
    shapes = flat + [(2 * value_size, rows) if turned else (rows, 2 * value_size)] * 2 + [b.layer_out.shape] * 2
    any_spec = pl.BlockSpec(memory_space=pl.ANY)
    results = pl.pallas_call(
        functools.partial(finish_kernel, key_size),
        out_shape=tuple(jax.ShapeDtypeStruct(s, F32) for s in shapes),
        in_specs=[pl.BlockSpec(memory_space=pltpu.VMEM), any_spec, any_spec],
        out_specs=tuple([any_spec] * len(shapes)),
        scratch_shapes=[pltpu.VMEM(s, F32) for s in shapes] + [pltpu.SemaphoreType.DMA((2 + len(shapes),))],
        name="finish",
    )(b.halves, b.layer_out, b.grad_inputs)
    gq, gk, gv, gg, gu, go, gd, layer_out, grad_inputs = results
    if not turned:
        go, gd = go.T, gd.T
    return types.SimpleNamespace(
        gq=gq, gk=gk, gv=gv, gg=gg, gu=gu, go=go, gd=gd, layer_out=layer_out, grad_inputs=grad_inputs, sums_out=b.sums_out
    )


def rotate(values, cosine, sine):
    half = values.shape[1] // 2
    first, second = values[:, :half], values[:, half:]
    return jnp.concatenate([first * cosine - second * sine, first * sine + second * cosine], axis=1)


def unrotate(values, cosine, sine):
    half = values.shape[1] // 2
    first, second = values[:, :half], values[:, half:]
    return jnp.concatenate([first * cosine + second * sine, second * cosine - first * sine], axis=1)


def on_device(
    plan,
    inputs,
    decay_exponent,
    first_gain,
    first_bias,
    query_weight,
    key_weight,
    value_weight,
    gate_weight,
    out_weight,
    second_gain,
    second_bias,
    up_weight,
    down_weight,
    cotangent,
):
    length, model = inputs.shape
    rows = query_weight.shape[0]
    pair_bit = lax.axis_index(plan.pair)
    column = lax.axis_index(plan.head_axes)
    width = cotangent.shape[1]

    key_size = query_weight.shape[1] // 2
    value_size = value_weight.shape[1] // 2
    hidden = up_weight.shape[1] // 2

    vec = jnp.stack([first_gain, first_bias, second_gain, second_bias] * 2).astype(F32)

    exponent = pick(decay_exponent, pair_bit, 0).astype(F32)
    lograte = jnp.log1p(-jnp.exp2(-exponent))
    offset = jnp.arange(length, dtype=F32)
    seq_index = lax.axis_index(plan.seq_axes)
    pair_weight = 2 ** plan.seq.index(plan.pair)
    first_slot = seq_index - pair_bit * pair_weight
    starts = jnp.stack([first_slot, first_slot + pair_weight]) * length
    frequency = np.exp(-math.log(10000.0) * np.arange(key_size // 2, dtype=np.float32) / (key_size // 2 - 1))
    frequency = frequency.astype(np.float32)
    angles = np.arange(length)[:, None] * frequency.astype(np.float64)[None, :]
    cos_off, sin_off = jnp.asarray(np.cos(angles), F32), jnp.asarray(np.sin(angles), F32)
    start_angles = starts.astype(F32)[:, None] * frequency[None, :]
    turn = jnp.stack([jnp.cos(start_angles), jnp.sin(start_angles)] * 4, axis=1)
    shards = [query_weight, key_weight, value_weight, gate_weight, out_weight, up_weight, down_weight]
    rate = jnp.full((8, 128), lograte, F32)
    f = front(plan, shards, inputs, cotangent, vec, rate, turn, cos_off, sin_off, 1)
    b = back_pass(plan, f, cotangent, rate, turn, cos_off, sin_off, rows, 2)
    place = seq_index % (width // rows) * rows
    mine = lax.dynamic_slice_in_dim(b.sums_out, place, rows, 1)
    return (
        b.layer_out,
        b.grad_inputs,
        mine[0],
        mine[1],
        b.gq,
        b.gk,
        b.gv,
        b.gg,
        b.go,
        mine[2],
        mine[3],
        b.gu,
        b.gd,
    )


def solution(mesh):
    seq_bits = (mesh.shape["seq"]).bit_length() - 1
    head_bits = (mesh.shape["head"]).bit_length() - 1
    plan = Plan(seq_bits, head_bits)
    seq, head = plan.seq_axes, plan.head_axes
    fine = Mesh(mesh.devices.reshape((2,) * (seq_bits + head_bits)), seq + head)
    in_specs = (
        P(seq, None),
        P(head),
        P(seq),
        P(seq),
        P(seq, head),
        P(seq, head),
        P(seq, head),
        P(seq, head),
        P(head, seq),
        P(seq),
        P(seq),
        P(seq, head),
        P(head, seq),
        P(seq, head),
    )
    out_specs = (
        P(seq, head),
        P(seq, head),
        P(seq),
        P(seq),
        P(seq, head),
        P(seq, head),
        P(seq, head),
        P(seq, head),
        P(head, seq),
        P(seq),
        P(seq),
        P(seq, head),
        P(head, seq),
    )

    def step(*args):
        return on_device(plan, *args)

    return jax.shard_map(step, mesh=fine, in_specs=in_specs, out_specs=out_specs, check_vma=False)
```
